32 devices in a mesh: dp: 16 (over z, x, core), mp: 2 (over y).
Axes of the slice: x: 2, y: 2, z: 4, core: 2. Of those that a mesh axis runs over, the one named last changes fastest.
Arguments:
- node_feats: bfloat16 [256, 32768], P('mp', 'dp'), may hold values from -6 to 6
- proj_weight: bfloat16 [256, 256], P('mp'), may hold values from -0.375 to 0.375
- att_src: float32 [256], P('mp'), may hold values from -32 to 32
- att_dst: float32 [256], P('mp'), may hold values from -32 to 32
- out_bias: float32 [256], P('mp'), may hold values from -3 to 3
- tile_rows: int32 [512], P('dp'), may hold values from 0 to 255, as said below
- tile_cols: int32 [512], P('dp'), may hold values from 0 to 255, as said below
- tile_masks: int32 [512, 4, 128], P('dp'), may hold values from -2147483648 to 2147483646
Outputs:
- node_out: bfloat16 [256, 32768], P('mp', 'dp')
The draws below stay inside these ranges and needn't reach their ends.
Inputs may be any that keep to these rules, and one draw needn't show every extreme that they name: `tile_rows`: block b holds nodes 128 b to 128 b + 127 and belongs to index b // 16 of dp. Among the 32 tiles of one index of dp, no owner's blocks are named more than 4 times; on every index one owner's blocks are named exactly 4 times. `tile_cols`: the same bound holds for source blocks: among the 32 tiles of one index of dp, no owner's blocks are named more than 4 times, and one owner's exactly 4 times on every index.
All inputs are finite; a program needn't handle non-finite values.
Results may differ from the reference program's by a relative error of at most 0.0034.
Values may be sent and summed in bfloat16 or wider, within the bound.
A program may use at most 64 MiB of HBM per device.

```python
import jax
import jax.numpy as jnp
from jax import lax

FIN = 256
HEADS = 8
HD = 32
TILE = 128
TILES_DEV = 32
NODES = 32768
BLK_DEV = 16
NBLK = 256
TILES = 512
CAP = 4
N_DP = 16


def tile_blocks(key, salt):
    base_key = jax.random.fold_in(key, salt)
    hub_owner = jax.random.randint(jax.random.fold_in(base_key, 7), (), 0, N_DP)

    def device_tiles(device):
        device_key = jax.random.fold_in(base_key, device)
        key_rest, key_shift, key_local, key_order = jax.random.split(device_key, 4)
        rest_slots = CAP + jax.random.permutation(key_rest, N_DP * CAP - CAP)[:TILES_DEV - CAP]
        position = jnp.concatenate([jnp.arange(CAP, dtype=jnp.int32), rest_slots.astype(jnp.int32)])
        shifts = jnp.concatenate([jnp.zeros((1,), jnp.int32), 1 + jax.random.permutation(key_shift, N_DP - 1).astype(jnp.int32)])
        owners = (hub_owner + shifts[position // CAP]) % N_DP
        local_block = jax.random.randint(key_local, (TILES_DEV,), 0, BLK_DEV)
        blocks = owners * BLK_DEV + local_block
        return blocks[jax.random.permutation(key_order, TILES_DEV)]
    return jax.vmap(device_tiles)(jnp.arange(N_DP)).reshape(-1).astype(jnp.int32)


def draw_tile_rows(key, part):
    return tile_blocks(key, 101)


def draw_tile_cols(key, part):
    return tile_blocks(key, 202)


def attention_vector(key):
    key_base = jax.random.fold_in(key, 0)
    vector = 0.25 * jnp.clip(jax.random.normal(key_base, (HEADS, HD), jnp.float32), -4.0, 4.0)
    return vector.reshape(-1)


def draw_att_src(key, part):
    return attention_vector(jax.random.fold_in(key, 11))


def draw_att_dst(key, part):
    return attention_vector(jax.random.fold_in(key, 23))


def plant(entries, key, smallest, top_value):
    index_at = [jax.random.randint(jax.random.fold_in(key, axis), (), 0, length) for axis, length in enumerate(entries.shape)]
    widest = entries.shape.index(max(entries.shape))
    neighbour = index_at[:widest] + [(index_at[widest] + 1) % entries.shape[widest]] + index_at[widest + 1:]
    return entries.at[tuple(index_at)].set(smallest).at[tuple(neighbour)].set(top_value)


def levels(rng, shape, pieces, low, top_value):
    loudness, own = 1.0, jax.random.fold_in(rng, 6)
    for dim, parts in pieces:
        draws = jnp.exp(jax.random.uniform(jax.random.fold_in(own, dim), (parts,), jnp.float32, low / len(pieces), top_value / len(pieces)))
        loudness = loudness * jnp.repeat(draws, shape[dim] // parts).reshape([-1 if axis == dim else 1 for axis in range(len(shape))])
    return loudness


def bell_draw(stream_key, extent, width, limit, shards=(), held_as=jnp.bfloat16):
    values = width * jax.random.normal(stream_key, extent, jnp.float32)
    if shards:
        values = values * levels(stream_key, extent, shards, -0.22, 0.18)
    return jnp.clip(values, -limit, limit).astype(held_as)


def setup_inputs(seed: int = 0) -> dict:
    streams_of = jax.random.split(jax.random.key(seed), 9)
    return {
        "node_feats": bell_draw(streams_of[0], (FIN, NODES), 1.0, 6.0, ((0, 2), (1, 16))),
        "proj_weight": bell_draw(streams_of[1], (HEADS * HD, FIN), FIN ** -0.5, 0.375, ((0, 2),)),
        "att_src": draw_att_src(jax.random.fold_in(streams_of[8], 71), 0),
        "att_dst": draw_att_dst(jax.random.fold_in(streams_of[8], 71), 0),
        "out_bias": bell_draw(streams_of[4], (HEADS * HD,), 0.5, 3.0, ((0, 2),), jnp.float32),
        "tile_rows": draw_tile_rows(jax.random.fold_in(streams_of[8], 71), 0),
        "tile_cols": draw_tile_cols(jax.random.fold_in(streams_of[8], 71), 0),
        "tile_masks": plant(jax.random.randint(streams_of[7], (TILES, TILE // 32, TILE), -2147483648, 2147483647), jax.random.fold_in(streams_of[7], 1), -2147483648, 2147483646).astype(jnp.int32),
    }


far_below = -1.0e30


def leaky_relu(scores):
    return jnp.where(scores > 0, scores, 0.2 * scores)


def unpack_bits(packed):
    offsets = jnp.arange(32, dtype=jnp.int32)
    spread = jnp.bitwise_and(jnp.right_shift(packed[..., :, None, :], offsets[:, None]), 1)
    return spread.reshape(packed.shape[:-2] + (packed.shape[-2] * 32, packed.shape[-1])).astype(jnp.int32)


def edge_scores(edge_mask, source, target):
    raw_scores = leaky_relu(target[:, :, None, :] + source[:, :, :, None])
    return jnp.where(edge_mask[:, None] == 1, raw_scores, far_below)


def reference(node_feats, proj_weight, att_src, att_dst, out_bias, tile_rows, tile_cols, tile_masks):
    projected = jnp.dot(proj_weight, node_feats, preferred_element_type=jnp.float32)
    features = projected.astype(jnp.bfloat16)
    by_head = projected.reshape(HEADS, HD, NODES)
    source = jnp.einsum("hd,hdn->hn", att_src.reshape(HEADS, HD), by_head, precision=lax.Precision.HIGHEST)
    target = jnp.einsum("hd,hdn->hn", att_dst.reshape(HEADS, HD), by_head, precision=lax.Precision.HIGHEST)
    source_blocks = source.reshape(HEADS, NBLK, TILE).transpose(1, 0, 2)
    target_blocks = target.reshape(HEADS, NBLK, TILE).transpose(1, 0, 2)
    feat_blocks = features.reshape(HEADS, HD, NBLK, TILE).transpose(2, 0, 1, 3)
    group_rows = tile_rows.reshape(-1, TILES_DEV)
    group_cols = tile_cols.reshape(-1, TILES_DEV)
    group_masks = tile_masks.reshape(-1, TILES_DEV, TILE // 32, TILE)

    def tile_scores(inputs):
        row_ids, col_ids, packed = inputs
        edge_mask = unpack_bits(packed)
        scores = edge_scores(edge_mask, source_blocks[col_ids], target_blocks[row_ids])
        tile_peaks = jnp.max(scores, axis=2)
        weights = jnp.where(edge_mask[:, None] == 1, jnp.exp(scores - tile_peaks[:, :, None, :]), 0.0)
        return tile_peaks, weights

    def first_pass(inputs):
        tile_peaks, weights = tile_scores(inputs)
        return tile_peaks, jnp.sum(weights, axis=2)

    tile_peaks, masses = lax.map(first_pass, (group_rows, group_cols, group_masks))
    tile_peaks = tile_peaks.reshape(TILES, HEADS, TILE)
    masses = masses.reshape(TILES, HEADS, TILE)
    self_scores = leaky_relu(source_blocks + target_blocks)
    row_peak = self_scores.at[tile_rows].max(tile_peaks)
    self_weight = jnp.exp(self_scores - row_peak)
    denominator = self_weight.at[tile_rows].add(jnp.exp(tile_peaks - row_peak[tile_rows]) * masses)

    def second_pass(summed, inputs):
        row_ids, col_ids, packed = inputs
        peaks_here, weights = tile_scores(inputs)
        rounded = lax.optimization_barrier(weights.astype(jnp.bfloat16)).astype(jnp.float32)
        partial_values = jnp.einsum("ghdc,ghcr->ghdr", feat_blocks[col_ids].astype(jnp.float32), rounded)
        rescale = jnp.exp(peaks_here - row_peak[row_ids])
        return summed.at[row_ids].add(rescale[:, :, None, :] * partial_values), None

    start_sum = self_weight[:, :, None, :] * feat_blocks.astype(jnp.float32)
    summed, ignored = lax.scan(second_pass, start_sum, (group_rows, group_cols, group_masks))
    gathered = summed / denominator[:, :, None, :]
    flat_out = gathered.transpose(1, 2, 0, 3).reshape(HEADS * HD, NODES)
    return jax.nn.elu(flat_out + node_feats.astype(jnp.float32) + out_bias[:, None]).astype(jnp.bfloat16)
```

```python
import functools
import math

import jax
import jax.numpy as jnp
from jax import lax
from jax.experimental import pallas as pl
from jax.experimental.pallas import tpu as pltpu
from jax.sharding import PartitionSpec as P

HD = 32
LOG2E = 1.4426950408889634
FAR_BELOW = -1e30
FLOOR = -1e9
VMEM = pltpu.VMEM
LANES = 128
MESH = pl.DeviceIdType.MESH


def leaky_relu(scores):
    return jnp.maximum(scores, 0.2 * scores)


def main_kernel(
    heads,
    capacity,
    chunks,
    depth,
    peers,
    weight_ref,
    nodes_ref,
    params_ref,
    masks_ref,
    codes_ref,
    feats_ref,
    total_ref,
    part_ref,
    stats_ref,
    other_ref,
    *scratch,
):
    (
        first_half,
        all_source,
        targ,
        all_nodes,
        masks2,
        got_codes,
        codes2,
        u_send,
        u_all,
        score_send,
        score_recv,
        table_v,
        table,
        weights,
        keeps,
        scales,
        bests,
        masses,
        scan,
        part_send,
        stats_send,
        node_send,
        node_recv,
        u_ss,
        u_rs,
        score_ss,
        score_rs,
        mask_ss,
        mask_rs,
        code_ss,
        code_rs,
        far_ss,
        facing_ss,
        core_ss,
        recv_sem,
        pair_ss,
        pair_rs,
        part_ss,
        part_rs,
        local_sem,
    ) = scratch[: len(scratch) - heads]
    second_half = scratch[len(scratch) - heads :]

    devices = 4 * depth
    groups = depth // 2
    me = lax.axis_index("dp")
    core = lax.rem(me, 2)
    beside = lax.rem(lax.div(me, 2), 2)
    level = lax.div(me, 4)
    parity = lax.rem(level, 2)
    where_in = lax.div(level, 2)
    mine = lax.axis_index("mp")
    dims, columns = nodes_ref.shape
    head_dims = weight_ref.shape[0]
    size = LANES
    blocks = columns // size
    hb = blocks // 2
    per = blocks // chunks
    width = per * size
    slots = devices * capacity
    positions = 2 * slots
    early = chunks // 2
    score_item = early
    items = early + 1 + heads

    def place(lev, b, c):
        return (lev * 2 + b) * 2 + c

    def origin_of(q, b, c):
        return (q * 2 + b) * 2 + c

    own = origin_of(where_in, beside, core)
    facing = place(level, 1 - beside, core)
    other_core = place(level, beside, 1 - core)
    pair = place(level + 1 - 2 * parity, beside, core)

    barrier = pltpu.get_barrier_semaphore()
    for shift in range(1, devices):
        pl.semaphore_signal(barrier, 1, device_id={"dp": lax.rem(me + shift, devices)}, device_id_type=MESH)
    for shift in range(1, peers):
        pl.semaphore_signal(barrier, 1, device_id={"mp": lax.rem(mine + shift, peers)}, device_id_type=MESH)

    own_rows = pl.ds(pl.multiple_of(mine * dims, dims), dims)
    for chunk in range(chunks):
        all_nodes[chunk, own_rows, :] = nodes_ref[:, chunk * width : (chunk + 1) * width]
    masks2[pl.ds(me * capacity, capacity)] = masks_ref[me]
    got_codes[me] = codes_ref[me]
    params = jnp.transpose(params_ref[...])[:head_dims]
    wide = weight_ref[...].astype(jnp.float32)
    by_source = wide * (LOG2E * params[:, 0:1])
    by_target = wide * (LOG2E * params[:, 1:2])
    rows = []
    for scaled in (by_source, by_target):
        for head in range(heads):
            rows.append(jnp.sum(scaled[head * HD : (head + 1) * HD], axis=0, keepdims=True))
    reduced = jnp.concatenate(rows, axis=0)
    for peer in range(peers):
        u_send[peer] = reduced[:, peer * dims : (peer + 1) * dims]
    u_all[mine] = u_send[mine]
    pl.semaphore_wait(barrier, devices - 1 + peers - 1)

    def node_copy(shift, chunk):
        return pltpu.make_async_remote_copy(
            src_ref=nodes_ref.at[:, pl.ds(chunk * width, width)],
            dst_ref=all_nodes.at[chunk, own_rows, :],
            send_sem=node_send.at[shift - 1, chunk],
            recv_sem=node_recv.at[shift - 1, chunk],
            device_id={"mp": lax.rem(mine + shift, peers)},
            device_id_type=MESH,
        )

    def u_copy(shift):
        to = lax.rem(mine + shift, peers)
        return pltpu.make_async_remote_copy(
            src_ref=u_send.at[to],
            dst_ref=u_all.at[mine],
            send_sem=u_ss.at[shift - 1],
            recv_sem=u_rs.at[shift - 1],
            device_id={"mp": to},
            device_id_type=MESH,
        )

    def score_copy(shift):
        to = lax.rem(mine + shift, peers)
        return pltpu.make_async_remote_copy(
            src_ref=score_send.at[to],
            dst_ref=score_recv.at[mine],
            send_sem=score_ss.at[shift - 1],
            recv_sem=score_rs.at[shift - 1],
            device_id={"mp": to},
            device_id_type=MESH,
        )

    def mask_copy(shift):
        to = lax.rem(me + shift, devices)
        return pltpu.make_async_remote_copy(
            src_ref=masks_ref.at[to],
            dst_ref=masks2.at[pl.ds(me * capacity, capacity)],
            send_sem=mask_ss.at[shift - 1],
            recv_sem=mask_rs.at[shift - 1],
            device_id={"dp": to},
            device_id_type=MESH,
        )

    def code_copy(shift):
        to = lax.rem(me + shift, devices)
        return pltpu.make_async_remote_copy(
            src_ref=codes_ref.at[to],
            dst_ref=got_codes.at[me],
            send_sem=code_ss.at[shift - 1],
            recv_sem=code_rs.at[shift - 1],
            device_id={"dp": to},
            device_id_type=MESH,
        )

    def pair_copy(which):
        src, dst = (
            (masks2.at[pl.ds(0, slots)], masks2.at[pl.ds(slots, slots)]),
            (codes2.at[0], codes2.at[1]),
            (targ.at[pl.ds(blocks, blocks)], targ.at[pl.ds(0, blocks)]),
            (stats_send, other_ref),
        )[which]
        return pltpu.make_async_remote_copy(
            src_ref=src,
            dst_ref=dst,
            send_sem=pair_ss.at[which],
            recv_sem=pair_rs.at[which],
            device_id={"dp": pair},
            device_id_type=MESH,
        )

    def part_copy(head):
        return pltpu.make_async_remote_copy(
            src_ref=part_send.at[head],
            dst_ref=part_ref.at[head],
            send_sem=part_ss.at[head],
            recv_sem=part_rs.at[head],
            device_id={"dp": pair},
            device_id_type=MESH,
        )

    def item_ref(origin, item):
        if item < early:
            return first_half.at[pl.ds(origin * hb + item * per, per)]
        if item == score_item:
            return all_source.at[pl.ds(origin * blocks, blocks)]
        return second_half[item - score_item - 1].at[pl.ds(origin * hb, hb)]

    def send(origin, item, to, sem):
        part = item_ref(origin, item)
        return pltpu.make_async_remote_copy(
            src_ref=part,
            dst_ref=part,
            send_sem=sem,
            recv_sem=recv_sem.at[origin, item],
            device_id={"dp": to},
            device_id_type=MESH,
        )

    def far_copy(shift, item):
        to = place(2 * lax.rem(where_in + shift, groups) + parity, beside, core)
        return send(own, item, to, far_ss.at[shift - 1, item])

    def facing_copy(q, item):
        return send(origin_of(q, beside, core), item, facing, facing_ss.at[q, item])

    def core_copy(q, b, item):
        return send(origin_of(q, b, core), item, other_core, core_ss.at[q, b, item])

    def arrival(origin, item):
        send(origin, item, other_core, core_ss.at[0, 0, item]).wait_recv()

    def own_out(item):
        for shift in range(1, groups):
            far_copy(shift, item).start()
        facing_copy(where_in, item).start()
        core_copy(where_in, beside, item).start()

    def far_q(shift):
        return lax.rem(where_in + groups - shift, groups)

    def from_far(item):
        for shift in range(1, groups):
            q = far_q(shift)
            arrival(origin_of(q, beside, core), item)
            facing_copy(q, item).start()
            core_copy(q, beside, item).start()

    def from_facing(item):
        arrival(origin_of(where_in, 1 - beside, core), item)
        core_copy(where_in, 1 - beside, item).start()

    def from_facing_far(item):
        for shift in range(1, groups):
            q = far_q(shift)
            arrival(origin_of(q, 1 - beside, core), item)
            core_copy(q, 1 - beside, item).start()

    def from_core(item):
        for q in range(groups):
            for b in range(2):
                arrival(origin_of(q, b, 1 - core), item)

    def project(chunk):
        for shift in range(1, peers):
            node_copy(shift, chunk).wait_recv()
        projected = jnp.dot(weight_ref[...], all_nodes[chunk], preferred_element_type=jnp.float32)
        rounded = projected.astype(jnp.bfloat16)
        for j in range(per):
            block = chunk * per + j
            span = slice(j * size, (j + 1) * size)
            feats_ref[block] = rounded[:, span]
            if chunk < early:
                first_half[own * hb + block] = rounded[:, span]
            else:
                for head in range(heads):
                    second_half[head][own * hb + block - hb] = rounded[head * HD : (head + 1) * HD, span]

    for shift in range(1, peers):
        u_copy(shift).start()
    for shift in range(1, peers):
        node_copy(shift, 0).start()
    for shift in range(1, devices):
        code_copy(shift).start()
        mask_copy(shift).start()
    for chunk in range(1, min(2, chunks)):
        for shift in range(1, peers):
            node_copy(shift, chunk).start()

    for shift in range(1, peers):
        u_copy(shift).wait_recv()
    stacked = jnp.concatenate([u_all[peer] for peer in range(peers)], axis=0)
    high = stacked.astype(jnp.bfloat16)
    rest = stacked - high.astype(jnp.float32)
    middle = rest.astype(jnp.bfloat16)
    low = (rest - middle.astype(jnp.float32)).astype(jnp.bfloat16)
    pieces = jnp.concatenate([high, middle, low], axis=0)
    count = 2 * heads * peers
    scored = jnp.dot(pieces, nodes_ref[...], preferred_element_type=jnp.float32)
    scored = scored[:count] + scored[count : 2 * count] + scored[2 * count :]
    for peer in range(peers):
        score_send[peer] = scored[peer * 2 * heads : (peer + 1) * 2 * heads]
    score_recv[mine] = score_send[mine]
    for shift in range(1, peers):
        score_copy(shift).start()
    for chunk in range(2, chunks):
        for shift in range(1, peers):
            node_copy(shift, chunk).start()

    project(0)
    own_out(0)
    for shift in range(1, peers):
        score_copy(shift).wait_recv()
    scores = score_recv[0]
    for peer in range(1, peers):
        scores = scores + score_recv[peer]
    for block in range(blocks):
        span = slice(block * size, (block + 1) * size)
        source = scores[:heads, span]
        target = scores[heads:, span]
        all_source[own * blocks + block] = source
        targ[blocks + block] = target
        stats_ref[0, block] = leaky_relu(source + target)
    own_out(score_item)
    pair_copy(2).start()

    def tables():
        for shift in range(1, devices):
            code_copy(shift).wait_recv()
        gathered = got_codes[0]
        for device in range(1, devices):
            gathered = gathered + got_codes[device]
        codes2[0] = gathered
        pair_copy(1).start()
        for shift in range(1, devices):
            mask_copy(shift).wait_recv()
        pair_copy(0).start()

    def order():
        pair_copy(1).wait_recv()
        here = codes2[0]
        there = codes2[1]
        row = jnp.concatenate([here[0:1], there[0:1]], axis=1)
        where_col = jnp.concatenate([here[1:2], there[1:2]], axis=1)
        col_parity = jnp.concatenate([here[2:3], there[2:3]], axis=1)
        total_lanes = row.shape[1]
        lane = lax.broadcasted_iota(jnp.int32, (1, total_lanes), 1)
        key = row - 1 + jnp.where(lane < total_lanes // 2, blocks, 0)
        key = jnp.where((row > 0) & (col_parity == parity), key, 2 * blocks)
        both = jnp.concatenate([key, where_col] + [key] * 6, axis=0)
        turned = jnp.transpose(both)
        key_t = turned[:, 0:1]
        col_t = turned[:, 1:2]
        along = lax.broadcasted_iota(jnp.int32, (total_lanes, total_lanes), 1)
        down = lax.broadcasted_iota(jnp.int32, (total_lanes, total_lanes), 0)
        before = (key_t < key) | ((key_t == key) & (down < along))
        rank = jnp.sum(jnp.where(before, 1, 0), axis=0, keepdims=True)
        rank_t = jnp.transpose(jnp.concatenate([rank] * 8, axis=0))[:, 0:1]
        at = rank_t == along
        table_v[0:1] = jnp.sum(jnp.where(at, down, 0), axis=0, keepdims=True)
        table_v[1:2] = jnp.sum(jnp.where(at, key_t, 0), axis=0, keepdims=True)
        table_v[2:3] = jnp.sum(jnp.where(at, col_t, 0), axis=0, keepdims=True)
        table_v[3:4] = jnp.sum(jnp.where(key_t <= along, 1, 0), axis=0, keepdims=True)
        table_v[4:8] = jnp.zeros((4, total_lanes), jnp.int32)
        fetch = pltpu.make_async_copy(table_v, table, local_sem)
        fetch.start()
        fetch.wait()

    def after(chunk):
        plan = {
            1: [(from_facing, 0), (from_facing, score_item)],
            2: [(from_far, 0), (from_facing, 1)],
            3: [(from_far, score_item), (from_facing, 2)],
            4: [(from_facing_far, 0)],
            5: [(from_far, 1), (from_facing, 3), (from_facing_far, score_item)],
        }
        for what, item in plan.get(chunk, []):
            what(item)

    standard = early == 4
    for chunk in range(1, chunks):
        project(chunk)
        if chunk < early:
            own_out(chunk)
        if standard:
            after(chunk)
        if chunk == min(3, chunks - 1):
            tables()
        if chunk == min(6, chunks - 1):
            order()
    for head in range(heads):
        own_out(score_item + 1 + head)

    first = score_item + 1
    if standard and heads == 4:
        relays = [
            [(from_far, 2), (from_facing_far, 1)],
            [(from_facing, first), (from_far, 3), (from_facing_far, 2)],
            [(from_facing, first + 1), (from_far, first), (from_facing_far, 3)],
            [(from_facing, first + 2), (from_far, first + 1), (from_facing_far, first)],
            [(from_facing, first + 3), (from_far, first + 2), (from_facing_far, first + 1)],
            [(from_far, first + 3), (from_facing_far, first + 2)],
        ]
        last = [(from_facing_far, first + 3)]
    else:
        for item in [score_item] + [i for i in range(items) if i != score_item]:
            from_facing(item)
            from_far(item)
            from_facing_far(item)
        relays = [[]]
        last = []

    from_core(score_item)
    pair_copy(2).wait_recv()
    pair_copy(0).wait_recv()
    words = size // 32
    bit = lax.broadcasted_iota(jnp.int32, (32, size), 0)

    def partial(k):
        slot = table[0, k]
        key = table[1, k]
        column = table[2, k]
        half = lax.div(slot, LANES)
        index = half * slots + jnp.minimum(lax.rem(slot, LANES), slots - 1)
        packed = masks2[index] * jnp.where(key < 2 * blocks, 1, 0)
        edges = jnp.concatenate(
            [
                jnp.bitwise_and(jnp.right_shift(packed[word : word + 1, :], bit), 1)
                for word in range(words)
            ],
            axis=0,
        ) != 0
        source = all_source[column]
        source = jnp.transpose(jnp.concatenate([source] * (8 // heads), axis=0))
        target = targ[jnp.minimum(key, 2 * blocks - 1)]
        peaks, sums = [], []
        for head in range(heads):
            one = slice(head, head + 1)
            here = jnp.where(edges, source[:, one], FAR_BELOW)
            aim = target[one]
            peak = leaky_relu(aim + jnp.max(here, axis=0, keepdims=True))
            peak = jnp.maximum(peak, FLOOR)
            weight = jnp.exp2(leaky_relu(here + aim) - peak)
            peaks.append(peak)
            sums.append(jnp.sum(weight, axis=0, keepdims=True))
            weights[k, head] = weight.astype(jnp.bfloat16)
        same = (k > 0) & (key == table[1, jnp.maximum(k - 1, 0)])
        return same, jnp.concatenate(peaks, axis=0), jnp.concatenate(sums, axis=0)

    together = math.gcd(positions, 4)

    def step(index, carry):
        run, mass = carry
        parts = [(index * together + w, partial(index * together + w)) for w in range(together)]
        for k, (same, peak, summed) in parts:
            again = jnp.where(same, 1.0, 0.0)
            old = jnp.where(same, run, FLOOR)
            new = jnp.maximum(old, peak)
            keep = jnp.exp2(old - new) * again
            scale = jnp.exp2(peak - new)
            mass = mass * keep + summed * scale
            run = new
            keeps[k] = keep
            scales[k] = scale
            bests[k] = run
            masses[k] = mass
        return run, mass

    steps = positions // together
    carry = (jnp.full((heads, size), FLOOR, jnp.float32), jnp.zeros((heads, size), jnp.float32))
    at = 0
    for number, events in enumerate(relays):
        until = steps * (number + 1) // len(relays)
        for what, item in events:
            what(item)
        carry = lax.fori_loop(at, until, step, carry)
        at = until
    for what, item in last:
        what(item)

    def ending(key):
        upto = table[3, key]
        prior = table[3, max(key - 1, 0)] if key > 0 else 0
        return jnp.maximum(upto - 1, 0), upto > prior

    for block in range(blocks):
        index, some = ending(block)
        stats_send[0, block] = jnp.where(some, bests[index], FLOOR)
        stats_send[1, block] = jnp.where(some, masses[index], 0.0)
    pair_copy(3).start()
    for block in range(blocks):
        index, some = ending(blocks + block)
        stats_ref[1, block] = jnp.where(some, bests[index], FLOOR)
        stats_ref[2, block] = jnp.where(some, masses[index], 0.0)

    for item in range(early):
        from_core(item)
    unroll = math.gcd(positions, 8)

    for head in range(heads):
        from_core(score_item + 1 + head)
        rows = slice(head * HD, (head + 1) * HD)
        one = slice(head, head + 1)

        def accumulate(index, total, head=head, rows=rows, one=one):
            values = []
            for w in range(unroll):
                k = index * unroll + w
                column = table[2, k]
                origin = lax.div(column, blocks)
                block = lax.rem(column, blocks)
                spot = origin * hb + lax.rem(block, hb)
                feats = jnp.where(block < hb, first_half[spot, rows], second_half[head][spot])
                values.append(jnp.dot(feats, weights[k, head], preferred_element_type=jnp.float32))
            for w in range(unroll):
                k = index * unroll + w
                total = total * keeps[k, one] + values[w] * scales[k, one]
                scan[k] = total
            return total

        lax.fori_loop(0, positions // unroll, accumulate, jnp.zeros((HD, size), jnp.float32))
        for block in range(blocks):
            index, some = ending(block)
            part_send[head, block] = jnp.where(some, scan[index], 0.0).astype(jnp.bfloat16)
        part_copy(head).start()
        for block in range(blocks):
            index, some = ending(blocks + block)
            total_ref[head, block] = jnp.where(some, scan[index], 0.0)

    for shift in range(1, peers):
        u_copy(shift).wait_send()
        score_copy(shift).wait_send()
        for chunk in range(chunks):
            node_copy(shift, chunk).wait_send()
    for shift in range(1, devices):
        code_copy(shift).wait_send()
        mask_copy(shift).wait_send()
    for item in range(items):
        for shift in range(1, groups):
            far_copy(shift, item).wait_send()
        for q in range(groups):
            facing_copy(q, item).wait_send()
            for b in range(2):
                core_copy(q, b, item).wait_send()
    for which in range(4):
        pair_copy(which).wait_send()
    pair_copy(3).wait_recv()
    for head in range(heads):
        part_copy(head).wait()


def finish_kernel(
    heads,
    feats_ref,
    total_ref,
    part_ref,
    stats_ref,
    other_ref,
    nodes_ref,
    params_ref,
    out_ref,
):
    blocks = feats_ref.shape[0]
    size = LANES
    bias = jnp.transpose(params_ref[...])[:, 2:3]
    for block in range(blocks):
        span = slice(block * size, (block + 1) * size)
        itself = stats_ref[0, block]
        here = stats_ref[1, block]
        there = other_ref[0, block]
        best = jnp.maximum(jnp.maximum(itself, here), there)
        alone = jnp.exp2(itself - best)
        near = jnp.exp2(here - best)
        away = jnp.exp2(there - best)
        shared = 1.0 / (alone + near * stats_ref[2, block] + away * other_ref[1, block])
        alone = alone * shared
        near = near * shared
        away = away * shared
        for head in range(heads):
            rows = slice(head * HD, (head + 1) * HD)
            one = slice(head, head + 1)
            flat = (
                total_ref[head, block] * near[one]
                + part_ref[head, block].astype(jnp.float32) * away[one]
                + feats_ref[block, rows].astype(jnp.float32) * alone[one]
                + nodes_ref[rows, span].astype(jnp.float32)
                + bias[rows]
            )
            out_ref[rows, span] = jnp.where(flat > 0, flat, jnp.exp(flat) - 1.0).astype(out_ref.dtype)


def to_owners(tile_rows, tile_cols, tile_masks, blocks, devices):
    count = tile_rows.shape[0]
    capacity = max(2, 2 * count // devices)
    owners = tile_rows // blocks
    position = jnp.arange(count, dtype=jnp.int32)
    earlier = (owners[:, None] == owners[None, :]) & (position[None, :] < position[:, None])
    slots = owners * capacity + jnp.sum(earlier, axis=1)
    hits = slots[None, :] == jnp.arange(devices * capacity, dtype=jnp.int32)[:, None]
    col_owner = tile_cols // blocks
    col_level = col_owner // 4
    spot = ((col_level // 2) * 4 + col_owner % 4) * blocks + tile_cols % blocks
    parts = [tile_rows % blocks + 1, spot, col_level % 2, position]
    packed = jnp.sum(jnp.where(hits[None], jnp.stack(parts)[:, None, :], 0), axis=2)
    masks = jnp.take(tile_masks, packed[3], axis=0)
    codes = packed.reshape(4, devices, capacity).transpose(1, 0, 2)
    place = lax.axis_index("dp") * capacity
    codes = lax.dynamic_update_slice(jnp.zeros((devices, 4, LANES), jnp.int32), codes, (0, 0, place))
    return codes, masks.reshape(devices, capacity, masks.shape[1], masks.shape[2]), capacity


def local(node_feats, proj_weight, att_src, att_dst, out_bias, tile_rows, tile_cols, tile_masks):
    dims, columns = node_feats.shape
    head_dims, inputs = proj_weight.shape
    heads = head_dims // HD
    size = tile_masks.shape[2]
    words = tile_masks.shape[1]
    blocks = columns // size
    devices = lax.axis_size("dp")
    peers = lax.axis_size("mp")
    codes, masks, capacity = to_owners(tile_rows, tile_cols, tile_masks, blocks, devices)
    params = jnp.pad(jnp.stack([att_src, att_dst, out_bias]), ((0, 5), (0, -head_dims % 128)))
    depth = devices // 4
    groups = depth // 2
    origins = groups * 4
    chunks = math.gcd(blocks, max(2, 128 // devices))
    early = chunks // 2
    items = early + 1 + heads
    slots = devices * capacity
    positions = 2 * slots
    hb = blocks // 2
    whole = pl.BlockSpec(memory_space=VMEM)
    dma = pltpu.SemaphoreType.DMA
    f32 = jnp.float32
    bf16 = jnp.bfloat16
    others = max(1, peers - 1)
    feats, total, part, stats, other = pl.pallas_call(
        functools.partial(main_kernel, heads, capacity, chunks, depth, peers),
        out_shape=(
            jax.ShapeDtypeStruct((blocks, head_dims, size), bf16),
            jax.ShapeDtypeStruct((heads, blocks, HD, size), f32),
            jax.ShapeDtypeStruct((heads, blocks, HD, size), bf16),
            jax.ShapeDtypeStruct((3, blocks, heads, size), f32),
            jax.ShapeDtypeStruct((2, blocks, heads, size), f32),
        ),
        in_specs=[whole] * 5,
        out_specs=(whole,) * 5,
        scratch_shapes=[
            VMEM((origins * hb, head_dims, size), bf16),
            VMEM((origins * blocks, heads, size), f32),
            VMEM((2 * blocks, heads, size), f32),
            VMEM((chunks, inputs, columns // chunks), bf16),
            VMEM((2 * slots, words, size), jnp.int32),
            VMEM((devices, 4, LANES), jnp.int32),
            VMEM((2, 4, LANES), jnp.int32),
            VMEM((peers, 2 * heads, dims), f32),
            VMEM((peers, 2 * heads, dims), f32),
            VMEM((peers, 2 * heads, columns), f32),
            VMEM((peers, 2 * heads, columns), f32),
            VMEM((8, 2 * LANES), jnp.int32),
            pltpu.SMEM((8, 2 * LANES), jnp.int32),
            VMEM((positions, heads, size, size), bf16),
            VMEM((positions, heads, size), f32),
            VMEM((positions, heads, size), f32),
            VMEM((positions, heads, size), f32),
            VMEM((positions, heads, size), f32),
            VMEM((positions, HD, size), f32),
            VMEM((heads, blocks, HD, size), bf16),
            VMEM((2, blocks, heads, size), f32),
            dma((others, chunks)),
            dma((others, chunks)),
            dma((others,)),
            dma((others,)),
            dma((others,)),
            dma((others,)),
            dma((devices - 1,)),
            dma((devices - 1,)),
            dma((devices - 1,)),
            dma((devices - 1,)),
            dma((max(1, groups - 1), items)),
            dma((groups, items)),
            dma((groups, 2, items)),
            dma((origins, items)),
            dma((4,)),
            dma((4,)),
            dma((heads,)),
            dma((heads,)),
            dma,
        ]
        + [VMEM((origins * hb, HD, size), bf16) for _ in range(heads)],
        compiler_params=pltpu.CompilerParams(
            collective_id=0, has_side_effects=True, vmem_limit_bytes=48 * 1024 * 1024
        ),
        name="graph",
    )(proj_weight, node_feats, params, masks, codes)
    return pl.pallas_call(
        functools.partial(finish_kernel, heads),
        out_shape=jax.ShapeDtypeStruct((head_dims, columns), bf16),
        in_specs=[whole] * 7,
        out_specs=whole,
        compiler_params=pltpu.CompilerParams(vmem_limit_bytes=40 * 1024 * 1024),
        name="finish",
    )(feats, total, part, stats, other, node_feats, params)


def solution(mesh):
    return jax.shard_map(
        local,
        mesh=mesh,
        in_specs=(
            P("mp", "dp"),
            P("mp", None),
            P("mp"),
            P("mp"),
            P("mp"),
            P("dp"),
            P("dp"),
            P("dp", None, None),
        ),
        out_specs=P("mp", "dp"),
        check_vma=False,
    )
```

```python
import functools
import math

import jax
import jax.numpy as jnp
from jax import lax
from jax.experimental import pallas as pl
from jax.experimental.pallas import tpu as pltpu
from jax.sharding import PartitionSpec as P

HD = 32
LOG2E = 1.4426950408889634
FAR_BELOW = -1e30
FLOOR = -1e9
TOGETHER = 4
UNROLL = 32
VMEM = pltpu.VMEM
LANES = 128
MESH = pl.DeviceIdType.MESH


def leaky_relu(scores):
    return jnp.maximum(scores, 0.2 * scores)


def main_kernel(
    heads,
    capacity,
    chunks,
    depth,
    peers,
    weight_ref,
    nodes_ref,
    params_ref,
    masks_ref,
    codes_ref,
    feats_ref,
    total_ref,
    part_ref,
    stats_ref,
    other_ref,
    mass_ref,
    part_mass_ref,
    *scratch,
):
    (
        first_half,
        all_source,
        targ,
        all_nodes,
        masks2,
        got_codes,
        codes2,
        u_send,
        u_all,
        score_send,
        score_recv,
        table_v,
        table,
        weights,
        keeps,
        scales,
        bests,
        scan,
        part_send,
        mass_send,
        stats_send,
        node_send,
        node_recv,
        u_ss,
        u_rs,
        score_ss,
        score_rs,
        mask_ss,
        mask_rs,
        code_ss,
        code_rs,
        far_ss,
        facing_ss,
        core_ss,
        recv_sem,
        pair_ss,
        pair_rs,
        part_ss,
        part_rs,
        mass_ss,
        mass_rs,
        local_sem,
    ) = scratch[: len(scratch) - heads]
    second_half = scratch[len(scratch) - heads :]

    devices = 4 * depth
    groups = depth // 2
    me = lax.axis_index("dp")
    core = lax.rem(me, 2)
    beside = lax.rem(lax.div(me, 2), 2)
    level = lax.div(me, 4)
    parity = lax.rem(level, 2)
    where_in = lax.div(level, 2)
    mine = lax.axis_index("mp")
    dims, columns = nodes_ref.shape
    head_dims = weight_ref.shape[0]
    size = LANES
    blocks = columns // size
    hb = blocks // 2
    per = blocks // chunks
    width = per * size
    slots = devices * capacity
    early = chunks // 2
    score_item = early
    items = early + 1 + heads

    def place(lev, b, c):
        return (lev * 2 + b) * 2 + c

    def origin_of(q, b, c):
        return (q * 2 + b) * 2 + c

    own = origin_of(where_in, beside, core)
    facing = place(level, 1 - beside, core)
    other_core = place(level, beside, 1 - core)
    pair = place(level + 1 - 2 * parity, beside, core)

    barrier = pltpu.get_barrier_semaphore()
    for shift in range(1, devices):
        pl.semaphore_signal(barrier, 1, device_id={"dp": lax.rem(me + shift, devices)}, device_id_type=MESH)
    for shift in range(1, peers):
        pl.semaphore_signal(barrier, 1, device_id={"mp": lax.rem(mine + shift, peers)}, device_id_type=MESH)

    own_rows = pl.ds(pl.multiple_of(mine * dims, dims), dims)
    for chunk in range(chunks):
        all_nodes[chunk, own_rows, :] = nodes_ref[:, chunk * width : (chunk + 1) * width]
    masks2[pl.ds(me * capacity, capacity)] = masks_ref[me]
    got_codes[me] = codes_ref[me]
    params = jnp.transpose(params_ref[...])[:head_dims]
    wide = weight_ref[...].astype(jnp.float32)
    by_source = wide * (LOG2E * params[:, 0:1])
    by_target = wide * (LOG2E * params[:, 1:2])
    rows = []
    for scaled in (by_source, by_target):
        for head in range(heads):
            rows.append(jnp.sum(scaled[head * HD : (head + 1) * HD], axis=0, keepdims=True))
    reduced = jnp.concatenate(rows, axis=0)
    for peer in range(peers):
        u_send[peer] = reduced[:, peer * dims : (peer + 1) * dims]
    u_all[mine] = u_send[mine]
    pl.semaphore_wait(barrier, devices - 1 + peers - 1)

    def node_copy(shift, chunk):
        return pltpu.make_async_remote_copy(
            src_ref=nodes_ref.at[:, pl.ds(chunk * width, width)],
            dst_ref=all_nodes.at[chunk, own_rows, :],
            send_sem=node_send.at[shift - 1, chunk],
            recv_sem=node_recv.at[shift - 1, chunk],
            device_id={"mp": lax.rem(mine + shift, peers)},
            device_id_type=MESH,
        )

    def u_copy(shift):
        to = lax.rem(mine + shift, peers)
        return pltpu.make_async_remote_copy(
            src_ref=u_send.at[to],
            dst_ref=u_all.at[mine],
            send_sem=u_ss.at[shift - 1],
            recv_sem=u_rs.at[shift - 1],
            device_id={"mp": to},
            device_id_type=MESH,
        )

    def score_copy(shift):
        to = lax.rem(mine + shift, peers)
        return pltpu.make_async_remote_copy(
            src_ref=score_send.at[to],
            dst_ref=score_recv.at[mine],
            send_sem=score_ss.at[shift - 1],
            recv_sem=score_rs.at[shift - 1],
            device_id={"mp": to},
            device_id_type=MESH,
        )

    def mask_copy(shift):
        to = lax.rem(me + shift, devices)
        return pltpu.make_async_remote_copy(
            src_ref=masks_ref.at[to],
            dst_ref=masks2.at[pl.ds(me * capacity, capacity)],
            send_sem=mask_ss.at[shift - 1],
            recv_sem=mask_rs.at[shift - 1],
            device_id={"dp": to},
            device_id_type=MESH,
        )

    def code_copy(shift):
        to = lax.rem(me + shift, devices)
        return pltpu.make_async_remote_copy(
            src_ref=codes_ref.at[to],
            dst_ref=got_codes.at[me],
            send_sem=code_ss.at[shift - 1],
            recv_sem=code_rs.at[shift - 1],
            device_id={"dp": to},
            device_id_type=MESH,
        )

    def pair_copy(which):
        src, dst = (
            (masks2.at[pl.ds(0, slots)], masks2.at[pl.ds(slots, slots)]),
            (codes2.at[0], codes2.at[1]),
            (targ.at[pl.ds(blocks, blocks)], targ.at[pl.ds(0, blocks)]),
            (stats_send, other_ref),
        )[which]
        return pltpu.make_async_remote_copy(
            src_ref=src,
            dst_ref=dst,
            send_sem=pair_ss.at[which],
            recv_sem=pair_rs.at[which],
            device_id={"dp": pair},
            device_id_type=MESH,
        )

    def part_copy(head):
        return pltpu.make_async_remote_copy(
            src_ref=part_send.at[head],
            dst_ref=part_ref.at[head],
            send_sem=part_ss.at[head],
            recv_sem=part_rs.at[head],
            device_id={"dp": pair},
            device_id_type=MESH,
        )

    def mass_copy(head):
        return pltpu.make_async_remote_copy(
            src_ref=mass_send.at[head],
            dst_ref=part_mass_ref.at[head],
            send_sem=mass_ss.at[head],
            recv_sem=mass_rs.at[head],
            device_id={"dp": pair},
            device_id_type=MESH,
        )

    def item_ref(origin, item):
        if item < early:
            return first_half.at[pl.ds(origin * hb + item * per, per)]
        if item == score_item:
            return all_source.at[pl.ds(origin * blocks, blocks)]
        return second_half[item - score_item - 1].at[pl.ds(origin * hb, hb)]

    def send(origin, item, to, sem):
        part = item_ref(origin, item)
        return pltpu.make_async_remote_copy(
            src_ref=part,
            dst_ref=part,
            send_sem=sem,
            recv_sem=recv_sem.at[origin, item],
            device_id={"dp": to},
            device_id_type=MESH,
        )

    def far_copy(shift, item):
        to = place(2 * lax.rem(where_in + shift, groups) + parity, beside, core)
        return send(own, item, to, far_ss.at[shift - 1, item])

    def facing_copy(q, item):
        return send(origin_of(q, beside, core), item, facing, facing_ss.at[q, item])

    def core_copy(q, b, item):
        return send(origin_of(q, b, core), item, other_core, core_ss.at[q, b, item])

    def arrival(origin, item):
        send(origin, item, other_core, core_ss.at[0, 0, item]).wait_recv()

    def own_core(item):
        core_copy(where_in, beside, item).start()

    def own_far(item):
        for shift in range(1, groups):
            far_copy(shift, item).start()

    at_end = (level == 0) | (level == depth - 1)

    def far_if_end(item):
        pl.when(at_end)(lambda: own_far(item))

    def far_if_middle(item):
        pl.when(jnp.logical_not(at_end))(lambda: own_far(item))

    def own_facing(item):
        facing_copy(where_in, item).start()

    def own_out(item):
        own_far(item)
        own_near(item)

    def own_near(item):
        own_facing(item)
        own_core(item)

    def far_q(shift):
        return lax.rem(where_in + groups - shift, groups)

    def from_far(item):
        for shift in range(1, groups):
            q = far_q(shift)
            arrival(origin_of(q, beside, core), item)
            facing_copy(q, item).start()
            core_copy(q, beside, item).start()

    def from_facing(item):
        arrival(origin_of(where_in, 1 - beside, core), item)
        core_copy(where_in, 1 - beside, item).start()

    def from_facing_far(item):
        for shift in range(1, groups):
            q = far_q(shift)
            arrival(origin_of(q, 1 - beside, core), item)
            core_copy(q, 1 - beside, item).start()

    def from_core(item):
        for q in range(groups):
            for b in range(2):
                arrival(origin_of(q, b, 1 - core), item)

    def project(chunk):
        for shift in range(1, peers):
            node_copy(shift, chunk).wait_recv()
        projected = jnp.dot(weight_ref[...], all_nodes[chunk], preferred_element_type=jnp.float32)
        rounded = projected.astype(jnp.bfloat16)
        for j in range(per):
            block = chunk * per + j
            span = slice(j * size, (j + 1) * size)
            feats_ref[block] = rounded[:, span]
            if chunk < early:
                first_half[own * hb + block] = rounded[:, span]
            else:
                for head in range(heads):
                    second_half[head][own * hb + block - hb] = rounded[head * HD : (head + 1) * HD, span]

    for shift in range(1, peers):
        u_copy(shift).start()
    for shift in range(1, peers):
        node_copy(shift, 0).start()
    for shift in range(1, devices):
        code_copy(shift).start()
        mask_copy(shift).start()

    for shift in range(1, peers):
        u_copy(shift).wait_recv()
    stacked = jnp.concatenate([u_all[peer] for peer in range(peers)], axis=0)
    high = stacked.astype(jnp.bfloat16)
    rest = stacked - high.astype(jnp.float32)
    middle = rest.astype(jnp.bfloat16)
    low = (rest - middle.astype(jnp.float32)).astype(jnp.bfloat16)
    pieces = jnp.concatenate([high, middle, low], axis=0)
    count = 2 * heads * peers
    scored = jnp.dot(pieces, nodes_ref[...], preferred_element_type=jnp.float32)
    scored = scored[:count] + scored[count : 2 * count] + scored[2 * count :]
    for peer in range(peers):
        score_send[peer] = scored[peer * 2 * heads : (peer + 1) * 2 * heads]
    score_recv[mine] = score_send[mine]
    for shift in range(1, peers):
        score_copy(shift).start()
    for chunk in range(1, chunks):
        for shift in range(1, peers):
            node_copy(shift, chunk).start()

    project(0)
    for shift in range(1, peers):
        score_copy(shift).wait_recv()
    scores = score_recv[0]
    for peer in range(1, peers):
        scores = scores + score_recv[peer]
    for block in range(blocks):
        span = slice(block * size, (block + 1) * size)
        source = scores[:heads, span]
        target = scores[heads:, span]
        all_source[own * blocks + block] = source
        targ[blocks + block] = target
        stats_ref[0, block] = leaky_relu(source + target)
    own_out(score_item)
    own_out(0)
    pair_copy(2).start()

    def tables():
        for shift in range(1, devices):
            code_copy(shift).wait_recv()
        gathered = got_codes[0]
        for device in range(1, devices):
            gathered = gathered + got_codes[device]
        codes2[0] = gathered
        pair_copy(1).start()
        for shift in range(1, devices):
            mask_copy(shift).wait_recv()
        pair_copy(0).start()

    def order():
        pair_copy(1).wait_recv()
        for which, codes in enumerate((codes2[1], codes2[0])):
            row, column, spot = codes[0:1], codes[1:2], codes[3:4]
            column_parity = jnp.bitwise_and(codes[2:3], 1)
            late = jnp.right_shift(codes[2:3], 1)
            lanes = row.shape[1]
            key = jnp.where((row > 0) & (column_parity == parity), row - 1, blocks)
            turned = jnp.transpose(jnp.concatenate([key, column, spot, late] + [key] * 4, axis=0))
            key_t = turned[:, 0:1]
            column_t = turned[:, 1:2]
            spot_t = turned[:, 2:3]
            late_t = turned[:, 3:4]
            along = lax.broadcasted_iota(jnp.int32, (lanes, lanes), 1)
            down = lax.broadcasted_iota(jnp.int32, (lanes, lanes), 0)
            before = (key_t < key) | ((key_t == key) & (down < along))
            rank = jnp.sum(jnp.where(before, 1, 0), axis=0, keepdims=True)
            rank_t = jnp.transpose(jnp.concatenate([rank] * 8, axis=0))[:, 0:1]
            at = rank_t == along
            slot = jnp.sum(jnp.where(at, down, 0), axis=0, keepdims=True)
            table_v[which, 0:1] = (1 - which) * slots + jnp.minimum(slot, slots - 1)
            table_v[which, 1:2] = jnp.sum(jnp.where(at, key_t, 0), axis=0, keepdims=True)
            table_v[which, 2:3] = jnp.sum(jnp.where(at, column_t, 0), axis=0, keepdims=True)
            table_v[which, 3:4] = jnp.sum(jnp.where(key_t <= along, 1, 0), axis=0, keepdims=True)
            table_v[which, 4:5] = jnp.sum(jnp.where(at, spot_t, 0), axis=0, keepdims=True)
            table_v[which, 5:6] = jnp.sum(jnp.where(at, late_t, 0), axis=0, keepdims=True)
            table_v[which, 6:8] = jnp.zeros((2, lanes), jnp.int32)
        table_copy().start()

    def table_copy():
        return pltpu.make_async_copy(table_v, table, local_sem)

    words = size // 32
    to_sign = 31 - lax.broadcasted_iota(jnp.int32, (32, size), 0)

    def partial(which, k):
        slot = table[which, 0, k]
        key = table[which, 1, k]
        column = table[which, 2, k]
        packed = masks2[slot] * jnp.where(key < blocks, 1, 0)
        edges = jnp.concatenate(
            [
                jnp.left_shift(packed[word : word + 1, :], to_sign)
                for word in range(words)
            ],
            axis=0,
        ) < 0
        source = all_source[column]
        source = jnp.transpose(jnp.concatenate([source] * (8 // heads), axis=0))
        target = targ[which * blocks + jnp.minimum(key, blocks - 1)]
        peaks = []
        for head in range(heads):
            one = slice(head, head + 1)
            here = jnp.where(edges, source[:, one], FAR_BELOW)
            aim = target[one]
            peak = leaky_relu(aim + jnp.max(here, axis=0, keepdims=True))
            peak = jnp.maximum(peak, FLOOR)
            weight = jnp.exp2(leaky_relu(here + aim) - peak)
            peaks.append(peak)
            weights[which * slots + k, head] = weight.astype(jnp.bfloat16)
        same = (k > 0) & (key == table[which, 1, jnp.maximum(k - 1, 0)])
        return same, jnp.concatenate(peaks, axis=0)

    together = math.gcd(slots, TOGETHER)
    turns = math.gcd(slots, 4) // together
    steps = slots // (together * turns)

    def weigh(which, index, run):
        parts = [(index * together + w, partial(which, index * together + w)) for w in range(together)]
        for k, (same, peak) in parts:
            again = jnp.where(same, 1.0, 0.0)
            old = jnp.where(same, run, FLOOR)
            run = jnp.maximum(old, peak)
            spot = which * slots + k
            keeps[spot] = jnp.exp2(old - run) * again
            scales[spot] = jnp.exp2(peak - run)
            bests[spot] = run
        return run

    def fresh():
        return jnp.full((heads, size), FLOOR, jnp.float32)

    ones = jnp.ones((16, size), jnp.bfloat16)

    def multiply(which, head, first, unroll, total):
        rows = slice(head * HD, (head + 1) * HD)
        one = slice(head, head + 1)
        values = []
        for w in range(unroll):
            spot = table[which, 4, first + w]
            late = table[which, 5, first + w]
            feats = jnp.where(late == 0, first_half[spot, rows], second_half[head][spot])
            feats = jnp.concatenate([feats, ones], axis=0)
            values.append(
                jnp.dot(feats, weights[which * slots + first + w, head], preferred_element_type=jnp.float32)
            )
        for w in range(unroll):
            spot = which * slots + first + w
            total = total * keeps[spot, one] + values[w][: HD + 8] * scales[spot, one]
            scan[first + w] = total
        return total

    def ending(which, key):
        upto = table[which, 3, key]
        prior = table[which, 3, key - 1] if key > 0 else 0
        return jnp.maximum(upto - 1, 0), upto > prior

    def play(events):
        for what, item in events:
            what(item)

    first = score_item + 1
    standard = early == 4 and heads == 4 and chunks == 8 and steps == 16

    def near_weights(count, state):
        at, carry = state
        body = functools.partial(weigh, 0)
        return at + count, lax.fori_loop(at * turns, (at + count) * turns, body, carry)

    def own_weights(count, state):
        at, carry = state
        body = functools.partial(weigh, 1)
        return at + count, lax.fori_loop(at * turns, (at + count) * turns, body, carry)

    def near_values(head):
        from_core(first + head)

        def body(index, total):
            return multiply(0, head, index * unroll, unroll, total)

        lax.fori_loop(0, slots // unroll, body, jnp.zeros((HD + 8, size), jnp.float32))
        for block in range(blocks):
            index, some = ending(0, block)
            found = jnp.where(some, scan[index], 0.0)
            part_send[head, block] = found[:HD].astype(jnp.bfloat16)
            mass_send[head, block : block + 1] = found[HD : HD + 1]
        part_copy(head).start()
        mass_copy(head).start()

    def own_values(head):
        def body(index, total):
            return multiply(1, head, index * unroll, unroll, total)

        lax.fori_loop(0, slots // unroll, body, jnp.zeros((HD + 8, size), jnp.float32))
        for block in range(blocks):
            index, some = ending(1, block)
            found = jnp.where(some, scan[index], 0.0)
            total_ref[head, block] = found[:HD]
            mass_ref[head, block : block + 1] = found[HD : HD + 1]

    def near_stats():
        for block in range(blocks):
            index, some = ending(0, block)
            stats_send[block] = jnp.where(some, bests[index], FLOOR)
        pair_copy(3).start()

    def ready_to_weigh():
        table_copy().wait()
        from_core(score_item)
        pair_copy(2).wait_recv()
        pair_copy(0).wait_recv()

    unroll = math.gcd(slots, UNROLL)
    near = (0, fresh())
    mine_state = (0, fresh())
    if standard:
        project(1)
        far_if_middle(1)
        own_near(1)
        tables()
        project(2)
        from_facing(score_item)
        far_if_middle(2)
        far_if_end(1)
        own_near(2)
        order()
        from_far(score_item)
        project(3)
        far_if_middle(3)
        far_if_end(2)
        own_near(3)
        project(4)
        from_facing_far(score_item)
        project(5)
        from_far(0)
        far_if_end(3)
        project(6)
        project(7)
        for head in range(heads):
            far_if_middle(first + head)
            own_core(first + head)
        own_facing(first)
        ready_to_weigh()
        near = near_weights(2, near)
        play([(far_if_end, first), (from_far, 1), (own_facing, first + 1)])
        near = near_weights(4, near)
        play([(far_if_end, first + 1), (from_far, 2)])
        near = near_weights(4, near)
        play([(far_if_end, first + 2), (own_facing, first + 2)])
        near = near_weights(3, near)
        play([(from_far, 3), (own_facing, first + 3)])
        near = near_weights(3, near)
        play([(far_if_end, first + 3)])
        near_stats()
        play([(from_far, first)])
        mine_state = own_weights(3, mine_state)
        play([(from_facing, 0), (from_facing, 1), (from_facing, 2), (from_facing, 3), (from_facing, first)])
        mine_state = own_weights(1, mine_state)
        play([(from_far, first + 1), (from_facing_far, 0), (from_facing_far, 1), (from_facing_far, 2)])
        mine_state = own_weights(3, mine_state)
        play([(from_facing_far, 3), (from_far, first + 2), (from_facing_far, first), (from_facing, first + 1)])
        mine_state = own_weights(2, mine_state)
        for item in range(early):
            from_core(item)
        near_values(0)
        play([(from_facing_far, first + 1), (from_facing, first + 2), (from_far, first + 3)])
        mine_state = own_weights(3, mine_state)
        near_values(1)
        play([(from_facing_far, first + 2), (from_facing, first + 3)])
        mine_state = own_weights(2, mine_state)
        near_values(2)
        play([(from_facing_far, first + 3)])
        mine_state = own_weights(2, mine_state)
        near_values(3)
        for head in range(heads):
            own_values(head)
    else:
        for chunk in range(1, chunks):
            project(chunk)
            if chunk < early:
                own_out(chunk)
        tables()
        order()
        for head in range(heads):
            own_out(first + head)
        for item in [score_item] + [i for i in range(items) if i != score_item]:
            play([(from_facing, item), (from_far, item), (from_facing_far, item)])
        ready_to_weigh()
        near = near_weights(steps, near)
        near_stats()
        mine_state = own_weights(steps, mine_state)
        for item in range(early):
            from_core(item)
        for head in range(heads):
            near_values(head)
            own_values(head)

    for block in range(blocks):
        index, some = ending(1, block)
        stats_ref[1, block] = jnp.where(some, bests[slots + index], FLOOR)
    for shift in range(1, peers):
        u_copy(shift).wait_send()
        score_copy(shift).wait_send()
        for chunk in range(chunks):
            node_copy(shift, chunk).wait_send()
    for shift in range(1, devices):
        code_copy(shift).wait_send()
        mask_copy(shift).wait_send()
    for item in range(items):
        for shift in range(1, groups):
            far_copy(shift, item).wait_send()
        for q in range(groups):
            facing_copy(q, item).wait_send()
            for b in range(2):
                core_copy(q, b, item).wait_send()
    for which in range(4):
        pair_copy(which).wait_send()
    pair_copy(3).wait_recv()
    for head in range(heads):
        part_copy(head).wait()
        mass_copy(head).wait()


def finish_kernel(
    heads,
    feats_ref,
    total_ref,
    part_ref,
    stats_ref,
    other_ref,
    mass_ref,
    part_mass_ref,
    nodes_ref,
    params_ref,
    out_ref,
):
    blocks = feats_ref.shape[0]
    size = LANES
    bias = jnp.transpose(params_ref[...])[:, 2:3]
    for block in range(blocks):
        span = slice(block * size, (block + 1) * size)
        itself = stats_ref[0, block]
        here = stats_ref[1, block]
        there = other_ref[block]
        mass = jnp.concatenate([mass_ref[head, block : block + 1] for head in range(heads)], axis=0)
        part_mass = jnp.concatenate([part_mass_ref[head, block : block + 1] for head in range(heads)], axis=0)
        best = jnp.maximum(jnp.maximum(itself, here), there)
        alone = jnp.exp2(itself - best)
        near = jnp.exp2(here - best)
        away = jnp.exp2(there - best)
        shared = 1.0 / (alone + near * mass + away * part_mass)
        alone = alone * shared
        near = near * shared
        away = away * shared
        for head in range(heads):
            rows = slice(head * HD, (head + 1) * HD)
            one = slice(head, head + 1)
            flat = (
                total_ref[head, block] * near[one]
                + part_ref[head, block].astype(jnp.float32) * away[one]
                + feats_ref[block, rows].astype(jnp.float32) * alone[one]
                + nodes_ref[rows, span].astype(jnp.float32)
                + bias[rows]
            )
            out_ref[rows, span] = jnp.where(flat > 0, flat, jnp.exp(flat) - 1.0).astype(out_ref.dtype)


def to_owners(tile_rows, tile_cols, tile_masks, blocks, devices):
    count = tile_rows.shape[0]
    capacity = max(2, 2 * count // devices)
    owners = tile_rows // blocks
    position = jnp.arange(count, dtype=jnp.int32)
    earlier = (owners[:, None] == owners[None, :]) & (position[None, :] < position[:, None])
    slots = owners * capacity + jnp.sum(earlier, axis=1)
    hits = slots[None, :] == jnp.arange(devices * capacity, dtype=jnp.int32)[:, None]
    col_owner = tile_cols // blocks
    col_level = col_owner // 4
    col_group = (col_level // 2) * 4 + col_owner % 4
    col_block = tile_cols % blocks
    hb = blocks // 2
    parts = [
        tile_rows % blocks + 1,
        col_group * blocks + col_block,
        col_level % 2 + 2 * (col_block // hb),
        col_group * hb + col_block % hb,
        position,
    ]
    packed = jnp.sum(jnp.where(hits[None], jnp.stack(parts)[:, None, :], 0), axis=2)
    masks = jnp.take(tile_masks, packed[4], axis=0)
    codes = packed[:4].reshape(4, devices, capacity).transpose(1, 0, 2)
    codes = jnp.tile(codes, (1, 1, LANES // capacity))
    lane = jnp.arange(LANES, dtype=jnp.int32)
    codes = jnp.where(lane // capacity == lax.axis_index("dp"), codes, 0)
    return codes, masks.reshape(devices, capacity, masks.shape[1], masks.shape[2]), capacity


def local(node_feats, proj_weight, att_src, att_dst, out_bias, tile_rows, tile_cols, tile_masks):
    dims, columns = node_feats.shape
    head_dims, inputs = proj_weight.shape
    heads = head_dims // HD
    size = tile_masks.shape[2]
    words = tile_masks.shape[1]
    blocks = columns // size
    devices = lax.axis_size("dp")
    peers = lax.axis_size("mp")
    codes, masks, capacity = to_owners(tile_rows, tile_cols, tile_masks, blocks, devices)
    params = jnp.pad(jnp.stack([att_src, att_dst, out_bias]), ((0, 5), (0, -head_dims % 128)))
    depth = devices // 4
    groups = depth // 2
    origins = groups * 4
    chunks = math.gcd(blocks, max(2, 128 // devices))
    early = chunks // 2
    items = early + 1 + heads
    slots = devices * capacity
    positions = 2 * slots
    hb = blocks // 2
    whole = pl.BlockSpec(memory_space=VMEM)
    dma = pltpu.SemaphoreType.DMA
    f32 = jnp.float32
    bf16 = jnp.bfloat16
    others = max(1, peers - 1)
    feats, total, part, stats, other, mass, part_mass = pl.pallas_call(
        functools.partial(main_kernel, heads, capacity, chunks, depth, peers),
        out_shape=(
            jax.ShapeDtypeStruct((blocks, head_dims, size), bf16),
            jax.ShapeDtypeStruct((heads, blocks, HD, size), f32),
            jax.ShapeDtypeStruct((heads, blocks, HD, size), bf16),
            jax.ShapeDtypeStruct((2, blocks, heads, size), f32),
            jax.ShapeDtypeStruct((blocks, heads, size), f32),
            jax.ShapeDtypeStruct((heads, blocks, size), f32),
            jax.ShapeDtypeStruct((heads, blocks, size), f32),
        ),
        in_specs=[whole] * 5,
        out_specs=(whole,) * 7,
        scratch_shapes=[
            VMEM((origins * hb, head_dims, size), bf16),
            VMEM((origins * blocks, heads, size), f32),
            VMEM((2 * blocks, heads, size), f32),
            VMEM((chunks, inputs, columns // chunks), bf16),
            VMEM((2 * slots, words, size), jnp.int32),
            VMEM((devices, 4, LANES), jnp.int32),
            VMEM((2, 4, LANES), jnp.int32),
            VMEM((peers, 2 * heads, dims), f32),
            VMEM((peers, 2 * heads, dims), f32),
            VMEM((peers, 2 * heads, columns), f32),
            VMEM((peers, 2 * heads, columns), f32),
            VMEM((2, 8, LANES), jnp.int32),
            pltpu.SMEM((2, 8, LANES), jnp.int32),
            VMEM((positions, heads, size, size), bf16),
            VMEM((positions, heads, size), f32),
            VMEM((positions, heads, size), f32),
            VMEM((positions, heads, size), f32),
            VMEM((slots, HD + 8, size), f32),
            VMEM((heads, blocks, HD, size), bf16),
            VMEM((heads, blocks, size), f32),
            VMEM((blocks, heads, size), f32),
            dma((others, chunks)),
            dma((others, chunks)),
            dma((others,)),
            dma((others,)),
            dma((others,)),
            dma((others,)),
            dma((devices - 1,)),
            dma((devices - 1,)),
            dma((devices - 1,)),
            dma((devices - 1,)),
            dma((max(1, groups - 1), items)),
            dma((groups, items)),
            dma((groups, 2, items)),
            dma((origins, items)),
            dma((4,)),
            dma((4,)),
            dma((heads,)),
            dma((heads,)),
            dma((heads,)),
            dma((heads,)),
            dma,
        ]
        + [VMEM((origins * hb, HD, size), bf16) for _ in range(heads)],
        compiler_params=pltpu.CompilerParams(
            collective_id=0, has_side_effects=True, vmem_limit_bytes=48 * 1024 * 1024
        ),
        name="graph",
    )(proj_weight, node_feats, params, masks, codes)
    return pl.pallas_call(
        functools.partial(finish_kernel, heads),
        out_shape=jax.ShapeDtypeStruct((head_dims, columns), bf16),
        in_specs=[whole] * 9,
        out_specs=whole,
        compiler_params=pltpu.CompilerParams(vmem_limit_bytes=40 * 1024 * 1024),
        name="finish",
    )(feats, total, part, stats, other, mass, part_mass, node_feats, params)


def solution(mesh):
    return jax.shard_map(
        local,
        mesh=mesh,
        in_specs=(
            P("mp", "dp"),
            P("mp", None),
            P("mp"),
            P("mp"),
            P("mp"),
            P("dp"),
            P("dp"),
            P("dp", None, None),
        ),
        out_specs=P("mp", "dp"),
        check_vma=False,
    )
```

```python
import functools
import math

import jax
import jax.numpy as jnp
from jax import lax
from jax.experimental import pallas as pl
from jax.experimental.pallas import tpu as pltpu
from jax.sharding import PartitionSpec as P

HD = 32
LOG2E = 1.4426950408889634
FAR_BELOW = -1e30
FLOOR = -1e9
TOGETHER = 4
UNROLL = 32
VMEM = pltpu.VMEM
LANES = 128
MESH = pl.DeviceIdType.MESH


def leaky_relu(scores):
    return jnp.maximum(scores, 0.2 * scores)


def main_kernel(
    heads,
    capacity,
    chunks,
    depth,
    peers,
    weight_ref,
    nodes_ref,
    att_src_ref,
    att_dst_ref,
    tiles_ref,
    tile_rows,
    tile_cols,
    feats_ref,
    total_ref,
    part_ref,
    stats_ref,
    other_ref,
    mass_ref,
    part_mass_ref,
    *scratch,
):
    (
        first_half,
        all_source,
        targ,
        all_nodes,
        masks_out,
        masks2,
        code_rows,
        codes_out,
        pick,
        got_codes,
        u_send,
        u_all,
        score_send,
        score_recv,
        table_v,
        table,
        weights,
        keeps,
        scales,
        bests,
        scan,
        part_send,
        mass_send,
        stats_send,
        node_send,
        node_recv,
        u_ss,
        u_rs,
        score_ss,
        score_rs,
        mask_ss,
        mask_rs,
        code_ss,
        code_rs,
        far_ss,
        facing_ss,
        core_ss,
        recv_sem,
        pair_ss,
        pair_rs,
        part_ss,
        part_rs,
        mass_ss,
        mass_rs,
        local_sem,
        pick_sem,
    ) = scratch[: len(scratch) - heads]
    second_half = scratch[len(scratch) - heads :]

    devices = 4 * depth
    groups = depth // 2
    me = lax.axis_index("dp")
    core = lax.rem(me, 2)
    beside = lax.rem(lax.div(me, 2), 2)
    level = lax.div(me, 4)
    parity = lax.rem(level, 2)
    where_in = lax.div(level, 2)
    mine = lax.axis_index("mp")
    dims, columns = nodes_ref.shape
    head_dims = weight_ref.shape[0]
    size = LANES
    blocks = columns // size
    hb = blocks // 2
    per = blocks // chunks
    width = per * size
    slots = devices * capacity
    early = chunks // 2
    score_item = early
    items = early + 1 + heads

    def place(lev, b, c):
        return (lev * 2 + b) * 2 + c

    def origin_of(q, b, c):
        return (q * 2 + b) * 2 + c

    own = origin_of(where_in, beside, core)
    facing = place(level, 1 - beside, core)
    other_core = place(level, beside, 1 - core)
    pair = place(level + 1 - 2 * parity, beside, core)

    barrier = pltpu.get_barrier_semaphore()
    for shift in range(1, devices):
        pl.semaphore_signal(barrier, 1, device_id={"dp": lax.rem(me + shift, devices)}, device_id_type=MESH)
    for shift in range(1, peers):
        pl.semaphore_signal(barrier, 1, device_id={"mp": lax.rem(mine + shift, peers)}, device_id_type=MESH)

    own_rows = pl.ds(pl.multiple_of(mine * dims, dims), dims)

    def as_column(ref):
        row = ref[...]
        if head_dims < LANES:
            row = jnp.concatenate([row, jnp.zeros((1, LANES - head_dims), row.dtype)], axis=1)
        return jnp.transpose(jnp.concatenate([row] * 8, axis=0))[:head_dims, 0:1]

    wide = weight_ref[...].astype(jnp.float32)
    by_source = wide * (LOG2E * as_column(att_src_ref))
    by_target = wide * (LOG2E * as_column(att_dst_ref))
    rows = []
    for scaled in (by_source, by_target):
        for head in range(heads):
            rows.append(jnp.sum(scaled[head * HD : (head + 1) * HD], axis=0, keepdims=True))
    reduced = jnp.concatenate(rows, axis=0)
    for peer in range(peers):
        u_send[peer] = reduced[:, peer * dims : (peer + 1) * dims]
    u_all[mine] = u_send[mine]
    pl.semaphore_wait(barrier, devices - 1 + peers - 1)

    def node_copy(shift, chunk):
        return pltpu.make_async_remote_copy(
            src_ref=nodes_ref.at[:, pl.ds(chunk * width, width)],
            dst_ref=all_nodes.at[chunk, own_rows, :],
            send_sem=node_send.at[shift - 1, chunk],
            recv_sem=node_recv.at[shift - 1, chunk],
            device_id={"mp": lax.rem(mine + shift, peers)},
            device_id_type=MESH,
        )

    def u_copy(shift):
        to = lax.rem(mine + shift, peers)
        return pltpu.make_async_remote_copy(
            src_ref=u_send.at[to],
            dst_ref=u_all.at[mine],
            send_sem=u_ss.at[shift - 1],
            recv_sem=u_rs.at[shift - 1],
            device_id={"mp": to},
            device_id_type=MESH,
        )

    def score_copy(shift):
        to = lax.rem(mine + shift, peers)
        return pltpu.make_async_remote_copy(
            src_ref=score_send.at[to],
            dst_ref=score_recv.at[mine],
            send_sem=score_ss.at[shift - 1],
            recv_sem=score_rs.at[shift - 1],
            device_id={"mp": to},
            device_id_type=MESH,
        )

    def mask_copy(shift):
        to = lax.rem(me + shift, devices)
        return pltpu.make_async_remote_copy(
            src_ref=masks_out.at[pl.ds(to * capacity, capacity)],
            dst_ref=masks2.at[pl.ds(me * capacity, capacity)],
            send_sem=mask_ss.at[shift - 1],
            recv_sem=mask_rs.at[shift - 1],
            device_id={"dp": to},
            device_id_type=MESH,
        )

    def code_copy(shift):
        to = lax.rem(me + shift, devices)
        return pltpu.make_async_remote_copy(
            src_ref=codes_out,
            dst_ref=got_codes.at[me],
            send_sem=code_ss.at[shift - 1],
            recv_sem=code_rs.at[shift - 1],
            device_id={"dp": to},
            device_id_type=MESH,
        )

    def pair_copy(which):
        src, dst = (
            (masks2.at[pl.ds(0, slots)], masks2.at[pl.ds(slots, slots)]),
            (targ.at[pl.ds(blocks, blocks)], targ.at[pl.ds(0, blocks)]),
            (stats_send, other_ref),
        )[which]
        return pltpu.make_async_remote_copy(
            src_ref=src,
            dst_ref=dst,
            send_sem=pair_ss.at[which],
            recv_sem=pair_rs.at[which],
            device_id={"dp": pair},
            device_id_type=MESH,
        )

    def part_copy(head):
        return pltpu.make_async_remote_copy(
            src_ref=part_send.at[head],
            dst_ref=part_ref.at[head],
            send_sem=part_ss.at[head],
            recv_sem=part_rs.at[head],
            device_id={"dp": pair},
            device_id_type=MESH,
        )

    def mass_copy(head):
        return pltpu.make_async_remote_copy(
            src_ref=mass_send.at[head],
            dst_ref=part_mass_ref.at[head],
            send_sem=mass_ss.at[head],
            recv_sem=mass_rs.at[head],
            device_id={"dp": pair},
            device_id_type=MESH,
        )

    def item_ref(origin, item):
        if item < early:
            return first_half.at[pl.ds(origin * hb + item * per, per)]
        if item == score_item:
            return all_source.at[pl.ds(origin * blocks, blocks)]
        return second_half[item - score_item - 1].at[pl.ds(origin * hb, hb)]

    def send(origin, item, to, sem):
        part = item_ref(origin, item)
        return pltpu.make_async_remote_copy(
            src_ref=part,
            dst_ref=part,
            send_sem=sem,
            recv_sem=recv_sem.at[origin, item],
            device_id={"dp": to},
            device_id_type=MESH,
        )

    def far_copy(shift, item):
        to = place(2 * lax.rem(where_in + shift, groups) + parity, beside, core)
        return send(own, item, to, far_ss.at[shift - 1, item])

    def facing_copy(q, item):
        return send(origin_of(q, beside, core), item, facing, facing_ss.at[q, item])

    def core_copy(q, b, item):
        return send(origin_of(q, b, core), item, other_core, core_ss.at[q, b, item])

    def arrival(origin, item):
        send(origin, item, other_core, core_ss.at[0, 0, item]).wait_recv()

    def own_core(item):
        core_copy(where_in, beside, item).start()

    def own_far(item):
        for shift in range(1, groups):
            far_copy(shift, item).start()

    at_end = (level == 0) | (level == depth - 1)

    def far_if_end(item):
        pl.when(at_end)(lambda: own_far(item))

    def far_if_middle(item):
        pl.when(jnp.logical_not(at_end))(lambda: own_far(item))

    def own_facing(item):
        facing_copy(where_in, item).start()

    def own_out(item):
        own_far(item)
        own_near(item)

    def own_near(item):
        own_facing(item)
        own_core(item)

    def far_q(shift):
        return lax.rem(where_in + groups - shift, groups)

    def from_far(item):
        for shift in range(1, groups):
            q = far_q(shift)
            arrival(origin_of(q, beside, core), item)
            facing_copy(q, item).start()
            core_copy(q, beside, item).start()

    def from_facing(item):
        arrival(origin_of(where_in, 1 - beside, core), item)
        core_copy(where_in, 1 - beside, item).start()

    def from_facing_far(item):
        for shift in range(1, groups):
            q = far_q(shift)
            arrival(origin_of(q, 1 - beside, core), item)
            core_copy(q, 1 - beside, item).start()

    def from_core(item):
        for q in range(groups):
            for b in range(2):
                arrival(origin_of(q, b, 1 - core), item)

    def project(chunk):
        for shift in range(1, peers):
            node_copy(shift, chunk).wait_recv()
        projected = jnp.dot(weight_ref[...], all_nodes[chunk], preferred_element_type=jnp.float32)
        rounded = projected.astype(jnp.bfloat16)
        for j in range(per):
            block = chunk * per + j
            span = slice(j * size, (j + 1) * size)
            feats_ref[block] = rounded[:, span]
            if chunk < early:
                first_half[own * hb + block] = rounded[:, span]
            else:
                for head in range(heads):
                    second_half[head][own * hb + block - hb] = rounded[head * HD : (head + 1) * HD, span]

    for shift in range(1, peers):
        u_copy(shift).start()
    for shift in range(1, peers):
        node_copy(shift, 0).start()

    tile_count = tile_rows.shape[0]
    owners = [lax.div(tile_rows[t], blocks) for t in range(tile_count)]
    lane = lax.broadcasted_iota(jnp.int32, (1, LANES), 1)
    fields = [jnp.zeros((1, LANES), jnp.int32) for _ in range(5)]
    for t in range(tile_count):
        turn = jnp.int32(0)
        for earlier in range(t):
            turn = turn + jnp.where(owners[earlier] == owners[t], 1, 0)
        row, column = tile_rows[t], tile_cols[t]
        column_owner = lax.div(column, blocks)
        column_level = lax.div(column_owner, 4)
        group = lax.div(column_level, 2) * 4 + lax.rem(column_owner, 4)
        block = lax.rem(column, blocks)
        parts = (
            row - owners[t] * blocks + 1,
            group * blocks + block,
            lax.rem(column_level, 2) + 2 * lax.div(block, hb),
            group * hb + lax.rem(block, hb),
            jnp.int32(t),
        )
        at = lane == owners[t] * capacity + turn
        fields = [jnp.where(at, part, field) for part, field in zip(parts, fields)]
    for number in range(4):
        codes_out[number : number + 1] = fields[number]
        got_codes[me, number : number + 1] = fields[number]
    code_rows[0:1] = fields[4]
    code_rows[1:8] = jnp.zeros((7, LANES), jnp.int32)
    fetch = pltpu.make_async_copy(code_rows, pick, pick_sem)
    fetch.start()
    for shift in range(1, devices):
        code_copy(shift).start()
    for chunk in range(chunks):
        all_nodes[chunk, own_rows, :] = nodes_ref[:, chunk * width : (chunk + 1) * width]
    fetch.wait()
    for slot in range(slots):
        masks_out[slot] = tiles_ref[pick[0, slot]]
    masks2[pl.ds(me * capacity, capacity)] = masks_out[pl.ds(me * capacity, capacity)]
    for shift in range(1, devices):
        mask_copy(shift).start()

    for shift in range(1, peers):
        u_copy(shift).wait_recv()
    stacked = jnp.concatenate([u_all[peer] for peer in range(peers)], axis=0)
    high = stacked.astype(jnp.bfloat16)
    rest = stacked - high.astype(jnp.float32)
    middle = rest.astype(jnp.bfloat16)
    low = (rest - middle.astype(jnp.float32)).astype(jnp.bfloat16)
    pieces = jnp.concatenate([high, middle, low], axis=0)
    count = 2 * heads * peers
    scored = jnp.dot(pieces, nodes_ref[...], preferred_element_type=jnp.float32)
    scored = scored[:count] + scored[count : 2 * count] + scored[2 * count :]
    for peer in range(peers):
        score_send[peer] = scored[peer * 2 * heads : (peer + 1) * 2 * heads]
    score_recv[mine] = score_send[mine]
    for shift in range(1, peers):
        score_copy(shift).start()
    for chunk in range(1, chunks):
        for shift in range(1, peers):
            node_copy(shift, chunk).start()

    project(0)
    for shift in range(1, peers):
        score_copy(shift).wait_recv()
    scores = score_recv[0]
    for peer in range(1, peers):
        scores = scores + score_recv[peer]
    for block in range(blocks):
        span = slice(block * size, (block + 1) * size)
        source = scores[:heads, span]
        target = scores[heads:, span]
        all_source[own * blocks + block] = source
        targ[blocks + block] = target
        stats_ref[0, block] = leaky_relu(source + target)
    own_out(score_item)
    own_out(0)
    pair_copy(1).start()

    def forward_masks():
        for shift in range(1, devices):
            mask_copy(shift).wait_recv()
        pair_copy(0).start()

    def order():
        for shift in range(1, devices):
            code_copy(shift).wait_recv()
        lane = lax.broadcasted_iota(jnp.int32, (4, LANES), 1)
        for which, holder in enumerate((pair, me)):
            codes = jnp.zeros((4, LANES), jnp.int32)
            for device in range(devices):
                turn = lax.rem((device - holder) * capacity + devices * LANES, LANES)
                moved = pltpu.roll(got_codes[device], turn, 1)
                here = (lane >= device * capacity) & (lane < (device + 1) * capacity)
                codes = jnp.where(here, moved, codes)
            row, column, spot = codes[0:1], codes[1:2], codes[3:4]
            column_parity = jnp.bitwise_and(codes[2:3], 1)
            late = jnp.right_shift(codes[2:3], 1)
            lanes = LANES
            key = jnp.where((row > 0) & (column_parity == parity), row - 1, blocks)
            turned = jnp.transpose(jnp.concatenate([key, column, spot, late] + [key] * 4, axis=0))
            key_t = turned[:, 0:1]
            column_t = turned[:, 1:2]
            spot_t = turned[:, 2:3]
            late_t = turned[:, 3:4]
            along = lax.broadcasted_iota(jnp.int32, (lanes, lanes), 1)
            down = lax.broadcasted_iota(jnp.int32, (lanes, lanes), 0)
            before = (key_t < key) | ((key_t == key) & (down < along))
            rank = jnp.sum(jnp.where(before, 1, 0), axis=0, keepdims=True)
            rank_t = jnp.transpose(jnp.concatenate([rank] * 8, axis=0))[:, 0:1]
            at = rank_t == along
            slot = jnp.sum(jnp.where(at, down, 0), axis=0, keepdims=True)
            table_v[which, 0:1] = (1 - which) * slots + jnp.minimum(slot, slots - 1)
            table_v[which, 1:2] = jnp.sum(jnp.where(at, key_t, 0), axis=0, keepdims=True)
            table_v[which, 2:3] = jnp.sum(jnp.where(at, column_t, 0), axis=0, keepdims=True)
            table_v[which, 3:4] = jnp.sum(jnp.where(key_t <= along, 1, 0), axis=0, keepdims=True)
            table_v[which, 4:5] = jnp.sum(jnp.where(at, spot_t, 0), axis=0, keepdims=True)
            table_v[which, 5:6] = jnp.sum(jnp.where(at, late_t, 0), axis=0, keepdims=True)
            table_v[which, 6:8] = jnp.zeros((2, lanes), jnp.int32)
        table_copy().start()

    def table_copy():
        return pltpu.make_async_copy(table_v, table, local_sem)

    words = size // 32
    to_sign = 31 - lax.broadcasted_iota(jnp.int32, (32, size), 0)

    def partial(which, k):
        slot = table[which, 0, k]
        key = table[which, 1, k]
        column = table[which, 2, k]
        packed = masks2[slot] * jnp.where(key < blocks, 1, 0)
        edges = jnp.concatenate(
            [
                jnp.left_shift(packed[word : word + 1, :], to_sign)
                for word in range(words)
            ],
            axis=0,
        ) < 0
        source = all_source[column]
        source = jnp.transpose(jnp.concatenate([source] * (8 // heads), axis=0))
        target = targ[which * blocks + jnp.minimum(key, blocks - 1)]
        peaks = []
        for head in range(heads):
            one = slice(head, head + 1)
            here = jnp.where(edges, source[:, one], FAR_BELOW)
            aim = target[one]
            peak = leaky_relu(aim + jnp.max(here, axis=0, keepdims=True))
            peak = jnp.maximum(peak, FLOOR)
            weight = jnp.exp2(leaky_relu(here + aim) - peak)
            peaks.append(peak)
            weights[which * slots + k, head] = weight.astype(jnp.bfloat16)
        same = (k > 0) & (key == table[which, 1, jnp.maximum(k - 1, 0)])
        return same, jnp.concatenate(peaks, axis=0)

    together = math.gcd(slots, TOGETHER)
    turns = math.gcd(slots, 4) // together
    steps = slots // (together * turns)

    def weigh(which, index, run):
        parts = [(index * together + w, partial(which, index * together + w)) for w in range(together)]
        for k, (same, peak) in parts:
            again = jnp.where(same, 1.0, 0.0)
            old = jnp.where(same, run, FLOOR)
            run = jnp.maximum(old, peak)
            spot = which * slots + k
            keeps[spot] = jnp.exp2(old - run) * again
            scales[spot] = jnp.exp2(peak - run)
            bests[spot] = run
        return run

    def fresh():
        return jnp.full((heads, size), FLOOR, jnp.float32)

    ones = jnp.ones((16, size), jnp.bfloat16)

    def multiply(which, head, first, unroll, total):
        rows = slice(head * HD, (head + 1) * HD)
        one = slice(head, head + 1)
        values = []
        for w in range(unroll):
            spot = table[which, 4, first + w]
            late = table[which, 5, first + w]
            feats = jnp.where(late == 0, first_half[spot, rows], second_half[head][spot])
            feats = jnp.concatenate([feats, ones], axis=0)
            values.append(
                jnp.dot(feats, weights[which * slots + first + w, head], preferred_element_type=jnp.float32)
            )
        for w in range(unroll):
            spot = which * slots + first + w
            total = total * keeps[spot, one] + values[w][: HD + 8] * scales[spot, one]
            scan[first + w] = total
        return total

    def ending(which, key):
        upto = table[which, 3, key]
        prior = table[which, 3, key - 1] if key > 0 else 0
        return jnp.maximum(upto - 1, 0), upto > prior

    def play(events):
        for what, item in events:
            what(item)

    first = score_item + 1
    standard = early == 4 and heads == 4 and chunks == 8 and steps == 16

    def near_weights(count, state):
        at, carry = state
        body = functools.partial(weigh, 0)
        return at + count, lax.fori_loop(at * turns, (at + count) * turns, body, carry)

    def own_weights(count, state):
        at, carry = state
        body = functools.partial(weigh, 1)
        return at + count, lax.fori_loop(at * turns, (at + count) * turns, body, carry)

    def near_values(head):
        from_core(first + head)

        def body(index, total):
            return multiply(0, head, index * unroll, unroll, total)

        lax.fori_loop(0, slots // unroll, body, jnp.zeros((HD + 8, size), jnp.float32))
        for block in range(blocks):
            index, some = ending(0, block)
            found = jnp.where(some, scan[index], 0.0)
            part_send[head, block] = found[:HD].astype(jnp.bfloat16)
            mass_send[head, block : block + 1] = found[HD : HD + 1]
        part_copy(head).start()
        mass_copy(head).start()

    def own_values(head):
        def body(index, total):
            return multiply(1, head, index * unroll, unroll, total)

        lax.fori_loop(0, slots // unroll, body, jnp.zeros((HD + 8, size), jnp.float32))
        for block in range(blocks):
            index, some = ending(1, block)
            found = jnp.where(some, scan[index], 0.0)
            total_ref[head, block] = found[:HD]
            mass_ref[head, block : block + 1] = found[HD : HD + 1]

    def near_stats():
        for block in range(blocks):
            index, some = ending(0, block)
            stats_send[block] = jnp.where(some, bests[index], FLOOR)
        pair_copy(2).start()

    def ready_to_weigh():
        table_copy().wait()
        from_core(score_item)
        pair_copy(1).wait_recv()
        pair_copy(0).wait_recv()

    unroll = math.gcd(slots, UNROLL)
    near = (0, fresh())
    mine_state = (0, fresh())
    if standard:
        project(1)
        far_if_middle(1)
        own_near(1)
        forward_masks()
        order()
        project(2)
        from_facing(score_item)
        far_if_middle(2)
        far_if_end(1)
        own_near(2)
        from_far(score_item)
        project(3)
        far_if_middle(3)
        far_if_end(2)
        own_near(3)
        project(4)
        from_facing_far(score_item)
        project(5)
        from_far(0)
        far_if_end(3)
        project(6)
        project(7)
        for head in range(heads):
            far_if_middle(first + head)
            own_core(first + head)
        own_facing(first)
        ready_to_weigh()
        near = near_weights(2, near)
        play([(far_if_end, first), (from_far, 1), (own_facing, first + 1)])
        near = near_weights(4, near)
        play([(far_if_end, first + 1), (from_far, 2)])
        near = near_weights(4, near)
        play([(far_if_end, first + 2), (from_far, 3), (own_facing, first + 2)])
        near = near_weights(3, near)
        play([(from_facing, 0), (from_facing, 1), (from_facing, 2), (from_facing, 3)])
        near = near_weights(3, near)
        play([(far_if_end, first + 3), (from_far, first), (own_facing, first + 3)])
        near_stats()
        mine_state = own_weights(2, mine_state)
        play([(from_facing, first), (from_facing_far, 0), (from_facing_far, 1), (from_facing_far, 2)])
        mine_state = own_weights(2, mine_state)
        play([(from_far, first + 1), (from_facing_far, 3), (from_facing, first + 1)])
        mine_state = own_weights(2, mine_state)
        play([(from_facing_far, first)])
        mine_state = own_weights(2, mine_state)
        play([(from_far, first + 2)])
        for item in range(early):
            from_core(item)
        near_values(0)
        play([(from_facing_far, first + 1), (from_facing, first + 2)])
        mine_state = own_weights(2, mine_state)
        near_values(1)
        play([(from_far, first + 3), (from_facing, first + 3)])
        mine_state = own_weights(1, mine_state)
        play([(from_facing_far, first + 2)])
        mine_state = own_weights(2, mine_state)
        near_values(2)
        play([(from_facing_far, first + 3)])
        mine_state = own_weights(2, mine_state)
        near_values(3)
        mine_state = own_weights(1, mine_state)
        for head in range(heads):
            own_values(head)
    else:
        for chunk in range(1, chunks):
            project(chunk)
            if chunk < early:
                own_out(chunk)
        forward_masks()
        order()
        for head in range(heads):
            own_out(first + head)
        for item in [score_item] + [i for i in range(items) if i != score_item]:
            play([(from_facing, item), (from_far, item), (from_facing_far, item)])
        ready_to_weigh()
        near = near_weights(steps, near)
        near_stats()
        mine_state = own_weights(steps, mine_state)
        for item in range(early):
            from_core(item)
        for head in range(heads):
            near_values(head)
            own_values(head)

    for block in range(blocks):
        index, some = ending(1, block)
        stats_ref[1, block] = jnp.where(some, bests[slots + index], FLOOR)
    for shift in range(1, peers):
        u_copy(shift).wait_send()
        score_copy(shift).wait_send()
        for chunk in range(chunks):
            node_copy(shift, chunk).wait_send()
    for shift in range(1, devices):
        code_copy(shift).wait_send()
        mask_copy(shift).wait_send()
    for item in range(items):
        for shift in range(1, groups):
            far_copy(shift, item).wait_send()
        for q in range(groups):
            facing_copy(q, item).wait_send()
            for b in range(2):
                core_copy(q, b, item).wait_send()
    for which in range(3):
        pair_copy(which).wait_send()
    pair_copy(2).wait_recv()
    for head in range(heads):
        part_copy(head).wait()
        mass_copy(head).wait()


def finish_kernel(
    heads,
    feats_ref,
    total_ref,
    part_ref,
    stats_ref,
    other_ref,
    mass_ref,
    part_mass_ref,
    nodes_ref,
    bias_ref,
    out_ref,
):
    blocks = feats_ref.shape[0]
    size = LANES
    row = bias_ref[...]
    width = row.shape[1]
    if width < LANES:
        row = jnp.concatenate([row, jnp.zeros((1, LANES - width), row.dtype)], axis=1)
    bias = jnp.transpose(jnp.concatenate([row] * 8, axis=0))[:width, 0:1]
    for block in range(blocks):
        span = slice(block * size, (block + 1) * size)
        itself = stats_ref[0, block]
        here = stats_ref[1, block]
        there = other_ref[block]
        mass = jnp.concatenate([mass_ref[head, block : block + 1] for head in range(heads)], axis=0)
        part_mass = jnp.concatenate([part_mass_ref[head, block : block + 1] for head in range(heads)], axis=0)
        best = jnp.maximum(jnp.maximum(itself, here), there)
        alone = jnp.exp2(itself - best)
        near = jnp.exp2(here - best)
        away = jnp.exp2(there - best)
        shared = 1.0 / (alone + near * mass + away * part_mass)
        alone = alone * shared
        near = near * shared
        away = away * shared
        for head in range(heads):
            rows = slice(head * HD, (head + 1) * HD)
            one = slice(head, head + 1)
            flat = (
                total_ref[head, block] * near[one]
                + part_ref[head, block].astype(jnp.float32) * away[one]
                + feats_ref[block, rows].astype(jnp.float32) * alone[one]
                + nodes_ref[rows, span].astype(jnp.float32)
                + bias[rows]
            )
            out_ref[rows, span] = jnp.where(flat > 0, flat, jnp.exp(flat) - 1.0).astype(out_ref.dtype)


def local(node_feats, proj_weight, att_src, att_dst, out_bias, tile_rows, tile_cols, tile_masks):
    dims, columns = node_feats.shape
    head_dims, inputs = proj_weight.shape
    heads = head_dims // HD
    size = tile_masks.shape[2]
    words = tile_masks.shape[1]
    blocks = columns // size
    devices = lax.axis_size("dp")
    peers = lax.axis_size("mp")
    capacity = max(2, 2 * tile_rows.shape[0] // devices)
    depth = devices // 4
    groups = depth // 2
    origins = groups * 4
    chunks = math.gcd(blocks, max(2, 128 // devices))
    early = chunks // 2
    items = early + 1 + heads
    slots = devices * capacity
    positions = 2 * slots
    hb = blocks // 2
    whole = pl.BlockSpec(memory_space=VMEM)
    smem = pltpu.SMEM
    dma = pltpu.SemaphoreType.DMA
    f32 = jnp.float32
    bf16 = jnp.bfloat16
    others = max(1, peers - 1)
    feats, total, part, stats, other, mass, part_mass = pl.pallas_call(
        functools.partial(main_kernel, heads, capacity, chunks, depth, peers),
        out_shape=(
            jax.ShapeDtypeStruct((blocks, head_dims, size), bf16),
            jax.ShapeDtypeStruct((heads, blocks, HD, size), f32),
            jax.ShapeDtypeStruct((heads, blocks, HD, size), bf16),
            jax.ShapeDtypeStruct((2, blocks, heads, size), f32),
            jax.ShapeDtypeStruct((blocks, heads, size), f32),
            jax.ShapeDtypeStruct((heads, blocks, size), f32),
            jax.ShapeDtypeStruct((heads, blocks, size), f32),
        ),
        in_specs=[whole] * 5 + [pl.BlockSpec(memory_space=smem)] * 2,
        out_specs=(whole,) * 7,
        scratch_shapes=[
            VMEM((origins * hb, head_dims, size), bf16),
            VMEM((origins * blocks, heads, size), f32),
            VMEM((2 * blocks, heads, size), f32),
            VMEM((chunks, inputs, columns // chunks), bf16),
            VMEM((slots, words, size), jnp.int32),
            VMEM((2 * slots, words, size), jnp.int32),
            VMEM((8, LANES), jnp.int32),
            VMEM((4, LANES), jnp.int32),
            smem((8, LANES), jnp.int32),
            VMEM((devices, 4, LANES), jnp.int32),
            VMEM((peers, 2 * heads, dims), f32),
            VMEM((peers, 2 * heads, dims), f32),
            VMEM((peers, 2 * heads, columns), f32),
            VMEM((peers, 2 * heads, columns), f32),
            VMEM((2, 8, LANES), jnp.int32),
            smem((2, 8, LANES), jnp.int32),
            VMEM((positions, heads, size, size), bf16),
            VMEM((positions, heads, size), f32),
            VMEM((positions, heads, size), f32),
            VMEM((positions, heads, size), f32),
            VMEM((slots, HD + 8, size), f32),
            VMEM((heads, blocks, HD, size), bf16),
            VMEM((heads, blocks, size), f32),
            VMEM((blocks, heads, size), f32),
            dma((others, chunks)),
            dma((others, chunks)),
            dma((others,)),
            dma((others,)),
            dma((others,)),
            dma((others,)),
            dma((devices - 1,)),
            dma((devices - 1,)),
            dma((devices - 1,)),
            dma((devices - 1,)),
            dma((max(1, groups - 1), items)),
            dma((groups, items)),
            dma((groups, 2, items)),
            dma((origins, items)),
            dma((3,)),
            dma((3,)),
            dma((heads,)),
            dma((heads,)),
            dma((heads,)),
            dma((heads,)),
            dma,
            dma,
        ]
        + [VMEM((origins * hb, HD, size), bf16) for _ in range(heads)],
        compiler_params=pltpu.CompilerParams(
            collective_id=0, has_side_effects=True, vmem_limit_bytes=48 * 1024 * 1024
        ),
        name="graph",
    )(
        proj_weight,
        node_feats,
        att_src.reshape(1, head_dims),
        att_dst.reshape(1, head_dims),
        tile_masks,
        tile_rows,
        tile_cols,
    )
    return pl.pallas_call(
        functools.partial(finish_kernel, heads),
        out_shape=jax.ShapeDtypeStruct((head_dims, columns), bf16),
        in_specs=[whole] * 9,
        out_specs=whole,
        compiler_params=pltpu.CompilerParams(vmem_limit_bytes=40 * 1024 * 1024),
        name="finish",
    )(feats, total, part, stats, other, mass, part_mass, node_feats, out_bias.reshape(1, head_dims))


def solution(mesh):
    return jax.shard_map(
        local,
        mesh=mesh,
        in_specs=(
            P("mp", "dp"),
            P("mp", None),
            P("mp"),
            P("mp"),
            P("mp"),
            P("dp"),
            P("dp"),
            P("dp", None, None),
        ),
        out_specs=P("mp", "dp"),
        check_vma=False,
    )
```

```python
import functools
import math

import jax
import jax.numpy as jnp
from jax import lax
from jax.experimental import pallas as pl
from jax.experimental.pallas import tpu as pltpu
from jax.sharding import PartitionSpec as P

HD = 32
LOG2E = 1.4426950408889634
FAR_BELOW = -1e30
FLOOR = -1e9
TOGETHER = 4
UNROLL = 32
VMEM = pltpu.VMEM
LANES = 128
MESH = pl.DeviceIdType.MESH


def leaky_relu(scores):
    return jnp.maximum(scores, 0.2 * scores)


def main_kernel(
    heads,
    capacity,
    chunks,
    depth,
    peers,
    weight_in,
    nodes_in,
    att_src_in,
    att_dst_in,
    bias_in,
    tiles_in,
    rows_in,
    cols_in,
    feats_ref,
    total_ref,
    part_ref,
    stats_ref,
    other_ref,
    mass_ref,
    part_mass_ref,
    nodes_ref,
    bias_ref,
    *scratch,
):
    (
        first_half,
        all_source,
        targ,
        all_nodes,
        masks_out,
        masks2,
        code_rows,
        codes_out,
        pick,
        got_codes,
        u_send,
        u_all,
        score_send,
        score_recv,
        table_v,
        table,
        weights,
        keeps,
        scales,
        bests,
        scan,
        part_send,
        mass_send,
        stats_send,
        node_send,
        node_recv,
        u_ss,
        u_rs,
        score_ss,
        score_rs,
        mask_ss,
        mask_rs,
        code_ss,
        code_rs,
        far_ss,
        facing_ss,
        core_ss,
        recv_sem,
        pair_ss,
        pair_rs,
        part_ss,
        part_rs,
        mass_ss,
        mass_rs,
        local_sem,
        pick_sem,
        load_sem,
        weight_ref,
        att_src_ref,
        att_dst_ref,
        tiles_ref,
        tile_rows,
        tile_cols,
    ) = scratch[: len(scratch) - heads]
    second_half = scratch[len(scratch) - heads :]

    devices = 4 * depth
    groups = depth // 2
    me = lax.axis_index("dp")
    core = lax.rem(me, 2)
    beside = lax.rem(lax.div(me, 2), 2)
    level = lax.div(me, 4)
    parity = lax.rem(level, 2)
    where_in = lax.div(level, 2)
    mine = lax.axis_index("mp")
    dims, columns = nodes_in.shape
    head_dims = weight_in.shape[0]
    size = LANES
    blocks = columns // size
    hb = blocks // 2
    per = blocks // chunks
    width = per * size
    slots = devices * capacity
    early = chunks // 2
    score_item = early
    items = early + 1 + heads

    def place(lev, b, c):
        return (lev * 2 + b) * 2 + c

    def origin_of(q, b, c):
        return (q * 2 + b) * 2 + c

    own = origin_of(where_in, beside, core)
    facing = place(level, 1 - beside, core)
    other_core = place(level, beside, 1 - core)
    pair = place(level + 1 - 2 * parity, beside, core)

    loads = [
        pltpu.make_async_copy(source, target, load_sem.at[number])
        for number, (source, target) in enumerate(
            (
                (weight_in, weight_ref),
                (att_src_in, att_src_ref),
                (att_dst_in, att_dst_ref),
                (nodes_in, nodes_ref),
                (rows_in, tile_rows),
                (cols_in, tile_cols),
                (tiles_in, tiles_ref),
                (bias_in, bias_ref),
            )
        )
    ]
    for load in loads:
        load.start()
    barrier = pltpu.get_barrier_semaphore()
    for shift in range(1, devices):
        pl.semaphore_signal(barrier, 1, device_id={"dp": lax.rem(me + shift, devices)}, device_id_type=MESH)
    for shift in range(1, peers):
        pl.semaphore_signal(barrier, 1, device_id={"mp": lax.rem(mine + shift, peers)}, device_id_type=MESH)

    own_rows = pl.ds(pl.multiple_of(mine * dims, dims), dims)

    def as_column(ref):
        row = ref[...]
        if head_dims < LANES:
            row = jnp.concatenate([row, jnp.zeros((1, LANES - head_dims), row.dtype)], axis=1)
        return jnp.transpose(jnp.concatenate([row] * 8, axis=0))[:head_dims, 0:1]

    for load in loads[:3]:
        load.wait()
    wide = weight_ref[...].astype(jnp.float32)
    by_source = wide * (LOG2E * as_column(att_src_ref))
    by_target = wide * (LOG2E * as_column(att_dst_ref))
    rows = []
    for scaled in (by_source, by_target):
        for head in range(heads):
            rows.append(jnp.sum(scaled[head * HD : (head + 1) * HD], axis=0, keepdims=True))
    reduced = jnp.concatenate(rows, axis=0)
    for peer in range(peers):
        u_send[peer] = reduced[:, peer * dims : (peer + 1) * dims]
    u_all[mine] = u_send[mine]
    for load in loads[3:]:
        load.wait()
    pl.semaphore_wait(barrier, devices - 1 + peers - 1)

    def node_copy(shift, chunk):
        return pltpu.make_async_remote_copy(
            src_ref=nodes_ref.at[:, pl.ds(chunk * width, width)],
            dst_ref=all_nodes.at[chunk, own_rows, :],
            send_sem=node_send.at[shift - 1, chunk],
            recv_sem=node_recv.at[shift - 1, chunk],
            device_id={"mp": lax.rem(mine + shift, peers)},
            device_id_type=MESH,
        )

    def u_copy(shift):
        to = lax.rem(mine + shift, peers)
        return pltpu.make_async_remote_copy(
            src_ref=u_send.at[to],
            dst_ref=u_all.at[mine],
            send_sem=u_ss.at[shift - 1],
            recv_sem=u_rs.at[shift - 1],
            device_id={"mp": to},
            device_id_type=MESH,
        )

    def score_copy(shift):
        to = lax.rem(mine + shift, peers)
        return pltpu.make_async_remote_copy(
            src_ref=score_send.at[to],
            dst_ref=score_recv.at[mine],
            send_sem=score_ss.at[shift - 1],
            recv_sem=score_rs.at[shift - 1],
            device_id={"mp": to},
            device_id_type=MESH,
        )

    def mask_copy(shift):
        to = lax.rem(me + shift, devices)
        return pltpu.make_async_remote_copy(
            src_ref=masks_out.at[pl.ds(to * capacity, capacity)],
            dst_ref=masks2.at[pl.ds(me * capacity, capacity)],
            send_sem=mask_ss.at[shift - 1],
            recv_sem=mask_rs.at[shift - 1],
            device_id={"dp": to},
            device_id_type=MESH,
        )

    def code_copy(shift):
        to = lax.rem(me + shift, devices)
        return pltpu.make_async_remote_copy(
            src_ref=codes_out,
            dst_ref=got_codes.at[me],
            send_sem=code_ss.at[shift - 1],
            recv_sem=code_rs.at[shift - 1],
            device_id={"dp": to},
            device_id_type=MESH,
        )

    def pair_copy(which):
        src, dst = (
            (masks2.at[pl.ds(0, slots)], masks2.at[pl.ds(slots, slots)]),
            (targ.at[pl.ds(blocks, blocks)], targ.at[pl.ds(0, blocks)]),
            (stats_send, other_ref),
        )[which]
        return pltpu.make_async_remote_copy(
            src_ref=src,
            dst_ref=dst,
            send_sem=pair_ss.at[which],
            recv_sem=pair_rs.at[which],
            device_id={"dp": pair},
            device_id_type=MESH,
        )

    def part_copy(head):
        return pltpu.make_async_remote_copy(
            src_ref=part_send.at[head],
            dst_ref=part_ref.at[head],
            send_sem=part_ss.at[head],
            recv_sem=part_rs.at[head],
            device_id={"dp": pair},
            device_id_type=MESH,
        )

    def mass_copy(head):
        return pltpu.make_async_remote_copy(
            src_ref=mass_send.at[head],
            dst_ref=part_mass_ref.at[head],
            send_sem=mass_ss.at[head],
            recv_sem=mass_rs.at[head],
            device_id={"dp": pair},
            device_id_type=MESH,
        )

    def item_ref(origin, item):
        if item < early:
            return first_half.at[pl.ds(origin * hb + item * per, per)]
        if item == score_item:
            return all_source.at[pl.ds(origin * blocks, blocks)]
        return second_half[item - score_item - 1].at[pl.ds(origin * hb, hb)]

    def send(origin, item, to, sem):
        part = item_ref(origin, item)
        return pltpu.make_async_remote_copy(
            src_ref=part,
            dst_ref=part,
            send_sem=sem,
            recv_sem=recv_sem.at[origin, item],
            device_id={"dp": to},
            device_id_type=MESH,
        )

    def far_copy(shift, item):
        to = place(2 * lax.rem(where_in + shift, groups) + parity, beside, core)
        return send(own, item, to, far_ss.at[shift - 1, item])

    def facing_copy(q, item):
        return send(origin_of(q, beside, core), item, facing, facing_ss.at[q, item])

    def core_copy(q, b, item):
        return send(origin_of(q, b, core), item, other_core, core_ss.at[q, b, item])

    def arrival(origin, item):
        send(origin, item, other_core, core_ss.at[0, 0, item]).wait_recv()

    def own_core(item):
        core_copy(where_in, beside, item).start()

    def own_far(item):
        for shift in range(1, groups):
            far_copy(shift, item).start()

    at_end = (level == 0) | (level == depth - 1)

    def far_if_end(item):
        pl.when(at_end)(lambda: own_far(item))

    def far_if_middle(item):
        pl.when(jnp.logical_not(at_end))(lambda: own_far(item))

    def own_facing(item):
        facing_copy(where_in, item).start()

    def own_out(item):
        own_far(item)
        own_near(item)

    def own_near(item):
        own_facing(item)
        own_core(item)

    def far_q(shift):
        return lax.rem(where_in + groups - shift, groups)

    def from_far(item):
        for shift in range(1, groups):
            q = far_q(shift)
            arrival(origin_of(q, beside, core), item)
            facing_copy(q, item).start()
            core_copy(q, beside, item).start()

    def from_facing(item):
        arrival(origin_of(where_in, 1 - beside, core), item)
        core_copy(where_in, 1 - beside, item).start()

    def from_facing_far(item):
        for shift in range(1, groups):
            q = far_q(shift)
            arrival(origin_of(q, 1 - beside, core), item)
            core_copy(q, 1 - beside, item).start()

    def from_core(item):
        for q in range(groups):
            for b in range(2):
                arrival(origin_of(q, b, 1 - core), item)

    def project(chunk):
        for shift in range(1, peers):
            node_copy(shift, chunk).wait_recv()
        projected = jnp.dot(weight_ref[...], all_nodes[chunk], preferred_element_type=jnp.float32)
        rounded = projected.astype(jnp.bfloat16)
        for j in range(per):
            block = chunk * per + j
            span = slice(j * size, (j + 1) * size)
            feats_ref[block] = rounded[:, span]
            if chunk < early:
                first_half[own * hb + block] = rounded[:, span]
            else:
                for head in range(heads):
                    second_half[head][own * hb + block - hb] = rounded[head * HD : (head + 1) * HD, span]

    for shift in range(1, peers):
        u_copy(shift).start()
    for shift in range(1, peers):
        node_copy(shift, 0).start()

    tile_count = tile_rows.shape[0]
    owners = [lax.div(tile_rows[t], blocks) for t in range(tile_count)]
    lane = lax.broadcasted_iota(jnp.int32, (1, LANES), 1)
    fields = [jnp.zeros((1, LANES), jnp.int32) for _ in range(5)]
    for t in range(tile_count):
        turn = jnp.int32(0)
        for earlier in range(t):
            turn = turn + jnp.where(owners[earlier] == owners[t], 1, 0)
        row, column = tile_rows[t], tile_cols[t]
        column_owner = lax.div(column, blocks)
        column_level = lax.div(column_owner, 4)
        group = lax.div(column_level, 2) * 4 + lax.rem(column_owner, 4)
        block = lax.rem(column, blocks)
        parts = (
            row - owners[t] * blocks + 1,
            group * blocks + block,
            lax.rem(column_level, 2) + 2 * lax.div(block, hb),
            group * hb + lax.rem(block, hb),
            jnp.int32(t),
        )
        at = lane == owners[t] * capacity + turn
        fields = [jnp.where(at, part, field) for part, field in zip(parts, fields)]
    for number in range(4):
        codes_out[number : number + 1] = fields[number]
        got_codes[me, number : number + 1] = fields[number]
    code_rows[0:1] = fields[4]
    code_rows[1:8] = jnp.zeros((7, LANES), jnp.int32)
    fetch = pltpu.make_async_copy(code_rows, pick, pick_sem)
    fetch.start()
    for shift in range(1, devices):
        code_copy(shift).start()
    for chunk in range(chunks):
        all_nodes[chunk, own_rows, :] = nodes_ref[:, chunk * width : (chunk + 1) * width]
    fetch.wait()
    for slot in range(slots):
        masks_out[slot] = tiles_ref[pick[0, slot]]
    masks2[pl.ds(me * capacity, capacity)] = masks_out[pl.ds(me * capacity, capacity)]
    for shift in range(1, devices):
        mask_copy(shift).start()

    for shift in range(1, peers):
        u_copy(shift).wait_recv()
    stacked = jnp.concatenate([u_all[peer] for peer in range(peers)], axis=0)
    high = stacked.astype(jnp.bfloat16)
    rest = stacked - high.astype(jnp.float32)
    middle = rest.astype(jnp.bfloat16)
    low = (rest - middle.astype(jnp.float32)).astype(jnp.bfloat16)
    pieces = jnp.concatenate([high, middle, low], axis=0)
    count = 2 * heads * peers
    scored = jnp.dot(pieces, nodes_ref[...], preferred_element_type=jnp.float32)
    scored = scored[:count] + scored[count : 2 * count] + scored[2 * count :]
    for peer in range(peers):
        score_send[peer] = scored[peer * 2 * heads : (peer + 1) * 2 * heads]
    score_recv[mine] = score_send[mine]
    for shift in range(1, peers):
        score_copy(shift).start()
    for chunk in range(1, chunks):
        for shift in range(1, peers):
            node_copy(shift, chunk).start()

    project(0)
    for shift in range(1, peers):
        score_copy(shift).wait_recv()
    scores = score_recv[0]
    for peer in range(1, peers):
        scores = scores + score_recv[peer]
    for block in range(blocks):
        span = slice(block * size, (block + 1) * size)
        source = scores[:heads, span]
        target = scores[heads:, span]
        all_source[own * blocks + block] = source
        targ[blocks + block] = target
        stats_ref[0, block] = leaky_relu(source + target)
    own_out(score_item)
    own_out(0)
    pair_copy(1).start()

    def forward_masks():
        for shift in range(1, devices):
            mask_copy(shift).wait_recv()
        pair_copy(0).start()

    def order():
        for shift in range(1, devices):
            code_copy(shift).wait_recv()
        lane = lax.broadcasted_iota(jnp.int32, (4, LANES), 1)
        for which, holder in enumerate((pair, me)):
            codes = jnp.zeros((4, LANES), jnp.int32)
            for device in range(devices):
                turn = lax.rem((device - holder) * capacity + devices * LANES, LANES)
                moved = pltpu.roll(got_codes[device], turn, 1)
                here = (lane >= device * capacity) & (lane < (device + 1) * capacity)
                codes = jnp.where(here, moved, codes)
            row, column, spot = codes[0:1], codes[1:2], codes[3:4]
            column_parity = jnp.bitwise_and(codes[2:3], 1)
            late = jnp.right_shift(codes[2:3], 1)
            lanes = LANES
            key = jnp.where((row > 0) & (column_parity == parity), row - 1, blocks)
            turned = jnp.transpose(jnp.concatenate([key, column, spot, late] + [key] * 4, axis=0))
            key_t = turned[:, 0:1]
            column_t = turned[:, 1:2]
            spot_t = turned[:, 2:3]
            late_t = turned[:, 3:4]
            along = lax.broadcasted_iota(jnp.int32, (lanes, lanes), 1)
            down = lax.broadcasted_iota(jnp.int32, (lanes, lanes), 0)
            before = (key_t < key) | ((key_t == key) & (down < along))
            rank = jnp.sum(jnp.where(before, 1, 0), axis=0, keepdims=True)
            rank_t = jnp.transpose(jnp.concatenate([rank] * 8, axis=0))[:, 0:1]
            at = rank_t == along
            slot = jnp.sum(jnp.where(at, down, 0), axis=0, keepdims=True)
            table_v[which, 0:1] = (1 - which) * slots + jnp.minimum(slot, slots - 1)
            table_v[which, 1:2] = jnp.sum(jnp.where(at, key_t, 0), axis=0, keepdims=True)
            table_v[which, 2:3] = jnp.sum(jnp.where(at, column_t, 0), axis=0, keepdims=True)
            table_v[which, 3:4] = jnp.sum(jnp.where(key_t <= along, 1, 0), axis=0, keepdims=True)
            table_v[which, 4:5] = jnp.sum(jnp.where(at, spot_t, 0), axis=0, keepdims=True)
            table_v[which, 5:6] = jnp.sum(jnp.where(at, late_t, 0), axis=0, keepdims=True)
            table_v[which, 6:8] = jnp.zeros((2, lanes), jnp.int32)
        table_copy().start()

    def table_copy():
        return pltpu.make_async_copy(table_v, table, local_sem)

    words = size // 32
    to_sign = 31 - lax.broadcasted_iota(jnp.int32, (32, size), 0)

    def partial(which, k):
        slot = table[which, 0, k]
        key = table[which, 1, k]
        column = table[which, 2, k]
        packed = masks2[slot] * jnp.where(key < blocks, 1, 0)
        edges = jnp.concatenate(
            [
                jnp.left_shift(packed[word : word + 1, :], to_sign)
                for word in range(words)
            ],
            axis=0,
        ) < 0
        source = all_source[column]
        source = jnp.transpose(jnp.concatenate([source] * (8 // heads), axis=0))
        target = targ[which * blocks + jnp.minimum(key, blocks - 1)]
        peaks = []
        for head in range(heads):
            one = slice(head, head + 1)
            here = jnp.where(edges, source[:, one], FAR_BELOW)
            aim = target[one]
            peak = leaky_relu(aim + jnp.max(here, axis=0, keepdims=True))
            peak = jnp.maximum(peak, FLOOR)
            weight = jnp.exp2(leaky_relu(here + aim) - peak)
            peaks.append(peak)
            weights[which * slots + k, head] = weight.astype(jnp.bfloat16)
        same = (k > 0) & (key == table[which, 1, jnp.maximum(k - 1, 0)])
        return same, jnp.concatenate(peaks, axis=0)

    together = math.gcd(slots, TOGETHER)
    turns = math.gcd(slots, 4) // together
    steps = slots // (together * turns)

    def weigh(which, index, run):
        parts = [(index * together + w, partial(which, index * together + w)) for w in range(together)]
        for k, (same, peak) in parts:
            again = jnp.where(same, 1.0, 0.0)
            old = jnp.where(same, run, FLOOR)
            run = jnp.maximum(old, peak)
            spot = which * slots + k
            keeps[spot] = jnp.exp2(old - run) * again
            scales[spot] = jnp.exp2(peak - run)
            bests[spot] = run
        return run

    def fresh():
        return jnp.full((heads, size), FLOOR, jnp.float32)

    ones = jnp.ones((16, size), jnp.bfloat16)

    def multiply(which, head, first, unroll, total):
        rows = slice(head * HD, (head + 1) * HD)
        one = slice(head, head + 1)
        values = []
        for w in range(unroll):
            spot = table[which, 4, first + w]
            late = table[which, 5, first + w]
            feats = jnp.where(late == 0, first_half[spot, rows], second_half[head][spot])
            feats = jnp.concatenate([feats, ones], axis=0)
            values.append(
                jnp.dot(feats, weights[which * slots + first + w, head], preferred_element_type=jnp.float32)
            )
        for w in range(unroll):
            spot = which * slots + first + w
            total = total * keeps[spot, one] + values[w][: HD + 8] * scales[spot, one]
            scan[first + w] = total
        return total

    def ending(which, key):
        upto = table[which, 3, key]
        prior = table[which, 3, key - 1] if key > 0 else 0
        return jnp.maximum(upto - 1, 0), upto > prior

    def play(events):
        for what, item in events:
            what(item)

    first = score_item + 1
    standard = early == 4 and heads == 4 and chunks == 8 and steps == 16

    def near_weights(count, state):
        at, carry = state
        body = functools.partial(weigh, 0)
        return at + count, lax.fori_loop(at * turns, (at + count) * turns, body, carry)

    def own_weights(count, state):
        at, carry = state
        body = functools.partial(weigh, 1)
        return at + count, lax.fori_loop(at * turns, (at + count) * turns, body, carry)

    def near_values(head):
        from_core(first + head)

        def body(index, total):
            return multiply(0, head, index * unroll, unroll, total)

        lax.fori_loop(0, slots // unroll, body, jnp.zeros((HD + 8, size), jnp.float32))
        for block in range(blocks):
            index, some = ending(0, block)
            found = jnp.where(some, scan[index], 0.0)
            part_send[head, block] = found[:HD].astype(jnp.bfloat16)
            mass_send[head, block : block + 1] = found[HD : HD + 1]
        part_copy(head).start()
        mass_copy(head).start()

    def own_values(head):
        def body(index, total):
            return multiply(1, head, index * unroll, unroll, total)

        lax.fori_loop(0, slots // unroll, body, jnp.zeros((HD + 8, size), jnp.float32))
        for block in range(blocks):
            index, some = ending(1, block)
            found = jnp.where(some, scan[index], 0.0)
            total_ref[head, block] = found[:HD]
            mass_ref[head, block : block + 1] = found[HD : HD + 1]

    def near_stats():
        for block in range(blocks):
            index, some = ending(0, block)
            stats_send[block] = jnp.where(some, bests[index], FLOOR)
        pair_copy(2).start()

    def ready_to_weigh():
        table_copy().wait()
        from_core(score_item)
        pair_copy(1).wait_recv()
        pair_copy(0).wait_recv()

    unroll = math.gcd(slots, UNROLL)
    near = (0, fresh())
    mine_state = (0, fresh())
    if standard:
        project(1)
        far_if_middle(1)
        own_near(1)
        forward_masks()
        order()
        project(2)
        from_facing(score_item)
        far_if_middle(2)
        far_if_end(1)
        own_near(2)
        from_far(score_item)
        project(3)
        far_if_middle(3)
        far_if_end(2)
        own_near(3)
        project(4)
        from_facing_far(score_item)
        project(5)
        from_far(0)
        far_if_end(3)
        project(6)
        project(7)
        for head in range(heads):
            far_if_middle(first + head)
            own_core(first + head)
        own_facing(first)
        ready_to_weigh()
        near = near_weights(2, near)
        play([(far_if_end, first), (from_far, 1), (own_facing, first + 1)])
        near = near_weights(4, near)
        play([(far_if_end, first + 1), (from_far, 2)])
        near = near_weights(4, near)
        play([(far_if_end, first + 2), (from_far, 3), (own_facing, first + 2)])
        near = near_weights(3, near)
        play([(from_facing, 0), (from_facing, 1), (from_facing, 2), (from_facing, 3)])
        near = near_weights(3, near)
        play([(far_if_end, first + 3), (from_far, first), (own_facing, first + 3)])
        near_stats()
        mine_state = own_weights(2, mine_state)
        play([(from_facing, first), (from_facing_far, 0), (from_facing_far, 1), (from_facing_far, 2)])
        mine_state = own_weights(2, mine_state)
        play([(from_far, first + 1), (from_facing_far, 3), (from_facing, first + 1)])
        mine_state = own_weights(2, mine_state)
        play([(from_facing_far, first)])
        mine_state = own_weights(2, mine_state)
        play([(from_far, first + 2)])
        for item in range(early):
            from_core(item)
        near_values(0)
        play([(from_facing_far, first + 1), (from_facing, first + 2)])
        mine_state = own_weights(2, mine_state)
        near_values(1)
        play([(from_far, first + 3), (from_facing, first + 3)])
        mine_state = own_weights(1, mine_state)
        play([(from_facing_far, first + 2)])
        mine_state = own_weights(2, mine_state)
        near_values(2)
        play([(from_facing_far, first + 3)])
        mine_state = own_weights(2, mine_state)
        near_values(3)
        mine_state = own_weights(1, mine_state)
        for head in range(heads):
            own_values(head)
    else:
        for chunk in range(1, chunks):
            project(chunk)
            if chunk < early:
                own_out(chunk)
        forward_masks()
        order()
        for head in range(heads):
            own_out(first + head)
        for item in [score_item] + [i for i in range(items) if i != score_item]:
            play([(from_facing, item), (from_far, item), (from_facing_far, item)])
        ready_to_weigh()
        near = near_weights(steps, near)
        near_stats()
        mine_state = own_weights(steps, mine_state)
        for item in range(early):
            from_core(item)
        for head in range(heads):
            near_values(head)
            own_values(head)

    for block in range(blocks):
        index, some = ending(1, block)
        stats_ref[1, block] = jnp.where(some, bests[slots + index], FLOOR)
    for shift in range(1, peers):
        u_copy(shift).wait_send()
        score_copy(shift).wait_send()
        for chunk in range(chunks):
            node_copy(shift, chunk).wait_send()
    for shift in range(1, devices):
        code_copy(shift).wait_send()
        mask_copy(shift).wait_send()
    for item in range(items):
        for shift in range(1, groups):
            far_copy(shift, item).wait_send()
        for q in range(groups):
            facing_copy(q, item).wait_send()
            for b in range(2):
                core_copy(q, b, item).wait_send()
    for which in range(3):
        pair_copy(which).wait_send()
    pair_copy(2).wait_recv()
    for head in range(heads):
        part_copy(head).wait()
        mass_copy(head).wait()


def finish_kernel(
    heads,
    feats_ref,
    total_ref,
    part_ref,
    stats_ref,
    other_ref,
    mass_ref,
    part_mass_ref,
    nodes_ref,
    bias_ref,
    out_ref,
):
    blocks = feats_ref.shape[0]
    size = LANES
    row = bias_ref[...]
    width = row.shape[1]
    if width < LANES:
        row = jnp.concatenate([row, jnp.zeros((1, LANES - width), row.dtype)], axis=1)
    bias = jnp.transpose(jnp.concatenate([row] * 8, axis=0))[:width, 0:1]
    for block in range(blocks):
        span = slice(block * size, (block + 1) * size)
        itself = stats_ref[0, block]
        here = stats_ref[1, block]
        there = other_ref[block]
        mass = jnp.concatenate([mass_ref[head, block : block + 1] for head in range(heads)], axis=0)
        part_mass = jnp.concatenate([part_mass_ref[head, block : block + 1] for head in range(heads)], axis=0)
        best = jnp.maximum(jnp.maximum(itself, here), there)
        alone = jnp.exp2(itself - best)
        near = jnp.exp2(here - best)
        away = jnp.exp2(there - best)
        shared = 1.0 / (alone + near * mass + away * part_mass)
        alone = alone * shared
        near = near * shared
        away = away * shared
        for head in range(heads):
            rows = slice(head * HD, (head + 1) * HD)
            one = slice(head, head + 1)
            flat = (
                total_ref[head, block] * near[one]
                + part_ref[head, block].astype(jnp.float32) * away[one]
                + feats_ref[block, rows].astype(jnp.float32) * alone[one]
                + nodes_ref[rows, span].astype(jnp.float32)
                + bias[rows]
            )
            out_ref[rows, span] = jnp.where(flat > 0, flat, jnp.exp(flat) - 1.0).astype(out_ref.dtype)


def local(node_feats, proj_weight, att_src, att_dst, out_bias, tile_rows, tile_cols, tile_masks):
    dims, columns = node_feats.shape
    head_dims, inputs = proj_weight.shape
    heads = head_dims // HD
    size = tile_masks.shape[2]
    words = tile_masks.shape[1]
    blocks = columns // size
    devices = lax.axis_size("dp")
    peers = lax.axis_size("mp")
    capacity = max(2, 2 * tile_rows.shape[0] // devices)
    depth = devices // 4
    groups = depth // 2
    origins = groups * 4
    chunks = math.gcd(blocks, max(2, 128 // devices))
    early = chunks // 2
    items = early + 1 + heads
    slots = devices * capacity
    positions = 2 * slots
    hb = blocks // 2
    whole = pl.BlockSpec(memory_space=VMEM)
    smem = pltpu.SMEM
    dma = pltpu.SemaphoreType.DMA
    f32 = jnp.float32
    bf16 = jnp.bfloat16
    others = max(1, peers - 1)
    feats, total, part, stats, other, mass, part_mass, nodes, bias = pl.pallas_call(
        functools.partial(main_kernel, heads, capacity, chunks, depth, peers),
        out_shape=(
            jax.ShapeDtypeStruct((blocks, head_dims, size), bf16),
            jax.ShapeDtypeStruct((heads, blocks, HD, size), f32),
            jax.ShapeDtypeStruct((heads, blocks, HD, size), bf16),
            jax.ShapeDtypeStruct((2, blocks, heads, size), f32),
            jax.ShapeDtypeStruct((blocks, heads, size), f32),
            jax.ShapeDtypeStruct((heads, blocks, size), f32),
            jax.ShapeDtypeStruct((heads, blocks, size), f32),
            jax.ShapeDtypeStruct((dims, columns), bf16),
            jax.ShapeDtypeStruct((1, head_dims), f32),
        ),
        in_specs=[pl.BlockSpec(memory_space=pltpu.HBM)] * 8,
        out_specs=(whole,) * 9,
        scratch_shapes=[
            VMEM((origins * hb, head_dims, size), bf16),
            VMEM((origins * blocks, heads, size), f32),
            VMEM((2 * blocks, heads, size), f32),
            VMEM((chunks, inputs, columns // chunks), bf16),
            VMEM((slots, words, size), jnp.int32),
            VMEM((2 * slots, words, size), jnp.int32),
            VMEM((8, LANES), jnp.int32),
            VMEM((4, LANES), jnp.int32),
            smem((8, LANES), jnp.int32),
            VMEM((devices, 4, LANES), jnp.int32),
            VMEM((peers, 2 * heads, dims), f32),
            VMEM((peers, 2 * heads, dims), f32),
            VMEM((peers, 2 * heads, columns), f32),
            VMEM((peers, 2 * heads, columns), f32),
            VMEM((2, 8, LANES), jnp.int32),
            smem((2, 8, LANES), jnp.int32),
            VMEM((positions, heads, size, size), bf16),
            VMEM((positions, heads, size), f32),
            VMEM((positions, heads, size), f32),
            VMEM((positions, heads, size), f32),
            VMEM((slots, HD + 8, size), f32),
            VMEM((heads, blocks, HD, size), bf16),
            VMEM((heads, blocks, size), f32),
            VMEM((blocks, heads, size), f32),
            dma((others, chunks)),
            dma((others, chunks)),
            dma((others,)),
            dma((others,)),
            dma((others,)),
            dma((others,)),
            dma((devices - 1,)),
            dma((devices - 1,)),
            dma((devices - 1,)),
            dma((devices - 1,)),
            dma((max(1, groups - 1), items)),
            dma((groups, items)),
            dma((groups, 2, items)),
            dma((origins, items)),
            dma((3,)),
            dma((3,)),
            dma((heads,)),
            dma((heads,)),
            dma((heads,)),
            dma((heads,)),
            dma,
            dma,
            dma((8,)),
            VMEM((head_dims, inputs), bf16),
            VMEM((1, head_dims), f32),
            VMEM((1, head_dims), f32),
            VMEM(tile_masks.shape, jnp.int32),
            smem(tile_rows.shape, jnp.int32),
            smem(tile_cols.shape, jnp.int32),
        ]
        + [VMEM((origins * hb, HD, size), bf16) for _ in range(heads)],
        compiler_params=pltpu.CompilerParams(
            collective_id=0, has_side_effects=True, vmem_limit_bytes=48 * 1024 * 1024
        ),
        name="graph",
    )(
        *[
            pltpu.with_memory_space_constraint(x, pltpu.HBM)
            for x in (
                proj_weight,
                node_feats,
                att_src.reshape(1, head_dims),
                att_dst.reshape(1, head_dims),
                out_bias.reshape(1, head_dims),
                tile_masks,
                tile_rows,
                tile_cols,
            )
        ]
    )
    return pl.pallas_call(
        functools.partial(finish_kernel, heads),
        out_shape=jax.ShapeDtypeStruct((head_dims, columns), bf16),
        in_specs=[whole] * 9,
        out_specs=whole,
        compiler_params=pltpu.CompilerParams(vmem_limit_bytes=40 * 1024 * 1024),
        name="finish",
    )(feats, total, part, stats, other, mass, part_mass, nodes, bias)


def solution(mesh):
    return jax.shard_map(
        local,
        mesh=mesh,
        in_specs=(
            P("mp", "dp"),
            P("mp", None),
            P("mp"),
            P("mp"),
            P("mp"),
            P("dp"),
            P("dp"),
            P("dp", None, None),
        ),
        out_specs=P("mp", "dp"),
        check_vma=False,
    )
```

```python
import functools
import math

import jax
import jax.numpy as jnp
from jax import lax
from jax.experimental import pallas as pl
from jax.experimental.pallas import tpu as pltpu
from jax.sharding import PartitionSpec as P

HD = 32
LOG2E = 1.4426950408889634
FAR_BELOW = -1e30
FLOOR = -1e9
CODE_BITS = 8
CODE = 1 << CODE_BITS
TOGETHER = 4
UNROLL = 32
VMEM = pltpu.VMEM
LANES = 128
MESH = pl.DeviceIdType.MESH


def leaky_relu(scores):
    return jnp.maximum(scores, 0.2 * scores)


def main_kernel(
    heads,
    capacity,
    chunks,
    depth,
    peers,
    weight_in,
    nodes_in,
    att_src_in,
    att_dst_in,
    bias_in,
    tiles_in,
    rows_in,
    cols_in,
    feats_ref,
    total_ref,
    part_ref,
    stats_ref,
    other_ref,
    mass_ref,
    part_mass_ref,
    nodes_ref,
    bias_ref,
    *scratch,
):
    (
        first_half,
        all_source,
        targ,
        all_nodes,
        masks_out,
        masks2,
        code_rows,
        codes_out,
        pick,
        got_codes,
        u_send,
        u_all,
        score_send,
        score_recv,
        table_v,
        table,
        weights,
        keeps,
        scales,
        bests,
        scan,
        part_send,
        mass_send,
        stats_send,
        node_send,
        node_recv,
        u_ss,
        u_rs,
        score_ss,
        score_rs,
        mask_ss,
        mask_rs,
        code_ss,
        code_rs,
        far_ss,
        facing_ss,
        core_ss,
        recv_sem,
        pair_ss,
        pair_rs,
        part_ss,
        part_rs,
        mass_ss,
        mass_rs,
        local_sem,
        pick_sem,
        load_sem,
        weight_ref,
        att_src_ref,
        att_dst_ref,
        tiles_ref,
        tile_rows,
        tile_cols,
    ) = scratch[: len(scratch) - heads]
    second_half = scratch[len(scratch) - heads :]

    devices = 4 * depth
    groups = depth // 2
    me = lax.axis_index("dp")
    core = lax.rem(me, 2)
    beside = lax.rem(lax.div(me, 2), 2)
    level = lax.div(me, 4)
    parity = lax.rem(level, 2)
    where_in = lax.div(level, 2)
    mine = lax.axis_index("mp")
    dims, columns = nodes_in.shape
    head_dims = weight_in.shape[0]
    size = LANES
    blocks = columns // size
    hb = blocks // 2
    per = blocks // chunks
    width = per * size
    slots = devices * capacity
    early = chunks // 2
    score_item = early
    items = early + 1 + heads

    def place(lev, b, c):
        return (lev * 2 + b) * 2 + c

    def origin_of(q, b, c):
        return (q * 2 + b) * 2 + c

    own = origin_of(where_in, beside, core)
    facing = place(level, 1 - beside, core)
    other_core = place(level, beside, 1 - core)
    pair = place(level + 1 - 2 * parity, beside, core)

    loads = [
        pltpu.make_async_copy(source, target, load_sem.at[number])
        for number, (source, target) in enumerate(
            (
                (weight_in, weight_ref),
                (att_src_in, att_src_ref),
                (att_dst_in, att_dst_ref),
                (nodes_in, nodes_ref),
                (rows_in, tile_rows),
                (cols_in, tile_cols),
                (tiles_in, tiles_ref),
                (bias_in, bias_ref),
            )
        )
    ]
    for load in loads:
        load.start()
    barrier = pltpu.get_barrier_semaphore()
    for shift in range(1, devices):
        pl.semaphore_signal(barrier, 1, device_id={"dp": lax.rem(me + shift, devices)}, device_id_type=MESH)
    for shift in range(1, peers):
        pl.semaphore_signal(barrier, 1, device_id={"mp": lax.rem(mine + shift, peers)}, device_id_type=MESH)

    own_rows = pl.ds(pl.multiple_of(mine * dims, dims), dims)

    def as_column(ref):
        row = ref[...]
        if head_dims < LANES:
            row = jnp.concatenate([row, jnp.zeros((1, LANES - head_dims), row.dtype)], axis=1)
        return jnp.transpose(jnp.concatenate([row] * 8, axis=0))[:head_dims, 0:1]

    for load in loads[:3]:
        load.wait()
    wide = weight_ref[...].astype(jnp.float32)
    by_source = wide * (LOG2E * as_column(att_src_ref))
    by_target = wide * (LOG2E * as_column(att_dst_ref))
    rows = []
    for scaled in (by_source, by_target):
        for head in range(heads):
            rows.append(jnp.sum(scaled[head * HD : (head + 1) * HD], axis=0, keepdims=True))
    reduced = jnp.concatenate(rows, axis=0)
    for peer in range(peers):
        u_send[peer] = reduced[:, peer * dims : (peer + 1) * dims]
    u_all[mine] = u_send[mine]
    for load in loads[3:]:
        load.wait()
    pl.semaphore_wait(barrier, devices - 1 + peers - 1)

    def node_copy(shift, chunk):
        return pltpu.make_async_remote_copy(
            src_ref=nodes_ref.at[:, pl.ds(chunk * width, width)],
            dst_ref=all_nodes.at[chunk, own_rows, :],
            send_sem=node_send.at[shift - 1, chunk],
            recv_sem=node_recv.at[shift - 1, chunk],
            device_id={"mp": lax.rem(mine + shift, peers)},
            device_id_type=MESH,
        )

    def u_copy(shift):
        to = lax.rem(mine + shift, peers)
        return pltpu.make_async_remote_copy(
            src_ref=u_send.at[to],
            dst_ref=u_all.at[mine],
            send_sem=u_ss.at[shift - 1],
            recv_sem=u_rs.at[shift - 1],
            device_id={"mp": to},
            device_id_type=MESH,
        )

    def score_copy(shift, side):
        to = lax.rem(mine + shift, peers)
        return pltpu.make_async_remote_copy(
            src_ref=score_send.at[side, to],
            dst_ref=score_recv.at[side, mine],
            send_sem=score_ss.at[side, shift - 1],
            recv_sem=score_rs.at[side, shift - 1],
            device_id={"mp": to},
            device_id_type=MESH,
        )

    def mask_copy(shift):
        to = lax.rem(me + shift, devices)
        return pltpu.make_async_remote_copy(
            src_ref=masks_out.at[pl.ds(to * capacity, capacity)],
            dst_ref=masks2.at[pl.ds(me * capacity, capacity)],
            send_sem=mask_ss.at[shift - 1],
            recv_sem=mask_rs.at[shift - 1],
            device_id={"dp": to},
            device_id_type=MESH,
        )

    def code_copy(shift):
        to = lax.rem(me + shift, devices)
        return pltpu.make_async_remote_copy(
            src_ref=codes_out,
            dst_ref=got_codes.at[me],
            send_sem=code_ss.at[shift - 1],
            recv_sem=code_rs.at[shift - 1],
            device_id={"dp": to},
            device_id_type=MESH,
        )

    def pair_copy(which):
        src, dst = (
            (masks2.at[pl.ds(0, slots)], masks2.at[pl.ds(slots, slots)]),
            (targ.at[pl.ds(blocks, blocks)], targ.at[pl.ds(0, blocks)]),
            (stats_send, other_ref),
        )[which]
        return pltpu.make_async_remote_copy(
            src_ref=src,
            dst_ref=dst,
            send_sem=pair_ss.at[which],
            recv_sem=pair_rs.at[which],
            device_id={"dp": pair},
            device_id_type=MESH,
        )

    def part_copy(head):
        return pltpu.make_async_remote_copy(
            src_ref=part_send.at[head],
            dst_ref=part_ref.at[head],
            send_sem=part_ss.at[head],
            recv_sem=part_rs.at[head],
            device_id={"dp": pair},
            device_id_type=MESH,
        )

    def mass_copy(head):
        return pltpu.make_async_remote_copy(
            src_ref=mass_send.at[head],
            dst_ref=part_mass_ref.at[head],
            send_sem=mass_ss.at[head],
            recv_sem=mass_rs.at[head],
            device_id={"dp": pair},
            device_id_type=MESH,
        )

    def item_ref(origin, item):
        if item < early:
            return first_half.at[pl.ds(origin * hb + item * per, per)]
        if item == score_item:
            return all_source.at[pl.ds(origin * blocks, blocks)]
        return second_half[item - score_item - 1].at[pl.ds(origin * hb, hb)]

    def send(origin, item, to, sem):
        part = item_ref(origin, item)
        return pltpu.make_async_remote_copy(
            src_ref=part,
            dst_ref=part,
            send_sem=sem,
            recv_sem=recv_sem.at[origin, item],
            device_id={"dp": to},
            device_id_type=MESH,
        )

    def far_copy(shift, item):
        to = place(2 * lax.rem(where_in + shift, groups) + parity, beside, core)
        return send(own, item, to, far_ss.at[shift - 1, item])

    def facing_copy(q, item):
        return send(origin_of(q, beside, core), item, facing, facing_ss.at[q, item])

    def core_copy(q, b, item):
        return send(origin_of(q, b, core), item, other_core, core_ss.at[q, b, item])

    def arrival(origin, item):
        send(origin, item, other_core, core_ss.at[0, 0, item]).wait_recv()

    def own_core(item):
        core_copy(where_in, beside, item).start()

    def own_far(item):
        for shift in range(1, groups):
            far_copy(shift, item).start()

    at_end = (level == 0) | (level == depth - 1)

    def far_if_end(item):
        pl.when(at_end)(lambda: own_far(item))

    def far_if_middle(item):
        pl.when(jnp.logical_not(at_end))(lambda: own_far(item))

    def own_facing(item):
        facing_copy(where_in, item).start()

    def own_out(item):
        own_far(item)
        own_near(item)

    def own_near(item):
        own_facing(item)
        own_core(item)

    def far_q(shift):
        return lax.rem(where_in + groups - shift, groups)

    def from_far(item):
        for shift in range(1, groups):
            q = far_q(shift)
            arrival(origin_of(q, beside, core), item)
            facing_copy(q, item).start()
            core_copy(q, beside, item).start()

    def from_facing(item):
        arrival(origin_of(where_in, 1 - beside, core), item)
        core_copy(where_in, 1 - beside, item).start()

    def from_facing_far(item):
        for shift in range(1, groups):
            q = far_q(shift)
            arrival(origin_of(q, 1 - beside, core), item)
            core_copy(q, 1 - beside, item).start()

    def from_core(item):
        for q in range(groups):
            for b in range(2):
                arrival(origin_of(q, b, 1 - core), item)

    def project(chunk):
        for shift in range(1, peers):
            node_copy(shift, chunk).wait_recv()
        projected = jnp.dot(weight_ref[...], all_nodes[chunk], preferred_element_type=jnp.float32)
        rounded = projected.astype(jnp.bfloat16)
        for j in range(per):
            block = chunk * per + j
            span = slice(j * size, (j + 1) * size)
            feats_ref[block] = rounded[:, span]
            if chunk < early:
                first_half[own * hb + block] = rounded[:, span]
            else:
                for head in range(heads):
                    second_half[head][own * hb + block - hb] = rounded[head * HD : (head + 1) * HD, span]

    for shift in range(1, peers):
        u_copy(shift).start()
    for shift in range(1, peers):
        node_copy(shift, 0).start()

    tile_count = tile_rows.shape[0]
    owners = [lax.div(tile_rows[t], blocks) for t in range(tile_count)]
    lane = lax.broadcasted_iota(jnp.int32, (1, LANES), 1)
    packed = jnp.zeros((1, LANES), jnp.int32)
    tile_at = jnp.zeros((1, LANES), jnp.int32)
    for t in range(tile_count):
        turn = jnp.int32(0)
        for earlier in range(t):
            turn = turn + jnp.where(owners[earlier] == owners[t], 1, 0)
        row, column = tile_rows[t], tile_cols[t]
        column_owner = lax.div(column, blocks)
        column_level = lax.div(column_owner, 4)
        group = lax.div(column_level, 2) * 4 + lax.rem(column_owner, 4)
        code = (group * blocks + lax.rem(column, blocks)) * 2 + lax.rem(column_level, 2)
        code = code * CODE + row - owners[t] * blocks + 1
        at = lane == owners[t] * capacity + turn
        packed = jnp.where(at, code, packed)
        tile_at = jnp.where(at, t, tile_at)
    codes_out[...] = packed
    got_codes[me] = packed
    code_rows[0:1] = tile_at
    code_rows[1:8] = jnp.zeros((7, LANES), jnp.int32)
    fetch = pltpu.make_async_copy(code_rows, pick, pick_sem)
    fetch.start()
    for shift in range(1, devices):
        code_copy(shift).start()
    for chunk in range(chunks):
        all_nodes[chunk, own_rows, :] = nodes_ref[:, chunk * width : (chunk + 1) * width]
    fetch.wait()
    for slot in range(slots):
        masks_out[slot] = tiles_ref[pick[0, slot]]
    masks2[pl.ds(me * capacity, capacity)] = masks_out[pl.ds(me * capacity, capacity)]
    for shift in range(1, devices):
        mask_copy(shift).start()

    for shift in range(1, peers):
        u_copy(shift).wait_recv()
    stacked = jnp.concatenate([u_all[peer] for peer in range(peers)], axis=0)
    high = stacked.astype(jnp.bfloat16)
    rest = stacked - high.astype(jnp.float32)
    middle = rest.astype(jnp.bfloat16)
    low = (rest - middle.astype(jnp.float32)).astype(jnp.bfloat16)
    pieces = jnp.concatenate([high, middle, low], axis=0)
    count = 2 * heads * peers
    scored = jnp.dot(pieces, nodes_ref[...], preferred_element_type=jnp.float32)
    scored = scored[:count] + scored[count : 2 * count] + scored[2 * count :]
    for side in range(2):
        for peer in range(peers):
            at = (2 * peer + side) * heads
            score_send[side, peer] = scored[at : at + heads]
        score_recv[side, mine] = score_send[side, mine]
        for shift in range(1, peers):
            score_copy(shift, side).start()
    for chunk in range(1, chunks):
        for shift in range(1, peers):
            node_copy(shift, chunk).start()

    def added(side):
        for shift in range(1, peers):
            score_copy(shift, side).wait_recv()
        scores = score_recv[side, 0]
        for peer in range(1, peers):
            scores = scores + score_recv[side, peer]
        return scores

    project(0)
    far_if_middle(0)
    source_scores = added(0)
    for block in range(blocks):
        span = slice(block * size, (block + 1) * size)
        all_source[own * blocks + block] = source_scores[:, span]
    own_out(score_item)
    own_near(0)
    target_scores = added(1)
    for block in range(blocks):
        span = slice(block * size, (block + 1) * size)
        targ[blocks + block] = target_scores[:, span]
        stats_ref[0, block] = leaky_relu(source_scores[:, span] + target_scores[:, span])
    pair_copy(1).start()
    far_if_end(0)

    def forward_masks():
        for shift in range(1, devices):
            mask_copy(shift).wait_recv()
        pair_copy(0).start()

    def order():
        for shift in range(1, devices):
            code_copy(shift).wait_recv()
        lane = lax.broadcasted_iota(jnp.int32, (1, LANES), 1)
        bits = blocks.bit_length() - 1
        for which, holder in enumerate((pair, me)):
            codes = jnp.zeros((1, LANES), jnp.int32)
            for device in range(devices):
                turn = lax.rem((device - holder) * capacity + devices * LANES, LANES)
                moved = pltpu.roll(got_codes[device], turn, 1)
                here = (lane >= device * capacity) & (lane < (device + 1) * capacity)
                codes = jnp.where(here, moved, codes)
            row = jnp.bitwise_and(codes, CODE - 1)
            column_parity = jnp.bitwise_and(jnp.right_shift(codes, CODE_BITS), 1)
            column = jnp.right_shift(codes, CODE_BITS + 1)
            block = jnp.bitwise_and(column, blocks - 1)
            late = jnp.right_shift(block, bits - 1)
            spot = jnp.right_shift(column, bits) * hb + jnp.bitwise_and(block, hb - 1)
            lanes = LANES
            key = jnp.where((row > 0) & (column_parity == parity), row - 1, blocks)
            turned = jnp.transpose(jnp.concatenate([key, column, spot, late] + [key] * 4, axis=0))
            key_t = turned[:, 0:1]
            column_t = turned[:, 1:2]
            spot_t = turned[:, 2:3]
            late_t = turned[:, 3:4]
            along = lax.broadcasted_iota(jnp.int32, (lanes, lanes), 1)
            down = lax.broadcasted_iota(jnp.int32, (lanes, lanes), 0)
            before = (key_t < key) | ((key_t == key) & (down < along))
            rank = jnp.sum(jnp.where(before, 1, 0), axis=0, keepdims=True)
            rank_t = jnp.transpose(jnp.concatenate([rank] * 8, axis=0))[:, 0:1]
            at = rank_t == along
            slot = jnp.sum(jnp.where(at, down, 0), axis=0, keepdims=True)
            table_v[which, 0:1] = (1 - which) * slots + jnp.minimum(slot, slots - 1)
            table_v[which, 1:2] = jnp.sum(jnp.where(at, key_t, 0), axis=0, keepdims=True)
            table_v[which, 2:3] = jnp.sum(jnp.where(at, column_t, 0), axis=0, keepdims=True)
            table_v[which, 3:4] = jnp.sum(jnp.where(key_t <= along, 1, 0), axis=0, keepdims=True)
            table_v[which, 4:5] = jnp.sum(jnp.where(at, spot_t, 0), axis=0, keepdims=True)
            table_v[which, 5:6] = jnp.sum(jnp.where(at, late_t, 0), axis=0, keepdims=True)
            table_v[which, 6:8] = jnp.zeros((2, lanes), jnp.int32)
        table_copy().start()

    def table_copy():
        return pltpu.make_async_copy(table_v, table, local_sem)

    words = size // 32
    to_sign = 31 - lax.broadcasted_iota(jnp.int32, (32, size), 0)

    def partial(which, k):
        slot = table[which, 0, k]
        key = table[which, 1, k]
        column = table[which, 2, k]
        packed = masks2[slot] * jnp.where(key < blocks, 1, 0)
        edges = jnp.concatenate(
            [
                jnp.left_shift(packed[word : word + 1, :], to_sign)
                for word in range(words)
            ],
            axis=0,
        ) < 0
        source = all_source[column]
        source = jnp.transpose(jnp.concatenate([source] * (8 // heads), axis=0))
        target = targ[which * blocks + jnp.minimum(key, blocks - 1)]
        peaks = []
        for head in range(heads):
            one = slice(head, head + 1)
            here = jnp.where(edges, source[:, one], FAR_BELOW)
            aim = target[one]
            peak = leaky_relu(aim + jnp.max(here, axis=0, keepdims=True))
            peak = jnp.maximum(peak, FLOOR)
            weight = jnp.exp2(leaky_relu(here + aim) - peak)
            peaks.append(peak)
            weights[which * slots + k, head] = weight.astype(jnp.bfloat16)
        same = (k > 0) & (key == table[which, 1, jnp.maximum(k - 1, 0)])
        return same, jnp.concatenate(peaks, axis=0)

    together = math.gcd(slots, TOGETHER)
    turns = math.gcd(slots, 4) // together
    steps = slots // (together * turns)

    def weigh(which, index, run):
        parts = [(index * together + w, partial(which, index * together + w)) for w in range(together)]
        for k, (same, peak) in parts:
            again = jnp.where(same, 1.0, 0.0)
            old = jnp.where(same, run, FLOOR)
            run = jnp.maximum(old, peak)
            spot = which * slots + k
            keeps[spot] = jnp.exp2(old - run) * again
            scales[spot] = jnp.exp2(peak - run)
            bests[spot] = run
        return run

    def fresh():
        return jnp.full((heads, size), FLOOR, jnp.float32)

    ones = jnp.ones((16, size), jnp.bfloat16)

    def multiply(which, head, first, unroll, total):
        rows = slice(head * HD, (head + 1) * HD)
        one = slice(head, head + 1)
        values = []
        for w in range(unroll):
            spot = table[which, 4, first + w]
            late = table[which, 5, first + w]
            feats = jnp.where(late == 0, first_half[spot, rows], second_half[head][spot])
            feats = jnp.concatenate([feats, ones], axis=0)
            values.append(
                jnp.dot(feats, weights[which * slots + first + w, head], preferred_element_type=jnp.float32)
            )
        for w in range(unroll):
            spot = which * slots + first + w
            total = total * keeps[spot, one] + values[w][: HD + 8] * scales[spot, one]
            scan[first + w] = total
        return total

    def ending(which, key):
        upto = table[which, 3, key]
        prior = table[which, 3, key - 1] if key > 0 else 0
        return jnp.maximum(upto - 1, 0), upto > prior

    def play(events):
        for what, item in events:
            what(item)

    first = score_item + 1
    standard = early == 4 and heads == 4 and chunks == 8 and steps == 16

    def near_weights(count, state):
        at, carry = state
        body = functools.partial(weigh, 0)
        return at + count, lax.fori_loop(at * turns, (at + count) * turns, body, carry)

    def own_weights(count, state):
        at, carry = state
        body = functools.partial(weigh, 1)
        return at + count, lax.fori_loop(at * turns, (at + count) * turns, body, carry)

    def near_values(head):
        from_core(first + head)

        def body(index, total):
            return multiply(0, head, index * unroll, unroll, total)

        lax.fori_loop(0, slots // unroll, body, jnp.zeros((HD + 8, size), jnp.float32))
        for block in range(blocks):
            index, some = ending(0, block)
            found = jnp.where(some, scan[index], 0.0)
            part_send[head, block] = found[:HD].astype(jnp.bfloat16)
            mass_send[head, block : block + 1] = found[HD : HD + 1]
        part_copy(head).start()
        mass_copy(head).start()

    def own_values(head):
        def body(index, total):
            return multiply(1, head, index * unroll, unroll, total)

        lax.fori_loop(0, slots // unroll, body, jnp.zeros((HD + 8, size), jnp.float32))
        for block in range(blocks):
            index, some = ending(1, block)
            found = jnp.where(some, scan[index], 0.0)
            total_ref[head, block] = found[:HD]
            mass_ref[head, block : block + 1] = found[HD : HD + 1]

    def near_stats():
        for block in range(blocks):
            index, some = ending(0, block)
            stats_send[block] = jnp.where(some, bests[index], FLOOR)
        pair_copy(2).start()

    def ready_to_weigh():
        table_copy().wait()
        from_core(score_item)
        pair_copy(1).wait_recv()
        pair_copy(0).wait_recv()

    unroll = math.gcd(slots, UNROLL)
    near = (0, fresh())
    mine_state = (0, fresh())
    if standard:
        project(1)
        far_if_middle(1)
        own_near(1)
        forward_masks()
        order()
        project(2)
        from_facing(score_item)
        far_if_middle(2)
        far_if_end(1)
        own_near(2)
        from_far(score_item)
        project(3)
        far_if_middle(3)
        own_near(3)
        project(4)
        far_if_end(2)
        from_facing_far(score_item)
        project(5)
        far_if_end(3)
        from_far(0)
        ready_to_weigh()
        near = near_weights(1, near)
        project(6)
        near = near_weights(1, near)
        project(7)
        for head in range(heads):
            far_if_middle(first + head)
            own_core(first + head)
        own_facing(first)
        far_if_end(first)
        near = near_weights(4, near)
        play([(far_if_end, first + 1), (from_far, 1)])
        near = near_weights(2, near)
        play([(from_far, 2)])
        near = near_weights(3, near)
        play([(far_if_end, first + 2), (from_far, 3)])
        play([(from_facing, 0), (from_facing, 1), (from_facing, 2), (from_facing, 3)])
        near = near_weights(3, near)
        play([(from_far, first), (own_facing, first + 1), (far_if_end, first + 3)])
        near = near_weights(2, near)
        near_stats()
        play([(own_facing, first + 2), (from_facing, first), (from_facing_far, 0), (from_facing_far, 1)])
        mine_state = own_weights(2, mine_state)
        play([(from_facing_far, 2), (from_facing_far, 3)])
        mine_state = own_weights(2, mine_state)
        play([(from_far, first + 1), (own_facing, first + 3)])
        mine_state = own_weights(1, mine_state)
        play([(from_facing_far, first)])
        mine_state = own_weights(2, mine_state)
        for item in range(early):
            from_core(item)
        near_values(0)
        play([(from_far, first + 2), (from_facing, first + 1)])
        mine_state = own_weights(1, mine_state)
        play([(from_facing_far, first + 1)])
        mine_state = own_weights(2, mine_state)
        play([(from_far, first + 3)])
        near_values(1)
        play([(from_facing, first + 2), (from_facing_far, first + 2)])
        mine_state = own_weights(2, mine_state)
        near_values(2)
        play([(from_facing, first + 3), (from_facing_far, first + 3)])
        mine_state = own_weights(1, mine_state)
        near_values(3)
        mine_state = own_weights(3, mine_state)
        for head in range(heads):
            own_values(head)
    else:
        for chunk in range(1, chunks):
            project(chunk)
            if chunk < early:
                own_out(chunk)
        forward_masks()
        order()
        for head in range(heads):
            own_out(first + head)
        for item in [score_item] + [i for i in range(items) if i != score_item]:
            play([(from_facing, item), (from_far, item), (from_facing_far, item)])
        ready_to_weigh()
        near = near_weights(steps, near)
        near_stats()
        mine_state = own_weights(steps, mine_state)
        for item in range(early):
            from_core(item)
        for head in range(heads):
            near_values(head)
            own_values(head)

    for block in range(blocks):
        index, some = ending(1, block)
        stats_ref[1, block] = jnp.where(some, bests[slots + index], FLOOR)
    for shift in range(1, peers):
        u_copy(shift).wait_send()
        for side in range(2):
            score_copy(shift, side).wait_send()
        for chunk in range(chunks):
            node_copy(shift, chunk).wait_send()
    for shift in range(1, devices):
        code_copy(shift).wait_send()
        mask_copy(shift).wait_send()
    for item in range(items):
        for shift in range(1, groups):
            far_copy(shift, item).wait_send()
        for q in range(groups):
            facing_copy(q, item).wait_send()
            for b in range(2):
                core_copy(q, b, item).wait_send()
    for which in range(3):
        pair_copy(which).wait_send()
    pair_copy(2).wait_recv()
    for head in range(heads):
        part_copy(head).wait()
        mass_copy(head).wait()


def finish_kernel(
    heads,
    feats_ref,
    total_ref,
    part_ref,
    stats_ref,
    other_ref,
    mass_ref,
    part_mass_ref,
    nodes_ref,
    bias_ref,
    out_ref,
):
    blocks = feats_ref.shape[0]
    size = LANES
    row = bias_ref[...]
    width = row.shape[1]
    if width < LANES:
        row = jnp.concatenate([row, jnp.zeros((1, LANES - width), row.dtype)], axis=1)
    bias = jnp.transpose(jnp.concatenate([row] * 8, axis=0))[:width, 0:1]
    for block in range(blocks):
        span = slice(block * size, (block + 1) * size)
        itself = stats_ref[0, block]
        here = stats_ref[1, block]
        there = other_ref[block]
        mass = jnp.concatenate([mass_ref[head, block : block + 1] for head in range(heads)], axis=0)
        part_mass = jnp.concatenate([part_mass_ref[head, block : block + 1] for head in range(heads)], axis=0)
        best = jnp.maximum(jnp.maximum(itself, here), there)
        alone = jnp.exp2(itself - best)
        near = jnp.exp2(here - best)
        away = jnp.exp2(there - best)
        shared = 1.0 / (alone + near * mass + away * part_mass)
        alone = alone * shared
        near = near * shared
        away = away * shared
        for head in range(heads):
            rows = slice(head * HD, (head + 1) * HD)
            one = slice(head, head + 1)
            flat = (
                total_ref[head, block] * near[one]
                + part_ref[head, block].astype(jnp.float32) * away[one]
                + feats_ref[block, rows].astype(jnp.float32) * alone[one]
                + nodes_ref[rows, span].astype(jnp.float32)
                + bias[rows]
            )
            out_ref[rows, span] = jnp.where(flat > 0, flat, jnp.exp(flat) - 1.0).astype(out_ref.dtype)


def local(node_feats, proj_weight, att_src, att_dst, out_bias, tile_rows, tile_cols, tile_masks):
    dims, columns = node_feats.shape
    head_dims, inputs = proj_weight.shape
    heads = head_dims // HD
    size = tile_masks.shape[2]
    words = tile_masks.shape[1]
    blocks = columns // size
    devices = lax.axis_size("dp")
    peers = lax.axis_size("mp")
    capacity = max(2, 2 * tile_rows.shape[0] // devices)
    depth = devices // 4
    groups = depth // 2
    origins = groups * 4
    chunks = math.gcd(blocks, max(2, 128 // devices))
    early = chunks // 2
    items = early + 1 + heads
    slots = devices * capacity
    positions = 2 * slots
    hb = blocks // 2
    whole = pl.BlockSpec(memory_space=VMEM)
    smem = pltpu.SMEM
    dma = pltpu.SemaphoreType.DMA
    f32 = jnp.float32
    bf16 = jnp.bfloat16
    others = max(1, peers - 1)
    feats, total, part, stats, other, mass, part_mass, nodes, bias = pl.pallas_call(
        functools.partial(main_kernel, heads, capacity, chunks, depth, peers),
        out_shape=(
            jax.ShapeDtypeStruct((blocks, head_dims, size), bf16),
            jax.ShapeDtypeStruct((heads, blocks, HD, size), f32),
            jax.ShapeDtypeStruct((heads, blocks, HD, size), bf16),
            jax.ShapeDtypeStruct((2, blocks, heads, size), f32),
            jax.ShapeDtypeStruct((blocks, heads, size), f32),
            jax.ShapeDtypeStruct((heads, blocks, size), f32),
            jax.ShapeDtypeStruct((heads, blocks, size), f32),
            jax.ShapeDtypeStruct((dims, columns), bf16),
            jax.ShapeDtypeStruct((1, head_dims), f32),
        ),
        in_specs=[pl.BlockSpec(memory_space=pltpu.HBM)] * 8,
        out_specs=(whole,) * 9,
        scratch_shapes=[
            VMEM((origins * hb, head_dims, size), bf16),
            VMEM((origins * blocks, heads, size), f32),
            VMEM((2 * blocks, heads, size), f32),
            VMEM((chunks, inputs, columns // chunks), bf16),
            VMEM((slots, words, size), jnp.int32),
            VMEM((2 * slots, words, size), jnp.int32),
            VMEM((8, LANES), jnp.int32),
            VMEM((1, LANES), jnp.int32),
            smem((8, LANES), jnp.int32),
            VMEM((devices, 1, LANES), jnp.int32),
            VMEM((peers, 2 * heads, dims), f32),
            VMEM((peers, 2 * heads, dims), f32),
            VMEM((2, peers, heads, columns), f32),
            VMEM((2, peers, heads, columns), f32),
            VMEM((2, 8, LANES), jnp.int32),
            smem((2, 8, LANES), jnp.int32),
            VMEM((positions, heads, size, size), bf16),
            VMEM((positions, heads, size), f32),
            VMEM((positions, heads, size), f32),
            VMEM((positions, heads, size), f32),
            VMEM((slots, HD + 8, size), f32),
            VMEM((heads, blocks, HD, size), bf16),
            VMEM((heads, blocks, size), f32),
            VMEM((blocks, heads, size), f32),
            dma((others, chunks)),
            dma((others, chunks)),
            dma((others,)),
            dma((others,)),
            dma((2, others)),
            dma((2, others)),
            dma((devices - 1,)),
            dma((devices - 1,)),
            dma((devices - 1,)),
            dma((devices - 1,)),
            dma((max(1, groups - 1), items)),
            dma((groups, items)),
            dma((groups, 2, items)),
            dma((origins, items)),
            dma((3,)),
            dma((3,)),
            dma((heads,)),
            dma((heads,)),
            dma((heads,)),
            dma((heads,)),
            dma,
            dma,
            dma((8,)),
            VMEM((head_dims, inputs), bf16),
            VMEM((1, head_dims), f32),
            VMEM((1, head_dims), f32),
            VMEM(tile_masks.shape, jnp.int32),
            smem(tile_rows.shape, jnp.int32),
            smem(tile_cols.shape, jnp.int32),
        ]
        + [VMEM((origins * hb, HD, size), bf16) for _ in range(heads)],
        compiler_params=pltpu.CompilerParams(
            collective_id=0, has_side_effects=True, vmem_limit_bytes=48 * 1024 * 1024
        ),
        name="graph",
    )(
        *[
            pltpu.with_memory_space_constraint(x, pltpu.HBM)
            for x in (
                proj_weight,
                node_feats,
                att_src.reshape(1, head_dims),
                att_dst.reshape(1, head_dims),
                out_bias.reshape(1, head_dims),
                tile_masks,
                tile_rows,
                tile_cols,
            )
        ]
    )
    return pl.pallas_call(
        functools.partial(finish_kernel, heads),
        out_shape=jax.ShapeDtypeStruct((head_dims, columns), bf16),
        in_specs=[whole] * 9,
        out_specs=whole,
        compiler_params=pltpu.CompilerParams(vmem_limit_bytes=40 * 1024 * 1024),
        name="finish",
    )(feats, total, part, stats, other, mass, part_mass, nodes, bias)


def solution(mesh):
    return jax.shard_map(
        local,
        mesh=mesh,
        in_specs=(
            P("mp", "dp"),
            P("mp", None),
            P("mp"),
            P("mp"),
            P("mp"),
            P("dp"),
            P("dp"),
            P("dp", None, None),
        ),
        out_specs=P("mp", "dp"),
        check_vma=False,
    )
```

```python
import functools
import math

import jax
import jax.numpy as jnp
from jax import lax
from jax.experimental import pallas as pl
from jax.experimental.pallas import tpu as pltpu
from jax.sharding import PartitionSpec as P

HD = 32
LOG2E = 1.4426950408889634
FAR_BELOW = -1e30
FLOOR = -1e9
CODE_BITS = 8
CODE = 1 << CODE_BITS
TOGETHER = 4
UNROLL = 64
VMEM = pltpu.VMEM
LANES = 128
MESH = pl.DeviceIdType.MESH


def leaky_relu(scores):
    return jnp.maximum(scores, 0.2 * scores)


def main_kernel(
    heads,
    capacity,
    chunks,
    depth,
    peers,
    weight_in,
    nodes_in,
    att_src_in,
    att_dst_in,
    bias_in,
    tiles_in,
    rows_in,
    cols_in,
    feats_ref,
    total_ref,
    part_ref,
    stats_ref,
    other_ref,
    mass_ref,
    part_mass_ref,
    nodes_ref,
    bias_ref,
    *scratch,
):
    (
        first_half,
        all_source,
        targ,
        all_nodes,
        masks_out,
        masks2,
        code_rows,
        codes_out,
        pick,
        got_codes,
        u_send,
        u_all,
        score_send,
        score_recv,
        table_v,
        table,
        weights,
        keeps,
        scales,
        bests,
        scan,
        part_send,
        mass_send,
        stats_send,
        node_send,
        node_recv,
        u_ss,
        u_rs,
        score_ss,
        score_rs,
        mask_ss,
        mask_rs,
        code_ss,
        code_rs,
        far_ss,
        facing_ss,
        core_ss,
        recv_sem,
        pair_ss,
        pair_rs,
        part_ss,
        part_rs,
        mass_ss,
        mass_rs,
        local_sem,
        pick_sem,
        load_sem,
        weight_ref,
        att_src_ref,
        att_dst_ref,
        tiles_ref,
        tile_rows,
        tile_cols,
    ) = scratch[: len(scratch) - heads]
    second_half = scratch[len(scratch) - heads :]

    devices = 4 * depth
    groups = depth // 2
    me = lax.axis_index("dp")
    core = lax.rem(me, 2)
    beside = lax.rem(lax.div(me, 2), 2)
    level = lax.div(me, 4)
    parity = lax.rem(level, 2)
    where_in = lax.div(level, 2)
    mine = lax.axis_index("mp")
    dims, columns = nodes_in.shape
    head_dims = weight_in.shape[0]
    size = LANES
    blocks = columns // size
    hb = blocks // 2
    per = blocks // chunks
    width = per * size
    slots = devices * capacity
    early = chunks // 2
    score_item = early
    items = early + 1 + heads

    def place(lev, b, c):
        return (lev * 2 + b) * 2 + c

    def origin_of(q, b, c):
        return (q * 2 + b) * 2 + c

    own = origin_of(where_in, beside, core)
    facing = place(level, 1 - beside, core)
    other_core = place(level, beside, 1 - core)
    pair = place(level + 1 - 2 * parity, beside, core)

    loads = [
        pltpu.make_async_copy(source, target, load_sem.at[number])
        for number, (source, target) in enumerate(
            (
                (weight_in, weight_ref),
                (att_src_in, att_src_ref),
                (att_dst_in, att_dst_ref),
                (nodes_in, nodes_ref),
                (rows_in, tile_rows),
                (cols_in, tile_cols),
                (tiles_in, tiles_ref),
                (bias_in, bias_ref),
            )
        )
    ]
    for load in loads:
        load.start()
    barrier = pltpu.get_barrier_semaphore()
    for shift in range(1, devices):
        pl.semaphore_signal(barrier, 1, device_id={"dp": lax.rem(me + shift, devices)}, device_id_type=MESH)
    for shift in range(1, peers):
        pl.semaphore_signal(barrier, 1, device_id={"mp": lax.rem(mine + shift, peers)}, device_id_type=MESH)

    own_rows = pl.ds(pl.multiple_of(mine * dims, dims), dims)

    def as_column(ref):
        row = ref[...]
        if head_dims < LANES:
            row = jnp.concatenate([row, jnp.zeros((1, LANES - head_dims), row.dtype)], axis=1)
        return jnp.transpose(jnp.concatenate([row] * 8, axis=0))[:head_dims, 0:1]

    for load in loads[:3]:
        load.wait()
    wide = weight_ref[...].astype(jnp.float32)
    by_source = wide * (LOG2E * as_column(att_src_ref))
    by_target = wide * (LOG2E * as_column(att_dst_ref))
    rows = []
    for scaled in (by_source, by_target):
        for head in range(heads):
            rows.append(jnp.sum(scaled[head * HD : (head + 1) * HD], axis=0, keepdims=True))
    reduced = jnp.concatenate(rows, axis=0)
    for peer in range(peers):
        u_send[peer] = reduced[:, peer * dims : (peer + 1) * dims]
    u_all[mine] = u_send[mine]
    for load in loads[3:]:
        load.wait()
    pl.semaphore_wait(barrier, devices - 1 + peers - 1)

    def node_copy(shift, chunk):
        return pltpu.make_async_remote_copy(
            src_ref=nodes_ref.at[:, pl.ds(chunk * width, width)],
            dst_ref=all_nodes.at[chunk, own_rows, :],
            send_sem=node_send.at[shift - 1, chunk],
            recv_sem=node_recv.at[shift - 1, chunk],
            device_id={"mp": lax.rem(mine + shift, peers)},
            device_id_type=MESH,
        )

    def u_copy(shift):
        to = lax.rem(mine + shift, peers)
        return pltpu.make_async_remote_copy(
            src_ref=u_send.at[to],
            dst_ref=u_all.at[mine],
            send_sem=u_ss.at[shift - 1],
            recv_sem=u_rs.at[shift - 1],
            device_id={"mp": to},
            device_id_type=MESH,
        )

    def score_copy(shift, side):
        to = lax.rem(mine + shift, peers)
        return pltpu.make_async_remote_copy(
            src_ref=score_send.at[side, to],
            dst_ref=score_recv.at[side, mine],
            send_sem=score_ss.at[side, shift - 1],
            recv_sem=score_rs.at[side, shift - 1],
            device_id={"mp": to},
            device_id_type=MESH,
        )

    def mask_copy(shift):
        to = lax.rem(me + shift, devices)
        return pltpu.make_async_remote_copy(
            src_ref=masks_out.at[pl.ds(to * capacity, capacity)],
            dst_ref=masks2.at[pl.ds(me * capacity, capacity)],
            send_sem=mask_ss.at[shift - 1],
            recv_sem=mask_rs.at[shift - 1],
            device_id={"dp": to},
            device_id_type=MESH,
        )

    def code_copy(shift):
        to = lax.rem(me + shift, devices)
        return pltpu.make_async_remote_copy(
            src_ref=codes_out,
            dst_ref=got_codes.at[me],
            send_sem=code_ss.at[shift - 1],
            recv_sem=code_rs.at[shift - 1],
            device_id={"dp": to},
            device_id_type=MESH,
        )

    def pair_copy(which):
        src, dst = (
            (masks2.at[pl.ds(0, slots)], masks2.at[pl.ds(slots, slots)]),
            (targ.at[pl.ds(blocks, blocks)], targ.at[pl.ds(0, blocks)]),
            (stats_send, other_ref),
        )[which]
        return pltpu.make_async_remote_copy(
            src_ref=src,
            dst_ref=dst,
            send_sem=pair_ss.at[which],
            recv_sem=pair_rs.at[which],
            device_id={"dp": pair},
            device_id_type=MESH,
        )

    def part_copy(head):
        return pltpu.make_async_remote_copy(
            src_ref=part_send.at[head],
            dst_ref=part_ref.at[head],
            send_sem=part_ss.at[head],
            recv_sem=part_rs.at[head],
            device_id={"dp": pair},
            device_id_type=MESH,
        )

    def mass_copy(head):
        return pltpu.make_async_remote_copy(
            src_ref=mass_send.at[head],
            dst_ref=part_mass_ref.at[head],
            send_sem=mass_ss.at[head],
            recv_sem=mass_rs.at[head],
            device_id={"dp": pair},
            device_id_type=MESH,
        )

    def item_ref(origin, item):
        if item < early:
            return first_half.at[pl.ds(origin * hb + item * per, per)]
        if item == score_item:
            return all_source.at[pl.ds(origin * blocks, blocks)]
        return second_half[item - score_item - 1].at[pl.ds(origin * hb, hb)]

    def send(origin, item, to, sem):
        part = item_ref(origin, item)
        return pltpu.make_async_remote_copy(
            src_ref=part,
            dst_ref=part,
            send_sem=sem,
            recv_sem=recv_sem.at[origin, item],
            device_id={"dp": to},
            device_id_type=MESH,
        )

    def far_copy(shift, item):
        to = place(2 * lax.rem(where_in + shift, groups) + parity, beside, core)
        return send(own, item, to, far_ss.at[shift - 1, item])

    def facing_copy(q, item):
        return send(origin_of(q, beside, core), item, facing, facing_ss.at[q, item])

    def core_copy(q, b, item):
        return send(origin_of(q, b, core), item, other_core, core_ss.at[q, b, item])

    def arrival(origin, item):
        send(origin, item, other_core, core_ss.at[0, 0, item]).wait_recv()

    def own_core(item):
        core_copy(where_in, beside, item).start()

    def own_far(item):
        for shift in range(1, groups):
            far_copy(shift, item).start()

    at_end = (level == 0) | (level == depth - 1)

    def far_if_end(item):
        pl.when(at_end)(lambda: own_far(item))

    def far_if_middle(item):
        pl.when(jnp.logical_not(at_end))(lambda: own_far(item))

    def own_facing(item):
        facing_copy(where_in, item).start()

    def own_out(item):
        own_far(item)
        own_near(item)

    def own_near(item):
        own_facing(item)
        own_core(item)

    def far_q(shift):
        return lax.rem(where_in + groups - shift, groups)

    def from_far(item):
        for shift in range(1, groups):
            q = far_q(shift)
            arrival(origin_of(q, beside, core), item)
            facing_copy(q, item).start()
            core_copy(q, beside, item).start()

    def from_facing(item):
        arrival(origin_of(where_in, 1 - beside, core), item)
        core_copy(where_in, 1 - beside, item).start()

    def from_facing_far(item):
        for shift in range(1, groups):
            q = far_q(shift)
            arrival(origin_of(q, 1 - beside, core), item)
            core_copy(q, 1 - beside, item).start()

    def from_core(item):
        for q in range(groups):
            for b in range(2):
                arrival(origin_of(q, b, 1 - core), item)

    def project(chunk):
        for shift in range(1, peers):
            node_copy(shift, chunk).wait_recv()
        projected = jnp.dot(weight_ref[...], all_nodes[chunk], preferred_element_type=jnp.float32)
        rounded = projected.astype(jnp.bfloat16)
        for j in range(per):
            block = chunk * per + j
            span = slice(j * size, (j + 1) * size)
            feats_ref[block] = rounded[:, span]
            if chunk < early:
                first_half[own * hb + block] = rounded[:, span]
            else:
                for head in range(heads):
                    second_half[head][own * hb + block - hb] = rounded[head * HD : (head + 1) * HD, span]

    for shift in range(1, peers):
        u_copy(shift).start()
    for shift in range(1, peers):
        node_copy(shift, 0).start()

    tile_count = tile_rows.shape[0]
    owners = [lax.div(tile_rows[t], blocks) for t in range(tile_count)]
    lane = lax.broadcasted_iota(jnp.int32, (1, LANES), 1)
    packed = jnp.zeros((1, LANES), jnp.int32)
    tile_at = jnp.zeros((1, LANES), jnp.int32)
    for t in range(tile_count):
        turn = jnp.int32(0)
        for earlier in range(t):
            turn = turn + jnp.where(owners[earlier] == owners[t], 1, 0)
        row, column = tile_rows[t], tile_cols[t]
        column_owner = lax.div(column, blocks)
        column_level = lax.div(column_owner, 4)
        group = lax.div(column_level, 2) * 4 + lax.rem(column_owner, 4)
        code = (group * blocks + lax.rem(column, blocks)) * 2 + lax.rem(column_level, 2)
        code = code * CODE + row - owners[t] * blocks + 1
        at = lane == owners[t] * capacity + turn
        packed = jnp.where(at, code, packed)
        tile_at = jnp.where(at, t, tile_at)
    codes_out[...] = packed
    got_codes[me] = packed
    code_rows[0:1] = tile_at
    code_rows[1:8] = jnp.zeros((7, LANES), jnp.int32)
    fetch = pltpu.make_async_copy(code_rows, pick, pick_sem)
    fetch.start()
    for shift in range(1, devices):
        code_copy(shift).start()
    for chunk in range(chunks):
        all_nodes[chunk, own_rows, :] = nodes_ref[:, chunk * width : (chunk + 1) * width]
    fetch.wait()
    for slot in range(slots):
        masks_out[slot] = tiles_ref[pick[0, slot]]
    masks2[pl.ds(me * capacity, capacity)] = masks_out[pl.ds(me * capacity, capacity)]
    for shift in range(1, devices):
        mask_copy(shift).start()

    for shift in range(1, peers):
        u_copy(shift).wait_recv()
    stacked = jnp.concatenate([u_all[peer] for peer in range(peers)], axis=0)
    high = stacked.astype(jnp.bfloat16)
    rest = stacked - high.astype(jnp.float32)
    middle = rest.astype(jnp.bfloat16)
    low = (rest - middle.astype(jnp.float32)).astype(jnp.bfloat16)
    pieces = jnp.concatenate([high, middle, low], axis=0)
    count = 2 * heads * peers
    scored = jnp.dot(pieces, nodes_ref[...], preferred_element_type=jnp.float32)
    scored = scored[:count] + scored[count : 2 * count] + scored[2 * count :]
    for side in range(2):
        for peer in range(peers):
            at = (2 * peer + side) * heads
            score_send[side, peer] = scored[at : at + heads]
        score_recv[side, mine] = score_send[side, mine]
        for shift in range(1, peers):
            score_copy(shift, side).start()
    for chunk in range(1, chunks):
        for shift in range(1, peers):
            node_copy(shift, chunk).start()

    def added(side):
        for shift in range(1, peers):
            score_copy(shift, side).wait_recv()
        scores = score_recv[side, 0]
        for peer in range(1, peers):
            scores = scores + score_recv[side, peer]
        return scores

    project(0)
    far_if_middle(0)
    source_scores = added(0)
    for block in range(blocks):
        span = slice(block * size, (block + 1) * size)
        all_source[own * blocks + block] = source_scores[:, span]
    own_out(score_item)
    own_near(0)
    target_scores = added(1)
    for block in range(blocks):
        span = slice(block * size, (block + 1) * size)
        targ[blocks + block] = target_scores[:, span]
        stats_ref[0, block] = leaky_relu(source_scores[:, span] + target_scores[:, span])
    pair_copy(1).start()
    far_if_end(0)

    def forward_masks():
        for shift in range(1, devices):
            mask_copy(shift).wait_recv()
        pair_copy(0).start()

    def order():
        for shift in range(1, devices):
            code_copy(shift).wait_recv()
        lane = lax.broadcasted_iota(jnp.int32, (1, LANES), 1)
        bits = blocks.bit_length() - 1
        for which, holder in enumerate((pair, me)):
            codes = jnp.zeros((1, LANES), jnp.int32)
            for device in range(devices):
                turn = lax.rem((device - holder) * capacity + devices * LANES, LANES)
                moved = pltpu.roll(got_codes[device], turn, 1)
                here = (lane >= device * capacity) & (lane < (device + 1) * capacity)
                codes = jnp.where(here, moved, codes)
            row = jnp.bitwise_and(codes, CODE - 1)
            column_parity = jnp.bitwise_and(jnp.right_shift(codes, CODE_BITS), 1)
            column = jnp.right_shift(codes, CODE_BITS + 1)
            block = jnp.bitwise_and(column, blocks - 1)
            late = jnp.right_shift(block, bits - 1)
            spot = jnp.right_shift(column, bits) * hb + jnp.bitwise_and(block, hb - 1)
            lanes = LANES
            key = jnp.where((row > 0) & (column_parity == parity), row - 1, blocks)
            turned = jnp.transpose(jnp.concatenate([key, column, spot, late] + [key] * 4, axis=0))
            key_t = turned[:, 0:1]
            column_t = turned[:, 1:2]
            spot_t = turned[:, 2:3]
            late_t = turned[:, 3:4]
            along = lax.broadcasted_iota(jnp.int32, (lanes, lanes), 1)
            down = lax.broadcasted_iota(jnp.int32, (lanes, lanes), 0)
            before = (key_t < key) | ((key_t == key) & (down < along))
            rank = jnp.sum(jnp.where(before, 1, 0), axis=0, keepdims=True)
            rank_t = jnp.transpose(jnp.concatenate([rank] * 8, axis=0))[:, 0:1]
            at = rank_t == along
            slot = jnp.sum(jnp.where(at, down, 0), axis=0, keepdims=True)
            table_v[which, 0:1] = (1 - which) * slots + jnp.minimum(slot, slots - 1)
            table_v[which, 1:2] = jnp.sum(jnp.where(at, key_t, 0), axis=0, keepdims=True)
            table_v[which, 2:3] = jnp.sum(jnp.where(at, column_t, 0), axis=0, keepdims=True)
            table_v[which, 3:4] = jnp.sum(jnp.where(key_t <= along, 1, 0), axis=0, keepdims=True)
            table_v[which, 4:5] = jnp.sum(jnp.where(at, spot_t, 0), axis=0, keepdims=True)
            table_v[which, 5:6] = jnp.sum(jnp.where(at, late_t, 0), axis=0, keepdims=True)
            table_v[which, 6:8] = jnp.zeros((2, lanes), jnp.int32)
        table_copy().start()

    def table_copy():
        return pltpu.make_async_copy(table_v, table, local_sem)

    words = size // 32
    to_sign = 31 - lax.broadcasted_iota(jnp.int32, (32, size), 0)

    def partial(which, k):
        slot = table[which, 0, k]
        key = table[which, 1, k]
        column = table[which, 2, k]
        packed = masks2[slot] * jnp.where(key < blocks, 1, 0)
        edges = jnp.concatenate(
            [
                jnp.left_shift(packed[word : word + 1, :], to_sign)
                for word in range(words)
            ],
            axis=0,
        ) < 0
        source = all_source[column]
        source = jnp.transpose(jnp.concatenate([source] * (8 // heads), axis=0))
        target = targ[which * blocks + jnp.minimum(key, blocks - 1)]
        peaks = []
        for head in range(heads):
            one = slice(head, head + 1)
            here = jnp.where(edges, source[:, one], FAR_BELOW)
            aim = target[one]
            peak = leaky_relu(aim + jnp.max(here, axis=0, keepdims=True))
            peak = jnp.maximum(peak, FLOOR)
            weight = jnp.exp2(leaky_relu(here + aim) - peak)
            peaks.append(peak)
            weights[which * slots + k, head] = weight.astype(jnp.bfloat16)
        same = (k > 0) & (key == table[which, 1, jnp.maximum(k - 1, 0)])
        return same, jnp.concatenate(peaks, axis=0)

    together = math.gcd(slots, TOGETHER)
    turns = math.gcd(slots, 4) // together
    steps = slots // (together * turns)

    def weigh(which, index, run):
        parts = [(index * together + w, partial(which, index * together + w)) for w in range(together)]
        for k, (same, peak) in parts:
            again = jnp.where(same, 1.0, 0.0)
            old = jnp.where(same, run, FLOOR)
            run = jnp.maximum(old, peak)
            spot = which * slots + k
            keeps[spot] = jnp.exp2(old - run) * again
            scales[spot] = jnp.exp2(peak - run)
            bests[spot] = run
        return run

    def fresh():
        return jnp.full((heads, size), FLOOR, jnp.float32)

    ones = jnp.ones((16, size), jnp.bfloat16)

    def multiply(which, head, first, unroll, total):
        rows = slice(head * HD, (head + 1) * HD)
        one = slice(head, head + 1)
        values = []
        for w in range(unroll):
            spot = table[which, 4, first + w]
            late = table[which, 5, first + w]
            feats = jnp.where(late == 0, first_half[spot, rows], second_half[head][spot])
            feats = jnp.concatenate([feats, ones], axis=0)
            values.append(
                jnp.dot(feats, weights[which * slots + first + w, head], preferred_element_type=jnp.float32)
            )
        for w in range(unroll):
            spot = which * slots + first + w
            total = total * keeps[spot, one] + values[w][: HD + 8] * scales[spot, one]
            scan[first + w] = total
        return total

    def ending(which, key):
        upto = table[which, 3, key]
        prior = table[which, 3, key - 1] if key > 0 else 0
        return jnp.maximum(upto - 1, 0), upto > prior

    def play(events):
        for what, item in events:
            what(item)

    first = score_item + 1
    standard = early == 4 and heads == 4 and chunks == 8 and steps == 16

    def near_weights(count, state):
        at, carry = state
        body = functools.partial(weigh, 0)
        return at + count, lax.fori_loop(at * turns, (at + count) * turns, body, carry)

    def own_weights(count, state):
        at, carry = state
        body = functools.partial(weigh, 1)
        return at + count, lax.fori_loop(at * turns, (at + count) * turns, body, carry)

    def near_values(head):
        from_core(first + head)

        def body(index, total):
            return multiply(0, head, index * unroll, unroll, total)

        lax.fori_loop(0, slots // unroll, body, jnp.zeros((HD + 8, size), jnp.float32))
        for block in range(blocks):
            index, some = ending(0, block)
            found = jnp.where(some, scan[index], 0.0)
            part_send[head, block] = found[:HD].astype(jnp.bfloat16)
            mass_send[head, block : block + 1] = found[HD : HD + 1]
        part_copy(head).start()
        mass_copy(head).start()

    def own_values(head):
        def body(index, total):
            return multiply(1, head, index * unroll, unroll, total)

        lax.fori_loop(0, slots // unroll, body, jnp.zeros((HD + 8, size), jnp.float32))
        for block in range(blocks):
            index, some = ending(1, block)
            found = jnp.where(some, scan[index], 0.0)
            total_ref[head, block] = found[:HD]
            mass_ref[head, block : block + 1] = found[HD : HD + 1]

    def near_stats():
        for block in range(blocks):
            index, some = ending(0, block)
            stats_send[block] = jnp.where(some, bests[index], FLOOR)
        pair_copy(2).start()

    def ready_to_weigh():
        table_copy().wait()
        from_core(score_item)
        pair_copy(1).wait_recv()
        pair_copy(0).wait_recv()

    unroll = math.gcd(slots, UNROLL)
    near = (0, fresh())
    mine_state = (0, fresh())
    if standard:
        project(1)
        far_if_middle(1)
        own_near(1)
        forward_masks()
        order()
        project(2)
        from_facing(score_item)
        far_if_middle(2)
        far_if_end(1)
        own_near(2)
        from_far(score_item)
        project(3)
        far_if_middle(3)
        own_near(3)
        project(4)
        far_if_end(2)
        from_facing_far(score_item)
        project(5)
        far_if_end(3)
        from_far(0)
        ready_to_weigh()
        near = near_weights(1, near)
        project(6)
        near = near_weights(1, near)
        project(7)
        for head in range(heads):
            far_if_middle(first + head)
            own_core(first + head)
        own_facing(first)
        far_if_end(first)
        near = near_weights(4, near)
        play([(far_if_end, first + 1), (from_far, 1)])
        near = near_weights(2, near)
        play([(from_far, 2)])
        near = near_weights(3, near)
        play([(far_if_end, first + 2), (from_far, 3)])
        play([(from_facing, 0), (from_facing, 1), (from_facing, 2), (from_facing, 3)])
        near = near_weights(3, near)
        play([(from_far, first), (own_facing, first + 1), (far_if_end, first + 3)])
        near = near_weights(2, near)
        near_stats()
        play([(from_facing, first), (from_facing_far, 0), (from_facing_far, 1)])
        mine_state = own_weights(2, mine_state)
        play([(from_facing_far, 2), (from_facing_far, 3)])
        mine_state = own_weights(2, mine_state)
        play([(from_far, first + 1), (own_facing, first + 2)])
        mine_state = own_weights(1, mine_state)
        play([(from_facing_far, first)])
        mine_state = own_weights(1, mine_state)
        for item in range(early):
            from_core(item)
        near_values(0)
        play([(from_far, first + 2), (own_facing, first + 3), (from_facing, first + 1)])
        mine_state = own_weights(2, mine_state)
        play([(from_facing_far, first + 1)])
        mine_state = own_weights(2, mine_state)
        play([(from_far, first + 3)])
        near_values(1)
        play([(from_facing, first + 2), (from_facing_far, first + 2)])
        mine_state = own_weights(2, mine_state)
        near_values(2)
        play([(from_facing, first + 3), (from_facing_far, first + 3)])
        mine_state = own_weights(1, mine_state)
        near_values(3)
        mine_state = own_weights(3, mine_state)
        for head in range(heads):
            own_values(head)
    else:
        for chunk in range(1, chunks):
            project(chunk)
            if chunk < early:
                own_out(chunk)
        forward_masks()
        order()
        for head in range(heads):
            own_out(first + head)
        for item in [score_item] + [i for i in range(items) if i != score_item]:
            play([(from_facing, item), (from_far, item), (from_facing_far, item)])
        ready_to_weigh()
        near = near_weights(steps, near)
        near_stats()
        mine_state = own_weights(steps, mine_state)
        for item in range(early):
            from_core(item)
        for head in range(heads):
            near_values(head)
            own_values(head)

    for block in range(blocks):
        index, some = ending(1, block)
        stats_ref[1, block] = jnp.where(some, bests[slots + index], FLOOR)
    for shift in range(1, peers):
        u_copy(shift).wait_send()
        for side in range(2):
            score_copy(shift, side).wait_send()
        for chunk in range(chunks):
            node_copy(shift, chunk).wait_send()
    for shift in range(1, devices):
        code_copy(shift).wait_send()
        mask_copy(shift).wait_send()
    for item in range(items):
        for shift in range(1, groups):
            far_copy(shift, item).wait_send()
        for q in range(groups):
            facing_copy(q, item).wait_send()
            for b in range(2):
                core_copy(q, b, item).wait_send()
    for which in range(3):
        pair_copy(which).wait_send()
    pair_copy(2).wait_recv()
    for head in range(heads):
        part_copy(head).wait()
        mass_copy(head).wait()


def finish_kernel(
    heads,
    feats_ref,
    total_ref,
    part_ref,
    stats_ref,
    other_ref,
    mass_ref,
    part_mass_ref,
    nodes_ref,
    bias_ref,
    out_ref,
):
    blocks = feats_ref.shape[0]
    size = LANES
    row = bias_ref[...]
    width = row.shape[1]
    if width < LANES:
        row = jnp.concatenate([row, jnp.zeros((1, LANES - width), row.dtype)], axis=1)
    bias = jnp.transpose(jnp.concatenate([row] * 8, axis=0))[:width, 0:1]
    for block in range(blocks):
        span = slice(block * size, (block + 1) * size)
        itself = stats_ref[0, block]
        here = stats_ref[1, block]
        there = other_ref[block]
        mass = jnp.concatenate([mass_ref[head, block : block + 1] for head in range(heads)], axis=0)
        part_mass = jnp.concatenate([part_mass_ref[head, block : block + 1] for head in range(heads)], axis=0)
        best = jnp.maximum(jnp.maximum(itself, here), there)
        alone = jnp.exp2(itself - best)
        near = jnp.exp2(here - best)
        away = jnp.exp2(there - best)
        shared = 1.0 / (alone + near * mass + away * part_mass)
        alone = alone * shared
        near = near * shared
        away = away * shared
        for head in range(heads):
            rows = slice(head * HD, (head + 1) * HD)
            one = slice(head, head + 1)
            flat = (
                total_ref[head, block] * near[one]
                + part_ref[head, block].astype(jnp.float32) * away[one]
                + feats_ref[block, rows].astype(jnp.float32) * alone[one]
                + nodes_ref[rows, span].astype(jnp.float32)
                + bias[rows]
            )
            out_ref[rows, span] = jnp.where(flat > 0, flat, jnp.exp(flat) - 1.0).astype(out_ref.dtype)


def local(node_feats, proj_weight, att_src, att_dst, out_bias, tile_rows, tile_cols, tile_masks):
    dims, columns = node_feats.shape
    head_dims, inputs = proj_weight.shape
    heads = head_dims // HD
    size = tile_masks.shape[2]
    words = tile_masks.shape[1]
    blocks = columns // size
    devices = lax.axis_size("dp")
    peers = lax.axis_size("mp")
    capacity = max(2, 2 * tile_rows.shape[0] // devices)
    depth = devices // 4
    groups = depth // 2
    origins = groups * 4
    chunks = math.gcd(blocks, max(2, 128 // devices))
    early = chunks // 2
    items = early + 1 + heads
    slots = devices * capacity
    positions = 2 * slots
    hb = blocks // 2
    whole = pl.BlockSpec(memory_space=VMEM)
    smem = pltpu.SMEM
    dma = pltpu.SemaphoreType.DMA
    f32 = jnp.float32
    bf16 = jnp.bfloat16
    others = max(1, peers - 1)
    feats, total, part, stats, other, mass, part_mass, nodes, bias = pl.pallas_call(
        functools.partial(main_kernel, heads, capacity, chunks, depth, peers),
        out_shape=(
            jax.ShapeDtypeStruct((blocks, head_dims, size), bf16),
            jax.ShapeDtypeStruct((heads, blocks, HD, size), f32),
            jax.ShapeDtypeStruct((heads, blocks, HD, size), bf16),
            jax.ShapeDtypeStruct((2, blocks, heads, size), f32),
            jax.ShapeDtypeStruct((blocks, heads, size), f32),
            jax.ShapeDtypeStruct((heads, blocks, size), f32),
            jax.ShapeDtypeStruct((heads, blocks, size), f32),
            jax.ShapeDtypeStruct((dims, columns), bf16),
            jax.ShapeDtypeStruct((1, head_dims), f32),
        ),
        in_specs=[pl.BlockSpec(memory_space=pltpu.HBM)] * 8,
        out_specs=(whole,) * 9,
        scratch_shapes=[
            VMEM((origins * hb, head_dims, size), bf16),
            VMEM((origins * blocks, heads, size), f32),
            VMEM((2 * blocks, heads, size), f32),
            VMEM((chunks, inputs, columns // chunks), bf16),
            VMEM((slots, words, size), jnp.int32),
            VMEM((2 * slots, words, size), jnp.int32),
            VMEM((8, LANES), jnp.int32),
            VMEM((1, LANES), jnp.int32),
            smem((8, LANES), jnp.int32),
            VMEM((devices, 1, LANES), jnp.int32),
            VMEM((peers, 2 * heads, dims), f32),
            VMEM((peers, 2 * heads, dims), f32),
            VMEM((2, peers, heads, columns), f32),
            VMEM((2, peers, heads, columns), f32),
            VMEM((2, 8, LANES), jnp.int32),
            smem((2, 8, LANES), jnp.int32),
            VMEM((positions, heads, size, size), bf16),
            VMEM((positions, heads, size), f32),
            VMEM((positions, heads, size), f32),
            VMEM((positions, heads, size), f32),
            VMEM((slots, HD + 8, size), f32),
            VMEM((heads, blocks, HD, size), bf16),
            VMEM((heads, blocks, size), f32),
            VMEM((blocks, heads, size), f32),
            dma((others, chunks)),
            dma((others, chunks)),
            dma((others,)),
            dma((others,)),
            dma((2, others)),
            dma((2, others)),
            dma((devices - 1,)),
            dma((devices - 1,)),
            dma((devices - 1,)),
            dma((devices - 1,)),
            dma((max(1, groups - 1), items)),
            dma((groups, items)),
            dma((groups, 2, items)),
            dma((origins, items)),
            dma((3,)),
            dma((3,)),
            dma((heads,)),
            dma((heads,)),
            dma((heads,)),
            dma((heads,)),
            dma,
            dma,
            dma((8,)),
            VMEM((head_dims, inputs), bf16),
            VMEM((1, head_dims), f32),
            VMEM((1, head_dims), f32),
            VMEM(tile_masks.shape, jnp.int32),
            smem(tile_rows.shape, jnp.int32),
            smem(tile_cols.shape, jnp.int32),
        ]
        + [VMEM((origins * hb, HD, size), bf16) for _ in range(heads)],
        compiler_params=pltpu.CompilerParams(
            collective_id=0, has_side_effects=True, vmem_limit_bytes=48 * 1024 * 1024
        ),
        name="graph",
    )(
        *[
            pltpu.with_memory_space_constraint(x, pltpu.HBM)
            for x in (
                proj_weight,
                node_feats,
                att_src.reshape(1, head_dims),
                att_dst.reshape(1, head_dims),
                out_bias.reshape(1, head_dims),
                tile_masks,
                tile_rows,
                tile_cols,
            )
        ]
    )
    return pl.pallas_call(
        functools.partial(finish_kernel, heads),
        out_shape=jax.ShapeDtypeStruct((head_dims, columns), bf16),
        in_specs=[whole] * 9,
        out_specs=whole,
        compiler_params=pltpu.CompilerParams(vmem_limit_bytes=40 * 1024 * 1024),
        name="finish",
    )(feats, total, part, stats, other, mass, part_mass, nodes, bias)


def solution(mesh):
    return jax.shard_map(
        local,
        mesh=mesh,
        in_specs=(
            P("mp", "dp"),
            P("mp", None),
            P("mp"),
            P("mp"),
            P("mp"),
            P("dp"),
            P("dp"),
            P("dp", None, None),
        ),
        out_specs=P("mp", "dp"),
        check_vma=False,
    )
```

```python
import functools
import math

import jax
import jax.numpy as jnp
from jax import lax
from jax.experimental import pallas as pl
from jax.experimental.pallas import tpu as pltpu
from jax.sharding import PartitionSpec as P

HD = 32
LOG2E = 1.4426950408889634
FAR_BELOW = -1e30
FLOOR = -1e9
CODE_BITS = 8
CODE = 1 << CODE_BITS
TOGETHER = 4
UNROLL = 64
VMEM = pltpu.VMEM
LANES = 128
MESH = pl.DeviceIdType.MESH


def leaky_relu(scores):
    return jnp.maximum(scores, 0.2 * scores)


def main_kernel(
    heads,
    capacity,
    chunks,
    depth,
    peers,
    weight_in,
    nodes_in,
    att_src_in,
    att_dst_in,
    bias_in,
    tiles_in,
    rows_in,
    cols_in,
    feats_ref,
    total_ref,
    part_ref,
    stats_ref,
    other_ref,
    mass_ref,
    part_mass_ref,
    nodes_ref,
    bias_ref,
    *scratch,
):
    (
        first_half,
        all_source,
        targ,
        all_nodes,
        masks_out,
        masks2,
        code_rows,
        codes_out,
        pick,
        got_codes,
        u_send,
        u_all,
        score_send,
        score_recv,
        table_v,
        table,
        weights,
        keeps,
        scales,
        bests,
        scan,
        part_send,
        mass_send,
        stats_send,
        node_send,
        node_recv,
        u_ss,
        u_rs,
        score_ss,
        score_rs,
        mask_ss,
        mask_rs,
        code_ss,
        code_rs,
        far_ss,
        facing_ss,
        core_ss,
        recv_sem,
        pair_ss,
        pair_rs,
        part_ss,
        part_rs,
        mass_ss,
        mass_rs,
        local_sem,
        pick_sem,
        load_sem,
        weight_ref,
        att_src_ref,
        att_dst_ref,
        tiles_ref,
        tile_rows,
        tile_cols,
    ) = scratch[: len(scratch) - heads]
    second_half = scratch[len(scratch) - heads :]

    devices = 4 * depth
    groups = depth // 2
    me = lax.axis_index("dp")
    core = lax.rem(me, 2)
    beside = lax.rem(lax.div(me, 2), 2)
    level = lax.div(me, 4)
    parity = lax.rem(level, 2)
    where_in = lax.div(level, 2)
    mine = lax.axis_index("mp")
    dims, columns = nodes_in.shape
    head_dims = weight_in.shape[0]
    size = LANES
    blocks = columns // size
    hb = blocks // 2
    per = blocks // chunks
    width = per * size
    slots = devices * capacity
    early = chunks // 2
    score_item = early
    items = early + 1 + heads

    def place(lev, b, c):
        return (lev * 2 + b) * 2 + c

    def origin_of(q, b, c):
        return (q * 2 + b) * 2 + c

    own = origin_of(where_in, beside, core)
    facing = place(level, 1 - beside, core)
    other_core = place(level, beside, 1 - core)
    pair = place(level + 1 - 2 * parity, beside, core)

    loads = [
        pltpu.make_async_copy(source, target, load_sem.at[number])
        for number, (source, target) in enumerate(
            (
                (weight_in, weight_ref),
                (att_src_in, att_src_ref),
                (att_dst_in, att_dst_ref),
                (nodes_in, nodes_ref),
                (rows_in, tile_rows),
                (cols_in, tile_cols),
                (tiles_in, tiles_ref),
                (bias_in, bias_ref),
            )
        )
    ]
    for load in loads:
        load.start()
    barrier = pltpu.get_barrier_semaphore()
    for shift in range(1, devices):
        pl.semaphore_signal(barrier, 1, device_id={"dp": lax.rem(me + shift, devices)}, device_id_type=MESH)
    for shift in range(1, peers):
        pl.semaphore_signal(barrier, 1, device_id={"mp": lax.rem(mine + shift, peers)}, device_id_type=MESH)

    own_rows = pl.ds(pl.multiple_of(mine * dims, dims), dims)

    def as_column(ref):
        row = ref[...]
        if head_dims < LANES:
            row = jnp.concatenate([row, jnp.zeros((1, LANES - head_dims), row.dtype)], axis=1)
        return jnp.transpose(jnp.concatenate([row] * 8, axis=0))[:head_dims, 0:1]

    for load in loads[:3]:
        load.wait()
    wide = weight_ref[...].astype(jnp.float32)
    by_source = wide * (LOG2E * as_column(att_src_ref))
    by_target = wide * (LOG2E * as_column(att_dst_ref))
    rows = []
    for scaled in (by_source, by_target):
        for head in range(heads):
            rows.append(jnp.sum(scaled[head * HD : (head + 1) * HD], axis=0, keepdims=True))
    reduced = jnp.concatenate(rows, axis=0)
    for peer in range(peers):
        u_send[peer] = reduced[:, peer * dims : (peer + 1) * dims]
    u_all[mine] = u_send[mine]
    for load in loads[3:]:
        load.wait()
    pl.semaphore_wait(barrier, devices - 1 + peers - 1)

    def node_copy(shift, chunk):
        return pltpu.make_async_remote_copy(
            src_ref=nodes_ref.at[:, pl.ds(chunk * width, width)],
            dst_ref=all_nodes.at[chunk, own_rows, :],
            send_sem=node_send.at[shift - 1, chunk],
            recv_sem=node_recv.at[shift - 1, chunk],
            device_id={"mp": lax.rem(mine + shift, peers)},
            device_id_type=MESH,
        )

    def u_copy(shift):
        to = lax.rem(mine + shift, peers)
        return pltpu.make_async_remote_copy(
            src_ref=u_send.at[to],
            dst_ref=u_all.at[mine],
            send_sem=u_ss.at[shift - 1],
            recv_sem=u_rs.at[shift - 1],
            device_id={"mp": to},
            device_id_type=MESH,
        )

    def score_copy(shift, side):
        to = lax.rem(mine + shift, peers)
        return pltpu.make_async_remote_copy(
            src_ref=score_send.at[side, to],
            dst_ref=score_recv.at[side, mine],
            send_sem=score_ss.at[side, shift - 1],
            recv_sem=score_rs.at[side, shift - 1],
            device_id={"mp": to},
            device_id_type=MESH,
        )

    def mask_copy(shift):
        to = lax.rem(me + shift, devices)
        return pltpu.make_async_remote_copy(
            src_ref=masks_out.at[pl.ds(to * capacity, capacity)],
            dst_ref=masks2.at[pl.ds(me * capacity, capacity)],
            send_sem=mask_ss.at[shift - 1],
            recv_sem=mask_rs.at[shift - 1],
            device_id={"dp": to},
            device_id_type=MESH,
        )

    def code_copy(shift):
        to = lax.rem(me + shift, devices)
        return pltpu.make_async_remote_copy(
            src_ref=codes_out,
            dst_ref=got_codes.at[me],
            send_sem=code_ss.at[shift - 1],
            recv_sem=code_rs.at[shift - 1],
            device_id={"dp": to},
            device_id_type=MESH,
        )

    def pair_copy(which):
        src, dst = (
            (masks2.at[pl.ds(0, slots)], masks2.at[pl.ds(slots, slots)]),
            (targ.at[pl.ds(blocks, blocks)], targ.at[pl.ds(0, blocks)]),
            (stats_send, other_ref),
        )[which]
        return pltpu.make_async_remote_copy(
            src_ref=src,
            dst_ref=dst,
            send_sem=pair_ss.at[which],
            recv_sem=pair_rs.at[which],
            device_id={"dp": pair},
            device_id_type=MESH,
        )

    def part_copy(head):
        return pltpu.make_async_remote_copy(
            src_ref=part_send.at[head],
            dst_ref=part_ref.at[head],
            send_sem=part_ss.at[head],
            recv_sem=part_rs.at[head],
            device_id={"dp": pair},
            device_id_type=MESH,
        )

    def mass_copy(head):
        return pltpu.make_async_remote_copy(
            src_ref=mass_send.at[head],
            dst_ref=part_mass_ref.at[head],
            send_sem=mass_ss.at[head],
            recv_sem=mass_rs.at[head],
            device_id={"dp": pair},
            device_id_type=MESH,
        )

    def item_ref(origin, item):
        if item < early:
            return first_half.at[pl.ds(origin * hb + item * per, per)]
        if item == score_item:
            return all_source.at[pl.ds(origin * blocks, blocks)]
        return second_half[item - score_item - 1].at[pl.ds(origin * hb, hb)]

    def send(origin, item, to, sem):
        part = item_ref(origin, item)
        return pltpu.make_async_remote_copy(
            src_ref=part,
            dst_ref=part,
            send_sem=sem,
            recv_sem=recv_sem.at[origin, item],
            device_id={"dp": to},
            device_id_type=MESH,
        )

    def far_copy(shift, item):
        to = place(2 * lax.rem(where_in + shift, groups) + parity, beside, core)
        return send(own, item, to, far_ss.at[shift - 1, item])

    def facing_copy(q, item):
        return send(origin_of(q, beside, core), item, facing, facing_ss.at[q, item])

    def core_copy(q, b, item):
        return send(origin_of(q, b, core), item, other_core, core_ss.at[q, b, item])

    def arrival(origin, item):
        send(origin, item, other_core, core_ss.at[0, 0, item]).wait_recv()

    def own_core(item):
        core_copy(where_in, beside, item).start()

    def own_far(item):
        for shift in range(1, groups):
            far_copy(shift, item).start()

    at_end = (level == 0) | (level == depth - 1)

    def far_if_end(item):
        pl.when(at_end)(lambda: own_far(item))

    def far_if_middle(item):
        pl.when(jnp.logical_not(at_end))(lambda: own_far(item))

    def own_facing(item):
        facing_copy(where_in, item).start()

    def own_out(item):
        own_far(item)
        own_near(item)

    def own_near(item):
        own_facing(item)
        own_core(item)

    def far_q(shift):
        return lax.rem(where_in + groups - shift, groups)

    def from_far(item):
        for shift in range(1, groups):
            q = far_q(shift)
            arrival(origin_of(q, beside, core), item)
            facing_copy(q, item).start()
            core_copy(q, beside, item).start()

    def from_facing(item):
        arrival(origin_of(where_in, 1 - beside, core), item)
        core_copy(where_in, 1 - beside, item).start()

    def from_facing_far(item):
        for shift in range(1, groups):
            q = far_q(shift)
            arrival(origin_of(q, 1 - beside, core), item)
            core_copy(q, 1 - beside, item).start()

    def from_core(item):
        for q in range(groups):
            for b in range(2):
                arrival(origin_of(q, b, 1 - core), item)

    def project(chunk):
        for shift in range(1, peers):
            node_copy(shift, chunk).wait_recv()
        projected = jnp.dot(weight_ref[...], all_nodes[chunk], preferred_element_type=jnp.float32)
        rounded = projected.astype(jnp.bfloat16)
        for j in range(per):
            block = chunk * per + j
            span = slice(j * size, (j + 1) * size)
            feats_ref[block] = rounded[:, span]
            if chunk < early:
                first_half[own * hb + block] = rounded[:, span]
            else:
                for head in range(heads):
                    second_half[head][own * hb + block - hb] = rounded[head * HD : (head + 1) * HD, span]

    for shift in range(1, peers):
        u_copy(shift).start()
    for shift in range(1, peers):
        node_copy(shift, 0).start()

    tile_count = tile_rows.shape[0]
    owners = [lax.div(tile_rows[t], blocks) for t in range(tile_count)]
    lane = lax.broadcasted_iota(jnp.int32, (1, LANES), 1)
    packed = jnp.zeros((1, LANES), jnp.int32)
    tile_at = jnp.zeros((1, LANES), jnp.int32)
    for t in range(tile_count):
        turn = jnp.int32(0)
        for earlier in range(t):
            turn = turn + jnp.where(owners[earlier] == owners[t], 1, 0)
        row, column = tile_rows[t], tile_cols[t]
        column_owner = lax.div(column, blocks)
        column_level = lax.div(column_owner, 4)
        group = lax.div(column_level, 2) * 4 + lax.rem(column_owner, 4)
        code = (group * blocks + lax.rem(column, blocks)) * 2 + lax.rem(column_level, 2)
        code = code * CODE + row - owners[t] * blocks + 1
        at = lane == owners[t] * capacity + turn
        packed = jnp.where(at, code, packed)
        tile_at = jnp.where(at, t, tile_at)
    codes_out[...] = packed
    got_codes[me] = packed
    code_rows[0:1] = tile_at
    code_rows[1:8] = jnp.zeros((7, LANES), jnp.int32)
    fetch = pltpu.make_async_copy(code_rows, pick, pick_sem)
    fetch.start()
    for shift in range(1, devices):
        code_copy(shift).start()
    for chunk in range(chunks):
        all_nodes[chunk, own_rows, :] = nodes_ref[:, chunk * width : (chunk + 1) * width]
    fetch.wait()
    for slot in range(slots):
        masks_out[slot] = tiles_ref[pick[0, slot]]
    masks2[pl.ds(me * capacity, capacity)] = masks_out[pl.ds(me * capacity, capacity)]
    for shift in range(1, devices):
        mask_copy(shift).start()

    for shift in range(1, peers):
        u_copy(shift).wait_recv()
    stacked = jnp.concatenate([u_all[peer] for peer in range(peers)], axis=0)
    high = stacked.astype(jnp.bfloat16)
    rest = stacked - high.astype(jnp.float32)
    middle = rest.astype(jnp.bfloat16)
    low = (rest - middle.astype(jnp.float32)).astype(jnp.bfloat16)
    pieces = jnp.concatenate([high, middle, low], axis=0)
    count = 2 * heads * peers
    scored = jnp.dot(pieces, nodes_ref[...], preferred_element_type=jnp.float32)
    scored = scored[:count] + scored[count : 2 * count] + scored[2 * count :]
    for side in range(2):
        for peer in range(peers):
            at = (2 * peer + side) * heads
            score_send[side, peer] = scored[at : at + heads]
        score_recv[side, mine] = score_send[side, mine]
        for shift in range(1, peers):
            score_copy(shift, side).start()
    for chunk in range(1, chunks):
        for shift in range(1, peers):
            node_copy(shift, chunk).start()

    def added(side):
        for shift in range(1, peers):
            score_copy(shift, side).wait_recv()
        scores = score_recv[side, 0]
        for peer in range(1, peers):
            scores = scores + score_recv[side, peer]
        return scores

    project(0)
    far_if_middle(0)
    source_scores = added(0)
    for block in range(blocks):
        span = slice(block * size, (block + 1) * size)
        all_source[own * blocks + block] = source_scores[:, span]
    own_out(score_item)
    own_near(0)
    target_scores = added(1)
    for block in range(blocks):
        span = slice(block * size, (block + 1) * size)
        targ[blocks + block] = target_scores[:, span]
        stats_ref[0, block] = leaky_relu(source_scores[:, span] + target_scores[:, span])
    pair_copy(1).start()
    far_if_end(0)

    def forward_masks():
        for shift in range(1, devices):
            mask_copy(shift).wait_recv()
        pair_copy(0).start()

    def order():
        for shift in range(1, devices):
            code_copy(shift).wait_recv()
        lane = lax.broadcasted_iota(jnp.int32, (1, LANES), 1)
        bits = blocks.bit_length() - 1
        for which, holder in enumerate((pair, me)):
            codes = jnp.zeros((1, LANES), jnp.int32)
            for device in range(devices):
                turn = lax.rem((device - holder) * capacity + devices * LANES, LANES)
                moved = pltpu.roll(got_codes[device], turn, 1)
                here = (lane >= device * capacity) & (lane < (device + 1) * capacity)
                codes = jnp.where(here, moved, codes)
            row = jnp.bitwise_and(codes, CODE - 1)
            column_parity = jnp.bitwise_and(jnp.right_shift(codes, CODE_BITS), 1)
            column = jnp.right_shift(codes, CODE_BITS + 1)
            block = jnp.bitwise_and(column, blocks - 1)
            late = jnp.right_shift(block, bits - 1)
            spot = jnp.right_shift(column, bits) * hb + jnp.bitwise_and(block, hb - 1)
            lanes = LANES
            key = jnp.where((row > 0) & (column_parity == parity), row - 1, blocks)
            turned = jnp.transpose(jnp.concatenate([key, column, spot, late] + [key] * 4, axis=0))
            key_t = turned[:, 0:1]
            column_t = turned[:, 1:2]
            spot_t = turned[:, 2:3]
            late_t = turned[:, 3:4]
            along = lax.broadcasted_iota(jnp.int32, (lanes, lanes), 1)
            down = lax.broadcasted_iota(jnp.int32, (lanes, lanes), 0)
            before = (key_t < key) | ((key_t == key) & (down < along))
            rank = jnp.sum(jnp.where(before, 1, 0), axis=0, keepdims=True)
            rank_t = jnp.transpose(jnp.concatenate([rank] * 8, axis=0))[:, 0:1]
            at = rank_t == along
            slot = jnp.sum(jnp.where(at, down, 0), axis=0, keepdims=True)
            table_v[which, 0:1] = (1 - which) * slots + jnp.minimum(slot, slots - 1)
            table_v[which, 1:2] = jnp.sum(jnp.where(at, key_t, 0), axis=0, keepdims=True)
            table_v[which, 2:3] = jnp.sum(jnp.where(at, column_t, 0), axis=0, keepdims=True)
            table_v[which, 3:4] = jnp.sum(jnp.where(key_t <= along, 1, 0), axis=0, keepdims=True)
            table_v[which, 4:5] = jnp.sum(jnp.where(at, spot_t, 0), axis=0, keepdims=True)
            table_v[which, 5:6] = jnp.sum(jnp.where(at, late_t, 0), axis=0, keepdims=True)
            table_v[which, 6:8] = jnp.zeros((2, lanes), jnp.int32)
        table_copy().start()

    def table_copy():
        return pltpu.make_async_copy(table_v, table, local_sem)

    words = size // 32
    to_sign = 31 - lax.broadcasted_iota(jnp.int32, (32, size), 0)

    def partial(which, k):
        slot = table[which, 0, k]
        key = table[which, 1, k]
        column = table[which, 2, k]
        packed = masks2[slot] * jnp.where(key < blocks, 1, 0)
        edges = jnp.concatenate(
            [
                jnp.left_shift(packed[word : word + 1, :], to_sign)
                for word in range(words)
            ],
            axis=0,
        ) < 0
        source = all_source[column]
        source = jnp.transpose(jnp.concatenate([source] * (8 // heads), axis=0))
        target = targ[which * blocks + jnp.minimum(key, blocks - 1)]
        peaks = []
        for head in range(heads):
            one = slice(head, head + 1)
            here = jnp.where(edges, source[:, one], FAR_BELOW)
            aim = target[one]
            peak = leaky_relu(aim + jnp.max(here, axis=0, keepdims=True))
            peak = jnp.maximum(peak, FLOOR)
            weight = jnp.exp2(leaky_relu(here + aim) - peak)
            peaks.append(peak)
            weights[which * slots + k, head] = weight.astype(jnp.bfloat16)
        same = (k > 0) & (key == table[which, 1, jnp.maximum(k - 1, 0)])
        return same, jnp.concatenate(peaks, axis=0)

    together = math.gcd(slots, TOGETHER)
    turns = math.gcd(slots, 4) // together
    steps = slots // (together * turns)

    def weigh(which, index, run):
        parts = [(index * together + w, partial(which, index * together + w)) for w in range(together)]
        for k, (same, peak) in parts:
            again = jnp.where(same, 1.0, 0.0)
            old = jnp.where(same, run, FLOOR)
            run = jnp.maximum(old, peak)
            spot = which * slots + k
            keeps[spot] = jnp.exp2(old - run) * again
            scales[spot] = jnp.exp2(peak - run)
            bests[spot] = run
        return run

    def fresh():
        return jnp.full((heads, size), FLOOR, jnp.float32)

    ones = jnp.ones((16, size), jnp.bfloat16)

    def multiply(which, head, first, unroll, total):
        rows = slice(head * HD, (head + 1) * HD)
        one = slice(head, head + 1)
        values = []
        for w in range(unroll):
            spot = table[which, 4, first + w]
            late = table[which, 5, first + w]
            feats = jnp.where(late == 0, first_half[spot, rows], second_half[head][spot])
            feats = jnp.concatenate([feats, ones], axis=0)
            values.append(
                jnp.dot(feats, weights[which * slots + first + w, head], preferred_element_type=jnp.float32)
            )
        for w in range(unroll):
            spot = which * slots + first + w
            total = total * keeps[spot, one] + values[w][: HD + 8] * scales[spot, one]
            scan[first + w] = total
        return total

    def ending(which, key):
        upto = table[which, 3, key]
        prior = table[which, 3, key - 1] if key > 0 else 0
        return jnp.maximum(upto - 1, 0), upto > prior

    def play(events):
        for what, item in events:
            what(item)

    first = score_item + 1
    standard = early == 4 and heads == 4 and chunks == 8 and steps == 16

    def near_weights(count, state):
        at, carry = state
        body = functools.partial(weigh, 0)
        return at + count, lax.fori_loop(at * turns, (at + count) * turns, body, carry)

    def own_weights(count, state):
        at, carry = state
        body = functools.partial(weigh, 1)
        return at + count, lax.fori_loop(at * turns, (at + count) * turns, body, carry)

    def near_values(head):
        from_core(first + head)

        def body(index, total):
            return multiply(0, head, index * unroll, unroll, total)

        lax.fori_loop(0, slots // unroll, body, jnp.zeros((HD + 8, size), jnp.float32))
        for block in range(blocks):
            index, some = ending(0, block)
            found = jnp.where(some, scan[index], 0.0)
            part_send[head, block] = found[:HD].astype(jnp.bfloat16)
            mass_send[head, block : block + 1] = found[HD : HD + 1]
        part_copy(head).start()
        mass_copy(head).start()

    def own_values(head):
        def body(index, total):
            return multiply(1, head, index * unroll, unroll, total)

        lax.fori_loop(0, slots // unroll, body, jnp.zeros((HD + 8, size), jnp.float32))
        for block in range(blocks):
            index, some = ending(1, block)
            found = jnp.where(some, scan[index], 0.0)
            total_ref[head, block] = found[:HD]
            mass_ref[head, block : block + 1] = found[HD : HD + 1]

    def near_stats():
        for block in range(blocks):
            index, some = ending(0, block)
            stats_send[block] = jnp.where(some, bests[index], FLOOR)
        pair_copy(2).start()

    def ready_to_weigh():
        table_copy().wait()
        from_core(score_item)
        pair_copy(1).wait_recv()
        pair_copy(0).wait_recv()

    unroll = math.gcd(slots, UNROLL)
    near = (0, fresh())
    mine_state = (0, fresh())
    if standard:
        project(1)
        far_if_middle(1)
        own_near(1)
        forward_masks()
        order()
        project(2)
        from_facing(score_item)
        far_if_middle(2)
        far_if_end(1)
        own_near(2)
        from_far(score_item)
        project(3)
        far_if_middle(3)
        own_near(3)
        project(4)
        far_if_end(2)
        from_facing_far(score_item)
        project(5)
        far_if_end(3)
        from_far(0)
        project(6)
        ready_to_weigh()
        near = near_weights(1, near)
        near = near_weights(1, near)
        project(7)
        for head in range(heads):
            far_if_middle(first + head)
            own_core(first + head)
        own_facing(first)
        far_if_end(first)
        near = near_weights(4, near)
        play([(far_if_end, first + 1), (from_far, 1)])
        near = near_weights(2, near)
        play([(from_far, 2)])
        near = near_weights(3, near)
        play([(far_if_end, first + 2), (from_far, 3)])
        play([(from_facing, 0), (from_facing, 1), (from_facing, 2), (from_facing, 3)])
        near = near_weights(3, near)
        play([(from_far, first), (own_facing, first + 1), (far_if_end, first + 3)])
        near = near_weights(2, near)
        near_stats()
        play([(from_facing, first), (from_facing_far, 0), (from_facing_far, 1)])
        mine_state = own_weights(2, mine_state)
        play([(from_facing_far, 2), (from_facing_far, 3)])
        mine_state = own_weights(2, mine_state)
        play([(from_far, first + 1), (own_facing, first + 2)])
        mine_state = own_weights(1, mine_state)
        play([(from_facing_far, first)])
        mine_state = own_weights(1, mine_state)
        for item in range(early):
            from_core(item)
        near_values(0)
        play([(from_far, first + 2), (own_facing, first + 3), (from_facing, first + 1)])
        mine_state = own_weights(2, mine_state)
        play([(from_facing_far, first + 1)])
        mine_state = own_weights(2, mine_state)
        play([(from_far, first + 3)])
        near_values(1)
        play([(from_facing, first + 2), (from_facing_far, first + 2)])
        mine_state = own_weights(2, mine_state)
        near_values(2)
        play([(from_facing, first + 3), (from_facing_far, first + 3)])
        mine_state = own_weights(1, mine_state)
        near_values(3)
        mine_state = own_weights(3, mine_state)
        for head in range(heads):
            own_values(head)
    else:
        for chunk in range(1, chunks):
            project(chunk)
            if chunk < early:
                own_out(chunk)
        forward_masks()
        order()
        for head in range(heads):
            own_out(first + head)
        for item in [score_item] + [i for i in range(items) if i != score_item]:
            play([(from_facing, item), (from_far, item), (from_facing_far, item)])
        ready_to_weigh()
        near = near_weights(steps, near)
        near_stats()
        mine_state = own_weights(steps, mine_state)
        for item in range(early):
            from_core(item)
        for head in range(heads):
            near_values(head)
            own_values(head)

    for block in range(blocks):
        index, some = ending(1, block)
        stats_ref[1, block] = jnp.where(some, bests[slots + index], FLOOR)
    for shift in range(1, peers):
        u_copy(shift).wait_send()
        for side in range(2):
            score_copy(shift, side).wait_send()
        for chunk in range(chunks):
            node_copy(shift, chunk).wait_send()
    for shift in range(1, devices):
        code_copy(shift).wait_send()
        mask_copy(shift).wait_send()
    for item in range(items):
        for shift in range(1, groups):
            far_copy(shift, item).wait_send()
        for q in range(groups):
            facing_copy(q, item).wait_send()
            for b in range(2):
                core_copy(q, b, item).wait_send()
    for which in range(3):
        pair_copy(which).wait_send()
    pair_copy(2).wait_recv()
    for head in range(heads):
        part_copy(head).wait()
        mass_copy(head).wait()


def finish_kernel(
    heads,
    feats_ref,
    total_ref,
    part_ref,
    stats_ref,
    other_ref,
    mass_ref,
    part_mass_ref,
    nodes_ref,
    bias_ref,
    out_ref,
):
    blocks = feats_ref.shape[0]
    size = LANES
    row = bias_ref[...]
    width = row.shape[1]
    if width < LANES:
        row = jnp.concatenate([row, jnp.zeros((1, LANES - width), row.dtype)], axis=1)
    bias = jnp.transpose(jnp.concatenate([row] * 8, axis=0))[:width, 0:1]
    for block in range(blocks):
        span = slice(block * size, (block + 1) * size)
        itself = stats_ref[0, block]
        here = stats_ref[1, block]
        there = other_ref[block]
        mass = jnp.concatenate([mass_ref[head, block : block + 1] for head in range(heads)], axis=0)
        part_mass = jnp.concatenate([part_mass_ref[head, block : block + 1] for head in range(heads)], axis=0)
        best = jnp.maximum(jnp.maximum(itself, here), there)
        alone = jnp.exp2(itself - best)
        near = jnp.exp2(here - best)
        away = jnp.exp2(there - best)
        shared = 1.0 / (alone + near * mass + away * part_mass)
        alone = alone * shared
        near = near * shared
        away = away * shared
        for head in range(heads):
            rows = slice(head * HD, (head + 1) * HD)
            one = slice(head, head + 1)
            flat = (
                total_ref[head, block] * near[one]
                + part_ref[head, block].astype(jnp.float32) * away[one]
                + feats_ref[block, rows].astype(jnp.float32) * alone[one]
                + nodes_ref[rows, span].astype(jnp.float32)
                + bias[rows]
            )
            out_ref[rows, span] = jnp.where(flat > 0, flat, jnp.exp(flat) - 1.0).astype(out_ref.dtype)


def local(node_feats, proj_weight, att_src, att_dst, out_bias, tile_rows, tile_cols, tile_masks):
    dims, columns = node_feats.shape
    head_dims, inputs = proj_weight.shape
    heads = head_dims // HD
    size = tile_masks.shape[2]
    words = tile_masks.shape[1]
    blocks = columns // size
    devices = lax.axis_size("dp")
    peers = lax.axis_size("mp")
    capacity = max(2, 2 * tile_rows.shape[0] // devices)
    depth = devices // 4
    groups = depth // 2
    origins = groups * 4
    chunks = math.gcd(blocks, max(2, 128 // devices))
    early = chunks // 2
    items = early + 1 + heads
    slots = devices * capacity
    positions = 2 * slots
    hb = blocks // 2
    whole = pl.BlockSpec(memory_space=VMEM)
    smem = pltpu.SMEM
    dma = pltpu.SemaphoreType.DMA
    f32 = jnp.float32
    bf16 = jnp.bfloat16
    others = max(1, peers - 1)
    feats, total, part, stats, other, mass, part_mass, nodes, bias = pl.pallas_call(
        functools.partial(main_kernel, heads, capacity, chunks, depth, peers),
        out_shape=(
            jax.ShapeDtypeStruct((blocks, head_dims, size), bf16),
            jax.ShapeDtypeStruct((heads, blocks, HD, size), f32),
            jax.ShapeDtypeStruct((heads, blocks, HD, size), bf16),
            jax.ShapeDtypeStruct((2, blocks, heads, size), f32),
            jax.ShapeDtypeStruct((blocks, heads, size), f32),
            jax.ShapeDtypeStruct((heads, blocks, size), f32),
            jax.ShapeDtypeStruct((heads, blocks, size), f32),
            jax.ShapeDtypeStruct((dims, columns), bf16),
            jax.ShapeDtypeStruct((1, head_dims), f32),
        ),
        in_specs=[pl.BlockSpec(memory_space=pltpu.HBM)] * 8,
        out_specs=(whole,) * 9,
        scratch_shapes=[
            VMEM((origins * hb, head_dims, size), bf16),
            VMEM((origins * blocks, heads, size), f32),
            VMEM((2 * blocks, heads, size), f32),
            VMEM((chunks, inputs, columns // chunks), bf16),
            VMEM((slots, words, size), jnp.int32),
            VMEM((2 * slots, words, size), jnp.int32),
            VMEM((8, LANES), jnp.int32),
            VMEM((1, LANES), jnp.int32),
            smem((8, LANES), jnp.int32),
            VMEM((devices, 1, LANES), jnp.int32),
            VMEM((peers, 2 * heads, dims), f32),
            VMEM((peers, 2 * heads, dims), f32),
            VMEM((2, peers, heads, columns), f32),
            VMEM((2, peers, heads, columns), f32),
            VMEM((2, 8, LANES), jnp.int32),
            smem((2, 8, LANES), jnp.int32),
            VMEM((positions, heads, size, size), bf16),
            VMEM((positions, heads, size), f32),
            VMEM((positions, heads, size), f32),
            VMEM((positions, heads, size), f32),
            VMEM((slots, HD + 8, size), f32),
            VMEM((heads, blocks, HD, size), bf16),
            VMEM((heads, blocks, size), f32),
            VMEM((blocks, heads, size), f32),
            dma((others, chunks)),
            dma((others, chunks)),
            dma((others,)),
            dma((others,)),
            dma((2, others)),
            dma((2, others)),
            dma((devices - 1,)),
            dma((devices - 1,)),
            dma((devices - 1,)),
            dma((devices - 1,)),
            dma((max(1, groups - 1), items)),
            dma((groups, items)),
            dma((groups, 2, items)),
            dma((origins, items)),
            dma((3,)),
            dma((3,)),
            dma((heads,)),
            dma((heads,)),
            dma((heads,)),
            dma((heads,)),
            dma,
            dma,
            dma((8,)),
            VMEM((head_dims, inputs), bf16),
            VMEM((1, head_dims), f32),
            VMEM((1, head_dims), f32),
            VMEM(tile_masks.shape, jnp.int32),
            smem(tile_rows.shape, jnp.int32),
            smem(tile_cols.shape, jnp.int32),
        ]
        + [VMEM((origins * hb, HD, size), bf16) for _ in range(heads)],
        compiler_params=pltpu.CompilerParams(
            collective_id=0, has_side_effects=True, vmem_limit_bytes=48 * 1024 * 1024
        ),
        name="graph",
    )(
        *[
            pltpu.with_memory_space_constraint(x, pltpu.HBM)
            for x in (
                proj_weight,
                node_feats,
                att_src.reshape(1, head_dims),
                att_dst.reshape(1, head_dims),
                out_bias.reshape(1, head_dims),
                tile_masks,
                tile_rows,
                tile_cols,
            )
        ]
    )
    return pl.pallas_call(
        functools.partial(finish_kernel, heads),
        out_shape=jax.ShapeDtypeStruct((head_dims, columns), bf16),
        in_specs=[whole] * 9,
        out_specs=whole,
        compiler_params=pltpu.CompilerParams(vmem_limit_bytes=40 * 1024 * 1024),
        name="finish",
    )(feats, total, part, stats, other, mass, part_mass, nodes, bias)


def solution(mesh):
    return jax.shard_map(
        local,
        mesh=mesh,
        in_specs=(
            P("mp", "dp"),
            P("mp", None),
            P("mp"),
            P("mp"),
            P("mp"),
            P("dp"),
            P("dp"),
            P("dp", None, None),
        ),
        out_specs=P("mp", "dp"),
        check_vma=False,
    )
```
